128 devices in a mesh: tp: 16 (over z, y), dp: 8 (over x, core).
Axes of the slice: x: 4, y: 4, z: 4, core: 2. Of those that a mesh axis runs over, the one named last changes fastest.
Arguments:
- hidden: bfloat16 [8192, 576], P('dp')
- norm_w: bfloat16 [576], replicated
- emb_table: bfloat16 [49152, 576], P('tp')
- teacher: bfloat16 [8192, 49152], P('dp', 'tp')
- loss_mask: int32 [8192], P('dp')
Outputs:
- output 1: float32 [], replicated
- output 2: bfloat16 [8192, 576], P('dp')
- output 3: float32 [49152, 576], P('tp', 'dp')
- output 4: float32 [576], replicated
All inputs are finite; a program needn't handle non-finite values.
Results may differ from the reference program's by a relative error of at most 0.001.
Values sent between devices are 32-bit elements.
A program may use at most 1 GiB of HBM per device.

```python
import jax
import jax.numpy as jnp
from jax import lax

MODEL_DIM = 576
VOCAB_SIZE = 49152
TOK_DEV = 1024
DP_SHARDS = 8
TOKENS = TOK_DEV * DP_SHARDS
SOFT_CAP = 30.0
NORM_EPS = 1e-6


def setup_inputs(seed: int = 0) -> dict:
    base_key = jax.random.key(seed)
    key_list = jax.random.split(base_key, 6)
    hidden = jax.random.normal(key_list[0], (TOKENS, MODEL_DIM), jnp.float32)
    norm_w = 0.5 * jax.random.normal(key_list[1], (MODEL_DIM,), jnp.float32)
    mean_dir = jax.random.normal(key_list[2], (MODEL_DIM,), jnp.float32)
    emb_noise = jax.random.normal(key_list[3], (VOCAB_SIZE, MODEL_DIM), jnp.float32)
    emb_table = (18.0 * mean_dir[None, :] + 1.5 * emb_noise) * (MODEL_DIM ** -0.5)
    teacher = 2.0 * jax.random.normal(key_list[4], (TOKENS, VOCAB_SIZE), jnp.float32)
    lengths = jax.random.randint(key_list[5], (DP_SHARDS,), 1, TOK_DEV + 1)
    lengths = jnp.where(jnp.arange(DP_SHARDS) == 0, TOK_DEV, lengths)
    loss_mask = (jnp.arange(TOK_DEV)[None, :] < lengths[:, None]).astype(jnp.int32)
    return {'hidden': hidden.astype(jnp.bfloat16), 'norm_w': norm_w.astype(jnp.bfloat16), 'emb_table': emb_table.astype(jnp.bfloat16), 'teacher': teacher.astype(jnp.bfloat16), 'loss_mask': loss_mask.reshape(TOKENS)}


def rms_norm(hid_f32, scale_f32):
    inv_rms = lax.rsqrt(jnp.mean(hid_f32 * hid_f32, axis=-1, keepdims=True) + NORM_EPS)
    return hid_f32 * inv_rms * (1.0 + scale_f32)


def reference(hidden, norm_w, emb_table, teacher, loss_mask):
    mask_f32 = loss_mask.astype(jnp.float32)
    weights = mask_f32 / jnp.sum(mask_f32)
    scale_f32 = norm_w.astype(jnp.float32)

    def block_step(acc_state, blk_inputs):
        emb_acc, scale_acc = acc_state
        hid_blk, teach_blk, weight_blk = blk_inputs
        normed_f32, norm_pull = jax.vjp(rms_norm, hid_blk.astype(jnp.float32), scale_f32)
        normed = normed_f32.astype(jnp.bfloat16)
        raw_logit = jnp.dot(normed, emb_table.T, preferred_element_type=jnp.float32)
        tanh_val = jnp.tanh(raw_logit / SOFT_CAP)
        capped = SOFT_CAP * tanh_val
        log_stu = jax.nn.log_softmax(capped, axis=-1)
        log_tea = jax.nn.log_softmax(teach_blk.astype(jnp.float32), axis=-1)
        prob_tea = jnp.exp(log_tea)
        kl_tok = jnp.sum(prob_tea * (log_tea - log_stu), axis=-1)
        loss_part = jnp.sum(weight_blk * kl_tok)
        d_raw = ((jnp.exp(log_stu) - prob_tea) * weight_blk[:, None] * (1.0 - tanh_val * tanh_val)).astype(jnp.bfloat16)
        grad_normed = jnp.dot(d_raw, emb_table, preferred_element_type=jnp.float32)
        emb_acc = emb_acc + jnp.dot(d_raw.T, normed, preferred_element_type=jnp.float32)
        grad_hid, grad_scale = norm_pull(grad_normed)
        return (emb_acc, scale_acc + grad_scale), (loss_part, grad_hid.astype(jnp.bfloat16))

    blocks_in = (hidden.reshape(DP_SHARDS, TOK_DEV, MODEL_DIM), teacher.reshape(DP_SHARDS, TOK_DEV, VOCAB_SIZE), weights.reshape(DP_SHARDS, TOK_DEV))
    start_acc = (jnp.zeros((VOCAB_SIZE, MODEL_DIM), jnp.float32), jnp.zeros((MODEL_DIM,), jnp.float32))
    final_acc, per_block = lax.scan(block_step, start_acc, blocks_in)
    d_emb, d_norm_w = final_acc
    loss_parts, grad_hid = per_block
    return jnp.sum(loss_parts), grad_hid.reshape(TOKENS, MODEL_DIM), d_emb, d_norm_w
```

```python
import jax
import jax.numpy as jnp
from jax import lax
from jax.experimental import pallas as pl
from jax.experimental.pallas import tpu as pltpu
from jax.sharding import PartitionSpec as P

CAP = 30.0
EPS = 1e-6
LOG2E = 1.4426950408889634
MESH = pl.DeviceIdType.MESH
F32 = jnp.float32
BF16 = jnp.bfloat16
RB = 32


def build(tok, dim, voc, nt, nd):
    side = 4
    ht = tok // 2
    zc = ht // side
    oc = zc // side
    zh = zc // 2
    cols = dim // nd
    nv = 4
    vc = voc // nv
    vh = vc // 2
    vb = 512 if voc % 512 == 0 else 128
    nvb = voc // vb
    half_d = dim // 2
    dpad = -(-dim // 128) * 128

    def kernel(hid, w_ref, mask_ref, e_hbm, t_hbm, loss_out, dh_out, det_out, dw_out,
               e_v, t_v, gb, gt, tv, dr, dg, dhf, acc, mcol, col, st_s, st_r, mk_s, mk_r, dwt_s, dwt_r, dwd_s, dwd_r,
               zr, p2r, det, d2r, xr,
               in_sem, ss_st, rs_st, ss_mk, rs_mk, ss_z, rs_z, ss_p, rs_p, ss_g, rs_g, ss_h, rs_h,
               ss_d, rs_d, ss_x, rs_x, ss_wt, rs_wt, ss_wd, rs_wd):
        t = lax.axis_index('tp')
        d = lax.axis_index('dp')
        z, y = t // side, lax.rem(t, side)
        x, c = d // 2, lax.rem(d, 2)
        sends = []

        def rcopy(src, dst, ssem, rsem, dev):
            cp = pltpu.make_async_remote_copy(src_ref=src, dst_ref=dst, send_sem=ssem, recv_sem=rsem,
                                              device_id=dev, device_id_type=MESH)
            cp.start()
            sends.append(cp)
            return cp

        in_cp = [pltpu.make_async_copy(e_hbm, e_v, in_sem.at[0])]
        for h in range(2):
            rows = pl.ds(h * ht, ht)
            in_cp.append(pltpu.make_async_copy(t_hbm.at[rows, :], t_v.at[rows, :], in_sem.at[1 + h]))
        for cp in (in_cp[1], in_cp[0], in_cp[2]):
            cp.start()

        barrier = pltpu.get_barrier_semaphore()
        for k in range(1, nt):
            pl.semaphore_signal(barrier, inc=1, device_id={'tp': lax.rem(t + k, nt), 'dp': d}, device_id_type=MESH)
        for k in range(1, nd):
            pl.semaphore_signal(barrier, inc=1, device_id={'tp': t, 'dp': lax.rem(d + k, nd)}, device_id_type=MESH)

        wp = 1.0 + w_ref[...].astype(F32)
        nb = min(256, tok)

        for i in range(tok // nb):
            r0 = i * nb
            xv = hid[r0:r0 + nb, :].astype(F32)
            s = lax.rsqrt(jnp.mean(xv * xv, axis=-1, keepdims=True) + EPS)
            g = xv * s * wp
            gb[r0:r0 + nb, :] = g.astype(BF16)
            gp = jnp.concatenate([g, jnp.zeros((nb, dpad - dim), F32)], axis=1) if dpad > dim else g
            gtv = gp.T
            gtv = jnp.concatenate([gtv[(2 * xx + cc) * cols:(2 * xx + cc + 1) * cols, :] for cc in range(2) for xx in range(side)], axis=0)
            gt[:, r0:r0 + nb] = gtv.astype(BF16)

        maskf = mask_ref[...].astype(F32)
        mk_s[...] = jnp.broadcast_to(jnp.sum(maskf, axis=1, keepdims=True), (8, 128))
        mk_r[d] = mk_s[...]
        pl.semaphore_wait(barrier, nt + nd - 2)
        mk_cp = [rcopy(mk_s, mk_r.at[d], ss_mk.at[k], rs_mk.at[k], {'tp': t, 'dp': lax.rem(d + k, nd)}) for k in range(1, nd)]

        def forward(h):
            base = h * ht
            in_cp[1 + h].wait()
            if h == 0:
                in_cp[0].wait()

            def mx(i, _):
                r = pl.multiple_of(base + i * 64, 64)
                m = t_v[pl.ds(r, 64), 0:128]
                for q in range(1, voc // 128):
                    m = jnp.maximum(m, t_v[pl.ds(r, 64), q * 128:(q + 1) * 128])
                mm = jnp.max(m.astype(F32), axis=1, keepdims=True)
                mcol[pl.ds(pl.multiple_of(i * 64, 64), 64), :] = jnp.broadcast_to(mm, (64, 128))
                return 0

            lax.fori_loop(0, ht // 64, mx, 0)
            acc[...] = jnp.zeros_like(acc)

            def vstep(b, _):
                v0 = pl.multiple_of(b * vb, vb)
                tv[pl.ds(base, ht), pl.ds(v0, vb)] = lax.dot_general(
                    gb[pl.ds(base, ht), :], e_v[pl.ds(v0, vb), :], (((1,), (1,)), ((), ())), preferred_element_type=F32)

                def rstep(i, _):
                    r = pl.multiple_of(base + i * RB, RB)
                    a = pl.ds(pl.multiple_of(i * RB, RB), RB)
                    m = mcol[a, :]
                    zs = jnp.zeros((RB, 128), F32)
                    zt = jnp.zeros((RB, 128), F32)
                    qs = jnp.zeros((RB, 128), F32)
                    for q in range(vb // 128):
                        lanes = pl.ds(pl.multiple_of(v0 + q * 128, 128), 128)
                        th = jnp.tanh(tv[pl.ds(r, RB), lanes] * (1.0 / CAP))
                        tv[pl.ds(r, RB), lanes] = th
                        u = t_v[pl.ds(r, RB), lanes].astype(F32) - m
                        et = jnp.exp2(u * LOG2E)
                        zs = zs + jnp.exp2(th * (CAP * LOG2E))
                        zt = zt + et
                        qs = qs + et * (u - CAP * th)
                    acc[0, a, :] += zs
                    acc[1, a, :] += zt
                    acc[2, a, :] += qs
                    return 0

                lax.fori_loop(0, ht // RB, rstep, 0)
                return 0

            lax.fori_loop(0, nvb, vstep, 0)
            parts = [mcol[...].T[0:1, :]] + [jnp.sum(acc[k].T, axis=0, keepdims=True) for k in range(3)]
            st_s[h] = jnp.concatenate(parts + [jnp.zeros((4, ht), F32)], axis=0)
            st_r[h, t] = st_s[h]
            return [rcopy(st_s.at[h], st_r.at[h, t], ss_st.at[h, k], rs_st.at[h, k], {'tp': lax.rem(t + k, nt), 'dp': d})
                    for k in range(1, nt)]

        def combine(h, cps, inv_m):
            for cp in cps:
                cp.wait_recv()
            mts = st_r[h, :, 0, :]
            mt = jnp.max(mts, axis=0, keepdims=True)
            dm = jnp.maximum(mts - mt, -3e38)
            e = jnp.exp(dm)
            zte = st_r[h, :, 2, :] * e
            zt = jnp.sum(zte, axis=0, keepdims=True)
            zs = jnp.sum(st_r[h, :, 1, :], axis=0, keepdims=True)
            a = jnp.sum(st_r[h, :, 3, :] * e + zte * dm, axis=0, keepdims=True)
            kl = a / zt - jnp.log(zt) + jnp.log(zs)
            w = maskf[:, h * ht:(h + 1) * ht] * inv_m
            for k, row in enumerate((w / zs, w / zt, mt)):
                col[k, h * ht:(h + 1) * ht, :] = jnp.broadcast_to(row, (128, ht)).T
            return jnp.sum(w * kl, axis=1, keepdims=True)

        def backward(h):
            base = h * ht

            def vstep(b, _):
                v0 = pl.multiple_of(b * vb, vb)

                def rstep(i, _):
                    r = pl.ds(pl.multiple_of(base + i * RB, RB), RB)
                    cs, ct, m = col[0, r, :], col[1, r, :], col[2, r, :]
                    for q in range(vb // 128):
                        lanes = pl.ds(pl.multiple_of(v0 + q * 128, 128), 128)
                        th = tv[r, lanes]
                        ps = jnp.exp2(th * (CAP * LOG2E)) * cs
                        pt = jnp.exp2((t_v[r, lanes].astype(F32) - m) * LOG2E) * ct
                        dr[r, lanes] = ((ps - pt) * (1.0 - th * th)).astype(BF16)
                    return 0

                lax.fori_loop(0, ht // RB, rstep, 0)
                return 0

            lax.fori_loop(0, nvb, vstep, 0)
            dg[pl.ds(base, ht), :] = jnp.dot(dr[pl.ds(base, ht), :], e_v[...], preferred_element_type=F32)

        p1 = (z, y)
        p2 = (y, z)

        def tp1(h, q):
            return {'tp': q * side + y if h == 0 else z * side + q, 'dp': d}

        def tp2(h, q):
            return {'tp': z * side + q if h == 0 else q * side + y, 'dp': d}

        def hrows(h, q, o, n):
            return pl.ds(pl.multiple_of(h * ht + q * zc + o, 8), n)

        def rs_start(h):
            p = p1[h]
            nxt, prv, opp = lax.rem(p + 1, side), lax.rem(p + 3, side), lax.rem(p + 2, side)
            cps = {}
            for name, dirn, q, o, dev in (('a', 0, opp, 0, nxt), ('a', 1, opp, zh, prv), ('b', 0, nxt, zh, nxt), ('b', 1, prv, 0, prv)):
                slot = 'abc'.index(name) * 2 + dirn
                cps[name, dirn] = rcopy(dg.at[hrows(h, q, o, zh), :], zr.at[h, slot], ss_z.at[h, slot], rs_z.at[h, slot], tp1(h, dev))
            return cps

        def rs_mid(h, cps):
            p = p1[h]
            nxt, prv = lax.rem(p + 1, side), lax.rem(p + 3, side)
            for dirn, q, o, dev in ((0, nxt, 0, nxt), (1, prv, zh, prv)):
                cps['a', dirn].wait_recv()
                dg[hrows(h, q, o, zh), :] += zr[h, dirn]
            for dirn, q, o, dev in ((0, nxt, 0, nxt), (1, prv, zh, prv)):
                slot = 4 + dirn
                cps['c', dirn] = rcopy(dg.at[hrows(h, q, o, zh), :], zr.at[h, slot], ss_z.at[h, slot], rs_z.at[h, slot], tp1(h, dev))

        def rs_end(h, cps):
            p = p1[h]
            for name in 'bc':
                for dirn in range(2):
                    cps[name, dirn].wait_recv()
            dg[hrows(h, p, 0, zh), :] += zr[h, 4] + zr[h, 3]
            dg[hrows(h, p, zh, zh), :] += zr[h, 2] + zr[h, 5]
            out = []
            for k in range(1, side):
                q = lax.rem(p2[h] + k, side)
                out.append(rcopy(dg.at[hrows(h, p, q * oc, oc), :], p2r.at[h, k - 1], ss_p.at[h, k - 1], rs_p.at[h, k - 1], tp2(h, q)))
            return out

        def norm_back(h, cps):
            for cp in cps:
                cp.wait_recv()
            rows = hrows(h, p1[h], p2[h] * oc, oc)
            gv = dg[rows, :] + p2r[h, 0] + p2r[h, 1] + p2r[h, 2]
            xv = hid[rows, :].astype(F32)
            s = lax.rsqrt(jnp.mean(xv * xv, axis=-1, keepdims=True) + EPS)
            cv = gv * wp
            m = jnp.mean(cv * xv, axis=-1, keepdims=True)
            dhf[rows, :] = s * cv - xv * (s * s * s * m)
            out = []
            for k in range(1, side):
                out.append(rcopy(dhf.at[rows, :], dhf.at[rows, :], ss_g.at[h, k - 1], rs_g.at[h, k - 1], tp2(h, lax.rem(p2[h] + k, side))))
            return out, jnp.sum(gv * xv * s, axis=0, keepdims=True)

        def ag_start(h, cps1):
            for cp in cps1:
                cp.wait_recv()
            p = p1[h]
            nxt, prv = lax.rem(p + 1, side), lax.rem(p + 3, side)
            cps = {}
            for name, dirn, o, dev in (('a', 0, 0, nxt), ('a', 1, zh, prv), ('b', 0, zh, nxt), ('b', 1, 0, prv)):
                slot = 'abc'.index(name) * 2 + dirn
                rows = hrows(h, p, o, zh)
                cps[name, dirn] = rcopy(dhf.at[rows, :], dhf.at[rows, :], ss_h.at[h, slot], rs_h.at[h, slot], tp1(h, dev))
            return cps

        def ag_mid(h, cps):
            p = p1[h]
            nxt, prv = lax.rem(p + 1, side), lax.rem(p + 3, side)
            for dirn, q, o, dev in ((0, prv, 0, nxt), (1, nxt, zh, prv)):
                cps['a', dirn].wait_recv()
                slot = 4 + dirn
                rows = hrows(h, q, o, zh)
                cps['c', dirn] = rcopy(dhf.at[rows, :], dhf.at[rows, :], ss_h.at[h, slot], rs_h.at[h, slot], tp1(h, dev))

        def ag_end(h, cps):
            for name in 'bc':
                for dirn in range(2):
                    cps[name, dirn].wait_recv()
            rows = pl.ds(h * ht, ht)
            dh_out[rows, :] = dhf[rows, :].astype(BF16)

        xn, xp, xo = lax.rem(x + 1, side), lax.rem(x + 3, side), lax.rem(x + 2, side)

        def piece(q):
            return pl.ds(pl.multiple_of(c * half_d + q * cols, 8), cols)

        lo, hi = pl.ds(0, vh), pl.ds(vh, vh)

        def de_start(j):
            det[j] = jnp.dot(gt[...], dr[:, j * vc:(j + 1) * vc], preferred_element_type=F32)
            other = pl.ds(pl.multiple_of((1 - c) * half_d, 8), half_d)
            return rcopy(det.at[j, other, :], d2r.at[j], ss_d.at[j], rs_d.at[j], {'tp': t, 'dp': x * 2 + 1 - c})

        def xsend(j, slot, q, lanes, dev):
            return rcopy(det.at[j, piece(q), lanes], xr.at[j, slot], ss_x.at[j, slot], rs_x.at[j, slot], {'tp': t, 'dp': dev * 2 + c})

        def x_start(j, cp):
            cp.wait_recv()
            mine = pl.ds(pl.multiple_of(c * half_d, 8), half_d)
            det[j, mine, :] += d2r[j]
            return {('a', 0): xsend(j, 0, xo, lo, xn), ('a', 1): xsend(j, 1, xo, hi, xp),
                    ('b', 0): xsend(j, 2, xn, hi, xn), ('b', 1): xsend(j, 3, xp, lo, xp)}

        def x_mid(j, cps):
            cps['a', 0].wait_recv()
            det[j, piece(xn), lo] += xr[j, 0]
            cps['a', 1].wait_recv()
            det[j, piece(xp), hi] += xr[j, 1]
            cps['c', 0] = xsend(j, 4, xn, lo, xn)
            cps['c', 1] = xsend(j, 5, xp, hi, xp)

        def x_end(j, cps):
            for name in 'bc':
                for dirn in range(2):
                    cps[name, dirn].wait_recv()
            det_out[:, j * vc:j * vc + vh] = det[j, piece(x), lo] + xr[j, 4] + xr[j, 3]
            det_out[:, j * vc + vh:(j + 1) * vc] = det[j, piece(x), hi] + xr[j, 2] + xr[j, 5]

        st0 = forward(0)
        st1 = forward(1)
        for cp in mk_cp:
            cp.wait_recv()
        inv_m = 1.0 / jnp.sum(mk_r[:, 0, :], axis=0, keepdims=True)[:, 0:1]
        loss = combine(0, st0, inv_m)
        backward(0)
        rs0 = rs_start(0)
        loss = loss + combine(1, st1, inv_m)
        backward(1)
        rs1 = rs_start(1)
        rs_mid(0, rs0)
        dd = [None] * nv
        xs = [None] * nv
        dd[0] = de_start(0)
        dd[1] = de_start(1)
        xs[0] = x_start(0, dd[0])
        rs_mid(1, rs1)
        dd[2] = de_start(2)
        xs[1] = x_start(1, dd[1])
        dd[3] = de_start(3)
        xs[2] = x_start(2, dd[2])
        xs[3] = x_start(3, dd[3])
        ph0 = rs_end(0, rs0)
        x_mid(0, xs[0])
        ph1 = rs_end(1, rs1)
        ag0, dw0 = norm_back(0, ph0)
        x_mid(1, xs[1])
        ag1, dw1 = norm_back(1, ph1)
        dwv = dw0 + dw1
        zero = jnp.zeros((8, 128), F32)
        dwt_s[...] = zero
        for k in range(dpad // 128):
            n = min(128, dim - k * 128)
            dwt_s[k:k + 1, 0:n] = dwv[:, k * 128:k * 128 + n]
        dwt_r[t] = dwt_s[...]
        wt = [rcopy(dwt_s, dwt_r.at[t], ss_wt.at[k], rs_wt.at[k], {'tp': lax.rem(t + k, nt), 'dp': d}) for k in range(1, nt)]
        gh0 = ag_start(0, ag0)
        gh1 = ag_start(1, ag1)
        x_mid(2, xs[2])
        ag_mid(0, gh0)
        ag_mid(1, gh1)
        x_mid(3, xs[3])
        for cp in wt:
            cp.wait_recv()
        dws = jnp.sum(dwt_r[...], axis=0)
        rowi = lax.broadcasted_iota(jnp.int32, (8, 128), 0)
        dwd_s[...] = jnp.where(rowi == 7, jnp.broadcast_to(loss, (8, 128)), dws)
        dwd_r[d] = dwd_s[...]
        wd = [rcopy(dwd_s, dwd_r.at[d], ss_wd.at[k], rs_wd.at[k], {'tp': t, 'dp': lax.rem(d + k, nd)}) for k in range(1, nd)]
        ag_end(0, gh0)
        ag_end(1, gh1)
        for j in range(nv):
            x_end(j, xs[j])
        for cp in wd:
            cp.wait_recv()
        dwf = jnp.sum(dwd_r[...], axis=0)
        loss_out[...] = dwf[7:8, 0:1]
        for k in range(dpad // 128):
            n = min(128, dim - k * 128)
            dw_out[:, k * 128:k * 128 + n] = dwf[k:k + 1, 0:n]
        for cp in sends:
            cp.wait_send()

    sem = pltpu.SemaphoreType.DMA
    scratch = [
        pltpu.VMEM((voc, dim), BF16), pltpu.VMEM((tok, voc), BF16), pltpu.VMEM((tok, dim), BF16), pltpu.VMEM((dim, tok), BF16),
        pltpu.VMEM((tok, voc), F32), pltpu.VMEM((tok, voc), BF16), pltpu.VMEM((tok, dim), F32), pltpu.VMEM((tok, dim), F32),
        pltpu.VMEM((3, ht, 128), F32), pltpu.VMEM((ht, 128), F32), pltpu.VMEM((3, tok, 128), F32),
        pltpu.VMEM((2, 8, ht), F32), pltpu.VMEM((2, nt, 8, ht), F32), pltpu.VMEM((8, 128), F32), pltpu.VMEM((nd, 8, 128), F32),
        pltpu.VMEM((8, 128), F32), pltpu.VMEM((nt, 8, 128), F32), pltpu.VMEM((8, 128), F32), pltpu.VMEM((nd, 8, 128), F32),
        pltpu.VMEM((2, 6, zh, dim), F32), pltpu.VMEM((2, 3, oc, dim), F32),
        pltpu.VMEM((nv, dim, vc), F32), pltpu.VMEM((nv, half_d, vc), F32), pltpu.VMEM((nv, 6, cols, vh), F32),
        sem((3,)), sem((2, nt)), sem((2, nt)), sem((nd,)), sem((nd,)), sem((2, 6)), sem((2, 6)), sem((2, 3)), sem((2, 3)),
        sem((2, 3)), sem((2, 3)), sem((2, 6)), sem((2, 6)), sem((nv,)), sem((nv,)), sem((nv, 6)), sem((nv, 6)),
        sem((nt,)), sem((nt,)), sem((nd,)), sem((nd,)),
    ]
    vm = pl.BlockSpec(memory_space=pltpu.VMEM)
    anys = pl.BlockSpec(memory_space=pl.ANY)
    return pl.pallas_call(
        kernel,
        out_shape=(jax.ShapeDtypeStruct((1, 1), F32), jax.ShapeDtypeStruct((tok, dim), BF16),
                   jax.ShapeDtypeStruct((cols, voc), F32), jax.ShapeDtypeStruct((1, dim), F32)),
        in_specs=[vm, vm, vm, anys, anys],
        out_specs=(vm, vm, vm, vm),
        scratch_shapes=scratch,
        compiler_params=pltpu.CompilerParams(collective_id=0, has_side_effects=True, vmem_limit_bytes=67043328),
        name='head',
    )


def solution(mesh):
    nt, nd = mesh.shape['tp'], mesh.shape['dp']

    def device_fn(hid, norm_w, emb, teach, mask):
        tok, dim = hid.shape
        voc = emb.shape[0]
        call = build(tok, dim, voc, nt, nd)
        loss, dh, det, dw = call(hid, norm_w.reshape(1, dim), mask.reshape(1, tok), emb, teach)
        return loss.reshape(()), dh, det.T, dw.reshape(dim)

    return jax.shard_map(device_fn, mesh=mesh, in_specs=(P('dp', None), P(None), P('tp', None), P('dp', 'tp'), P('dp')),
                         out_specs=(P(), P('dp', None), P('tp', 'dp'), P(None)), check_vma=False)
```

```python
import jax
import jax.numpy as jnp
from jax import lax
from jax.experimental import pallas as pl
from jax.experimental.pallas import tpu as pltpu
from jax.sharding import PartitionSpec as P

CAP = 30.0
EPS = 1e-6
LOG2E = 1.4426950408889634
MESH = pl.DeviceIdType.MESH
F32 = jnp.float32
BF16 = jnp.bfloat16
SIDE = 4
NV = 4


def build(tok, dim, voc, nt, nd):
    ht = tok // 2
    zc = ht // SIDE
    fp = dim // SIDE
    cols = dim // nd
    vc = voc // NV
    vh = vc // 2
    vb = 256
    nvb = voc // vb
    half_d = dim // 2
    dpad = -(-dim // 128) * 128

    def kernel(hid, w_ref, mask_ref, e_hbm, t_hbm, loss_out, dh_out, det_out, dw_out,
               et, t_v, gb, gt, tv, tx, scr, wpc, dg, dhf, acc, mcol, col, st_s, st_r, mk_s, mk_r, dwt_s, dwt_r, dwd_s, dwd_r,
               zr, p2r, agb, d2r, xr,
               in_sem, ss_st, rs_st, ss_mk, rs_mk, ss_z, rs_z, ss_p, rs_p, ss_g, rs_g, ss_h, rs_h,
               ss_d, rs_d, ss_x, rs_x, ss_wt, rs_wt, ss_wd, rs_wd):
        t = lax.axis_index('tp')
        d = lax.axis_index('dp')
        z, y = t // SIDE, lax.rem(t, SIDE)
        x, c = d // 2, lax.rem(d, 2)
        sends = []

        def rcopy(src, dst, ssem, rsem, dev):
            cp = pltpu.make_async_remote_copy(src_ref=src, dst_ref=dst, send_sem=ssem, recv_sem=rsem,
                                              device_id=dev, device_id_type=MESH)
            cp.start()
            sends.append(cp)
            return cp

        class RingSum:
            def __init__(self, sl, buf, ss, rs, dev, p):
                self.sl, self.buf, self.ss, self.rs, self.dev = sl, buf, ss, rs, dev
                self.p, self.nxt, self.prv, self.opp = p, lax.rem(p + 1, SIDE), lax.rem(p + 3, SIDE), lax.rem(p + 2, SIDE)

            def send(self, k, q, half, to):
                return rcopy(self.sl(q, half), self.buf(k), self.ss.at[k], self.rs.at[k], self.dev(to))

            def start(self):
                self.a0 = self.send(0, self.opp, 0, self.nxt)
                self.a1 = self.send(1, self.opp, 1, self.prv)
                self.b0 = self.send(2, self.nxt, 1, self.nxt)
                self.b1 = self.send(3, self.prv, 0, self.prv)

            def mid(self):
                self.a0.wait_recv()
                part = self.sl(self.nxt, 0)
                part[...] += self.buf(0)[...]
                self.c0 = self.send(4, self.nxt, 0, self.nxt)
                self.a1.wait_recv()
                part = self.sl(self.prv, 1)
                part[...] += self.buf(1)[...]
                self.c1 = self.send(5, self.prv, 1, self.prv)

            def end(self):
                for cp in (self.b0, self.b1, self.c0, self.c1):
                    cp.wait_recv()
                return (self.sl(self.p, 0)[...] + self.buf(4)[...] + self.buf(3)[...],
                        self.sl(self.p, 1)[...] + self.buf(2)[...] + self.buf(5)[...])

        class RingGather:
            def __init__(self, sl, ss, rs, dev, p):
                self.sl, self.ss, self.rs, self.dev = sl, ss, rs, dev
                self.p, self.nxt, self.prv = p, lax.rem(p + 1, SIDE), lax.rem(p + 3, SIDE)

            def send(self, k, q, half, to):
                return rcopy(self.sl(q, half), self.sl(q, half), self.ss.at[k], self.rs.at[k], self.dev(to))

            def start(self):
                self.a0 = self.send(0, self.p, 0, self.nxt)
                self.a1 = self.send(1, self.p, 1, self.prv)
                self.b0 = self.send(2, self.p, 1, self.nxt)
                self.b1 = self.send(3, self.p, 0, self.prv)

            def mid(self):
                self.a0.wait_recv()
                self.c0 = self.send(4, self.prv, 0, self.nxt)
                self.a1.wait_recv()
                self.c1 = self.send(5, self.nxt, 1, self.prv)

            def end(self):
                for cp in (self.b0, self.b1, self.c0, self.c1):
                    cp.wait_recv()

        in_cp = [pltpu.make_async_copy(e_hbm, et, in_sem.at[0])]
        for h in range(2):
            rows = pl.ds(h * ht, ht)
            in_cp.append(pltpu.make_async_copy(t_hbm.at[rows, :], t_v.at[rows, :], in_sem.at[1 + h]))
        for cp in (in_cp[1], in_cp[0], in_cp[2]):
            cp.start()

        barrier = pltpu.get_barrier_semaphore()
        for k in range(1, nt):
            pl.semaphore_signal(barrier, inc=1, device_id={'tp': lax.rem(t + k, nt), 'dp': d}, device_id_type=MESH)
        for k in range(1, nd):
            pl.semaphore_signal(barrier, inc=1, device_id={'tp': t, 'dp': lax.rem(d + k, nd)}, device_id_type=MESH)

        def pad_f(a, axis):
            shape = list(a.shape)
            shape[axis] = dpad - dim
            return jnp.concatenate([a, jnp.zeros(shape, F32)], axis=axis) if dpad > dim else a

        wrow = pad_f(1.0 + w_ref[...].astype(F32).reshape(1, dim), 1)
        wpc[...] = jnp.broadcast_to(wrow, (128, dpad)).T[:dim, :]

        def norm_step(i, _):
            r0 = pl.multiple_of(i * 128, 128)
            xv = hid[:, pl.ds(r0, 128)].astype(F32)
            s = lax.rsqrt(jnp.mean(xv * xv, axis=0, keepdims=True) + EPS)
            g = xv * s * wpc[...]
            gb[pl.ds(r0, 128), :] = pad_f(g, 0).T[:, :dim].astype(BF16)
            gp = [g[(2 * xx + cc) * cols:(2 * xx + cc + 1) * cols, :] for cc in range(2) for xx in range(SIDE)]
            gt[:, pl.ds(r0, 128)] = jnp.concatenate(gp, axis=0).astype(BF16)
            return 0

        lax.fori_loop(0, tok // 128, norm_step, 0)

        maskf = mask_ref[...].astype(F32)
        mk_s[...] = jnp.broadcast_to(jnp.sum(maskf, axis=1, keepdims=True), (8, 128))
        mk_r[d] = mk_s[...]
        pl.semaphore_wait(barrier, nt + nd - 2)
        mk_cp = [rcopy(mk_s, mk_r.at[d], ss_mk.at[k], rs_mk.at[k], {'tp': t, 'dp': lax.rem(d + k, nd)}) for k in range(1, nd)]

        def forward(h):
            base = h * ht
            in_cp[1 + h].wait()

            def mx(i, _):
                r = pl.multiple_of(base + i * 64, 64)
                m = t_v[pl.ds(r, 64), 0:128]
                for q in range(1, voc // 128):
                    m = jnp.maximum(m, t_v[pl.ds(r, 64), q * 128:(q + 1) * 128])
                mm = jnp.max(m.astype(F32), axis=1, keepdims=True)
                mcol[h, pl.ds(pl.multiple_of(i * 64, 64), 64), :] = jnp.broadcast_to(mm, (64, 128))
                return 0

            lax.fori_loop(0, ht // 64, mx, 0)
            if h == 0:
                in_cp[0].wait()
            acc[...] = jnp.zeros_like(acc)

            def fdot(b, slot):
                v0 = pl.multiple_of(b * vb, vb)
                scr[slot] = jnp.dot(gb[base:base + ht, :], et[:, pl.ds(v0, vb)], preferred_element_type=F32)

            def elem(b, slot):
                for i in range(0, ht, 32):
                    r = slice(base + i, base + i + 32)
                    a = slice(i, i + 32)
                    m = mcol[h, a, :]
                    zs, zt, qs = acc[0, a, :], acc[1, a, :], acc[2, a, :]
                    for q in range(vb // 128):
                        lanes = pl.ds(pl.multiple_of(b * vb + q * 128, 128), 128)
                        th = jnp.tanh(scr[slot, a, q * 128:(q + 1) * 128] * (1.0 / CAP))
                        tv[r, lanes] = th
                        u = t_v[r, lanes].astype(F32) - m
                        ex = jnp.exp2(u * LOG2E)
                        tx[r, lanes] = ex
                        zs = zs + jnp.exp2(th * (CAP * LOG2E))
                        zt = zt + ex
                        qs = qs + ex * (u - CAP * th)
                    acc[0, a, :] = zs
                    acc[1, a, :] = zt
                    acc[2, a, :] = qs

            fdot(0, 0)

            def vstep(i, _):
                b = i * 2
                fdot(b + 1, 1)
                elem(b, 0)
                fdot(jnp.minimum(b + 2, nvb - 1), 0)
                elem(b + 1, 1)
                return 0

            lax.fori_loop(0, nvb // 2, vstep, 0)
            parts = [mcol[h].T[0:1, :]] + [jnp.sum(acc[k].T, axis=0, keepdims=True) for k in range(3)]
            st_s[h] = jnp.concatenate(parts + [jnp.zeros((4, ht), F32)], axis=0)
            st_r[h, t] = st_s[h]
            return [rcopy(st_s.at[h], st_r.at[h, t], ss_st.at[h, k], rs_st.at[h, k], {'tp': lax.rem(t + k, nt), 'dp': d})
                    for k in range(1, nt)]

        def combine(h, cps, inv_m):
            for cp in cps:
                cp.wait_recv()
            mts = st_r[h, :, 0, :]
            mt = jnp.max(mts, axis=0, keepdims=True)
            dm = jnp.maximum(mts - mt, -3e38)
            e = jnp.exp(dm)
            zte = st_r[h, :, 2, :] * e
            zt = jnp.sum(zte, axis=0, keepdims=True)
            zs = jnp.sum(st_r[h, :, 1, :], axis=0, keepdims=True)
            a = jnp.sum(st_r[h, :, 3, :] * e + zte * dm, axis=0, keepdims=True)
            kl = a / zt - jnp.log(zt) + jnp.log(zs)
            w = maskf[:, h * ht:(h + 1) * ht] * inv_m
            mine = jnp.exp(jnp.maximum(st_s[h, 0:1, :] - mt, -3e38))
            for k, row in enumerate((w / zs, w / zt * mine)):
                col[k, h * ht:(h + 1) * ht, :] = jnp.broadcast_to(row, (128, ht)).T
            return jnp.sum(w * kl, axis=1, keepdims=True)

        def dlogit(h):
            base = h * ht

            def rstep(i, _):
                r = pl.ds(pl.multiple_of(base + i * 16, 16), 16)
                cs, ct = col[0, r, :], col[1, r, :]
                for q in range(voc // 128):
                    lanes = slice(q * 128, (q + 1) * 128)
                    th = tv[r, lanes]
                    ps = jnp.exp2(th * (CAP * LOG2E)) * cs
                    t_v[r, lanes] = ((ps - tx[r, lanes] * ct) * (1.0 - th * th)).astype(BF16)
                return 0

            lax.fori_loop(0, ht // 16, rstep, 0)

        def dgrad(h):
            rows = slice(h * ht, (h + 1) * ht)
            dg[:, rows] = lax.dot_general(et[...], t_v[rows, :], (((1,), (1,)), ((), ())), preferred_element_type=F32)

        pos1, pos2 = (z, y), (y, z)

        def chunk(h, q):
            return pl.ds(pl.multiple_of(h * ht + q * zc, zc), zc)

        def frows(q, half):
            return pl.ds(pl.multiple_of(q * fp + half * (fp // 2), 8), fp // 2)

        def dev1(h):
            return lambda q: {'tp': q * SIDE + y if h == 0 else z * SIDE + q, 'dp': d}

        def dev2(h):
            return lambda q: {'tp': z * SIDE + q if h == 0 else q * SIDE + y, 'dp': d}

        def make(h):
            r1 = RingSum(lambda q, half: dg.at[half * half_d:(half + 1) * half_d, chunk(h, q)], lambda k: zr.at[h, k],
                         ss_z.at[h], rs_z.at[h], dev1(h), pos1[h])
            r2 = RingSum(lambda q, half: dg.at[frows(q, half), chunk(h, pos1[h])], lambda k: p2r.at[h, k],
                         ss_p.at[h], rs_p.at[h], dev2(h), pos2[h])
            g1 = RingGather(lambda q, half: agb.at[h, frows(q, half), :], ss_g.at[h], rs_g.at[h], dev2(h), pos2[h])
            g2 = RingGather(lambda q, half: dhf.at[half * half_d:(half + 1) * half_d, chunk(h, q)],
                            ss_h.at[h], rs_h.at[h], dev1(h), pos1[h])
            return r1, r2, g1, g2

        ring = (make(0), make(1))

        def rs_end(h):
            r1, r2 = ring[h][:2]
            lo_v, hi_v = r1.end()
            r1.sl(r1.p, 0)[...] = lo_v
            r1.sl(r1.p, 1)[...] = hi_v
            r2.start()

        def p2_end(h):
            r2, g1 = ring[h][1:3]
            lo_v, hi_v = r2.end()
            g1.sl(g1.p, 0)[...] = lo_v
            g1.sl(g1.p, 1)[...] = hi_v
            g1.start()

        def norm_back(h):
            g1, g2 = ring[h][2:]
            g1.end()
            ck = chunk(h, pos1[h])
            gv = agb[h]
            xv = hid[:, ck].astype(F32)
            s = lax.rsqrt(jnp.mean(xv * xv, axis=0, keepdims=True) + EPS)
            cv = gv * wpc[:, :zc]
            m = jnp.mean(cv * xv, axis=0, keepdims=True)
            dhf[:, ck] = s * cv - xv * (s * s * s * m)
            g2.start()
            return gv * xv * s

        def ag_end(h):
            ring[h][3].end()
            rows = slice(h * ht, (h + 1) * ht)
            dh_out[:, rows] = dhf[:, rows].astype(BF16)

        def de_start(j):
            tv[0:dim, j * vc:(j + 1) * vc] = jnp.dot(gt[...], t_v[:, j * vc:(j + 1) * vc], preferred_element_type=F32)
            other = pl.ds(pl.multiple_of((1 - c) * half_d, 8), half_d)
            return rcopy(tv.at[other, j * vc:(j + 1) * vc], d2r.at[j], ss_d.at[j], rs_d.at[j], {'tp': t, 'dp': x * 2 + 1 - c})

        def make_x(j):
            def sl(q, half):
                return tv.at[pl.ds(pl.multiple_of(c * half_d + q * cols, 8), cols), j * vc + half * vh:j * vc + (half + 1) * vh]

            return RingSum(sl, lambda k: xr.at[j, k], ss_x.at[j], rs_x.at[j], lambda q: {'tp': t, 'dp': q * 2 + c}, x)

        xring = [make_x(j) for j in range(NV)]

        def x_start(j, cp):
            cp.wait_recv()
            mine = pl.ds(pl.multiple_of(c * half_d, 8), half_d)
            tv[mine, j * vc:(j + 1) * vc] += d2r[j]
            xring[j].start()

        def x_end(j):
            lo_v, hi_v = xring[j].end()
            det_out[:, j * vc:j * vc + vh] = lo_v
            det_out[:, j * vc + vh:(j + 1) * vc] = hi_v

        st0 = forward(0)
        st1 = forward(1)
        for cp in mk_cp:
            cp.wait_recv()
        inv_m = 1.0 / jnp.sum(mk_r[:, 0, :], axis=0, keepdims=True)[:, 0:1]
        loss = combine(0, st0, inv_m)
        dlogit(0)
        dgrad(0)
        ring[0][0].start()
        loss = loss + combine(1, st1, inv_m)
        dlogit(1)
        dd = [None] * NV
        dd[0] = de_start(0)
        dgrad(1)
        ring[1][0].start()
        x_start(0, dd[0])
        dd[1] = de_start(1)
        ring[0][0].mid()
        dd[2] = de_start(2)
        x_start(1, dd[1])
        dd[3] = de_start(3)
        x_start(2, dd[2])
        ring[1][0].mid()
        x_start(3, dd[3])
        xring[0].mid()
        rs_end(0)
        xring[1].mid()
        rs_end(1)
        ring[0][1].mid()
        ring[1][1].mid()
        xring[2].mid()
        p2_end(0)
        p2_end(1)
        ring[0][2].mid()
        ring[1][2].mid()
        xring[3].mid()
        p0 = norm_back(0)
        p1 = norm_back(1)
        pw = jnp.where(y == 0, p0, 0.0) + jnp.where(z == 0, p1, 0.0)
        dwv = jnp.sum(pad_f(pw, 0).T, axis=0, keepdims=True)
        dwt_s[...] = jnp.zeros((8, 128), F32)
        for k in range(dpad // 128):
            dwt_s[k:k + 1, :] = dwv[:, k * 128:(k + 1) * 128]
        dwt_r[t] = dwt_s[...]
        wt = [rcopy(dwt_s, dwt_r.at[t], ss_wt.at[k], rs_wt.at[k], {'tp': lax.rem(t + k, nt), 'dp': d}) for k in range(1, nt)]
        ring[0][3].mid()
        ring[1][3].mid()
        x_end(0)
        for cp in wt:
            cp.wait_recv()
        dws = jnp.sum(dwt_r[...], axis=0)
        rowi = lax.broadcasted_iota(jnp.int32, (8, 128), 0)
        dwd_s[...] = jnp.where(rowi == 7, jnp.broadcast_to(loss, (8, 128)), dws)
        dwd_r[d] = dwd_s[...]
        wd = [rcopy(dwd_s, dwd_r.at[d], ss_wd.at[k], rs_wd.at[k], {'tp': t, 'dp': lax.rem(d + k, nd)}) for k in range(1, nd)]
        x_end(1)
        x_end(2)
        x_end(3)
        ag_end(0)
        ag_end(1)
        for cp in wd:
            cp.wait_recv()
        dwf = jnp.sum(dwd_r[...], axis=0)
        loss_out[...] = dwf[7:8, 0:1]
        for k in range(dpad // 128):
            n = min(128, dim - k * 128)
            dw_out[:, k * 128:k * 128 + n] = dwf[k:k + 1, 0:n]
        for cp in sends:
            cp.wait_send()

    sem = pltpu.SemaphoreType.DMA
    vmem = pltpu.VMEM
    scratch = [
        vmem((dim, voc), BF16), vmem((tok, voc), BF16), vmem((tok, dim), BF16), vmem((dim, tok), BF16),
        vmem((tok, voc), F32), vmem((tok, voc), F32), vmem((2, ht, vb), F32), vmem((dim, 128), F32),
        vmem((dim, tok), F32), vmem((dim, tok), F32),
        vmem((3, ht, 128), F32), vmem((2, ht, 128), F32), vmem((2, tok, 128), F32),
        vmem((2, 8, ht), F32), vmem((2, nt, 8, ht), F32), vmem((8, 128), F32), vmem((nd, 8, 128), F32),
        vmem((8, 128), F32), vmem((nt, 8, 128), F32), vmem((8, 128), F32), vmem((nd, 8, 128), F32),
        vmem((2, 6, half_d, zc), F32), vmem((2, 6, fp // 2, zc), F32), vmem((2, dim, zc), F32),
        vmem((NV, half_d, vc), F32), vmem((NV, 6, cols, vh), F32),
        sem((3,)), sem((2, nt)), sem((2, nt)), sem((nd,)), sem((nd,)), sem((2, 6)), sem((2, 6)), sem((2, 6)), sem((2, 6)),
        sem((2, 6)), sem((2, 6)), sem((2, 6)), sem((2, 6)), sem((NV,)), sem((NV,)), sem((NV, 6)), sem((NV, 6)),
        sem((nt,)), sem((nt,)), sem((nd,)), sem((nd,)),
    ]
    vm = pl.BlockSpec(memory_space=pltpu.VMEM)
    anys = pl.BlockSpec(memory_space=pl.ANY)
    return pl.pallas_call(
        kernel,
        out_shape=(jax.ShapeDtypeStruct((1, 1), F32), jax.ShapeDtypeStruct((dim, tok), BF16),
                   jax.ShapeDtypeStruct((cols, voc), F32), jax.ShapeDtypeStruct((1, dim), F32)),
        in_specs=[vm, vm, vm, anys, anys],
        out_specs=(vm, vm, vm, vm),
        scratch_shapes=scratch,
        compiler_params=pltpu.CompilerParams(collective_id=0, has_side_effects=True, vmem_limit_bytes=67043328),
        name='head',
    )


def solution(mesh):
    nt, nd = mesh.shape['tp'], mesh.shape['dp']

    def device_fn(hid, norm_w, emb, teach, mask):
        tok, dim = hid.shape
        call = build(tok, dim, emb.shape[0], nt, nd)
        loss, dh, det, dw = call(hid.T, norm_w, mask.reshape(1, tok), emb.T, teach)
        return loss.reshape(()), dh.T, det.T, dw.reshape(dim)

    return jax.shard_map(device_fn, mesh=mesh, in_specs=(P('dp', None), P(None), P('tp', None), P('dp', 'tp'), P('dp')),
                         out_specs=(P(), P('dp', None), P('tp', 'dp'), P(None)), check_vma=False)
```

```python
import jax
import jax.numpy as jnp
from jax import lax
from jax.experimental import pallas as pl
from jax.experimental.pallas import tpu as pltpu
from jax.sharding import PartitionSpec as P

CAP = 30.0
EPS = 1e-6
LOG2E = 1.4426950408889634
LN2 = 0.6931471805599453
MESH = pl.DeviceIdType.MESH
F32 = jnp.float32
BF16 = jnp.bfloat16
SIDE = 4
NV = 6


def build(tok, dim, voc, nt, nd):
    ht = tok // 2
    zc = ht // SIDE
    fp = dim // SIDE
    cols = dim // nd
    vc = voc // NV
    vh = vc // 2
    vb = min(512, voc // 2)
    nvb = voc // vb
    half_d = dim // 2
    dpad = -(-dim // 128) * 128

    def kernel(hid, w_ref, mask_ref, e_hbm, t_hbm, loss_out, dh_out, det_out, dw_out,
               et, t_v, gb, gt, tv, tx, scr, wpc, dg, dhf, acc, mcol, col, st_s, st_r, mk_s, mk_r, dwa_s, dwa_r, dwd_s, dwd_r, dhb, deb,
               zr, p2r, agb, d2r, xr,
               in_sem, ss_st, rs_st, ss_mk, rs_mk, ss_z, rs_z, ss_p, rs_p, ss_g, rs_g, ss_h, rs_h,
               ss_d, rs_d, ss_x, rs_x, ss_wa, rs_wa, ss_wd, rs_wd, out_sem):
        t = lax.axis_index('tp')
        d = lax.axis_index('dp')
        z, y = t // SIDE, lax.rem(t, SIDE)
        x, c = d // 2, lax.rem(d, 2)
        sends = []
        outs = []

        def rcopy(src, dst, ssem, rsem, dev):
            cp = pltpu.make_async_remote_copy(src_ref=src, dst_ref=dst, send_sem=ssem, recv_sem=rsem,
                                              device_id=dev, device_id_type=MESH)
            cp.start()
            sends.append(cp)
            return cp

        class RingSum:
            def __init__(self, sl, buf, ss, rs, dev, p):
                self.sl, self.buf, self.ss, self.rs, self.dev = sl, buf, ss, rs, dev
                self.p, self.nxt, self.prv, self.opp = p, lax.rem(p + 1, SIDE), lax.rem(p + 3, SIDE), lax.rem(p + 2, SIDE)

            def send(self, k, q, half, to):
                return rcopy(self.sl(q, half), self.buf(k), self.ss.at[k], self.rs.at[k], self.dev(to))

            def start(self):
                self.a0 = self.send(0, self.opp, 0, self.nxt)
                self.a1 = self.send(1, self.opp, 1, self.prv)
                self.b0 = self.send(2, self.nxt, 1, self.nxt)
                self.b1 = self.send(3, self.prv, 0, self.prv)

            def mid(self):
                self.a0.wait_recv()
                part = self.sl(self.nxt, 0)
                part[...] += self.buf(0)[...]
                self.c0 = self.send(4, self.nxt, 0, self.nxt)
                self.a1.wait_recv()
                part = self.sl(self.prv, 1)
                part[...] += self.buf(1)[...]
                self.c1 = self.send(5, self.prv, 1, self.prv)

            def end(self):
                for cp in (self.b0, self.b1, self.c0, self.c1):
                    cp.wait_recv()
                return (self.sl(self.p, 0)[...] + self.buf(4)[...] + self.buf(3)[...],
                        self.sl(self.p, 1)[...] + self.buf(2)[...] + self.buf(5)[...])

        class RingGather:
            def __init__(self, sl, ss, rs, dev, p):
                self.sl, self.ss, self.rs, self.dev = sl, ss, rs, dev
                self.p, self.nxt, self.prv = p, lax.rem(p + 1, SIDE), lax.rem(p + 3, SIDE)

            def send(self, k, q, half, to):
                return rcopy(self.sl(q, half), self.sl(q, half), self.ss.at[k], self.rs.at[k], self.dev(to))

            def start(self):
                self.a0 = self.send(0, self.p, 0, self.nxt)
                self.a1 = self.send(1, self.p, 1, self.prv)
                self.b0 = self.send(2, self.p, 1, self.nxt)
                self.b1 = self.send(3, self.p, 0, self.prv)

            def mid(self):
                self.a0.wait_recv()
                self.c0 = self.send(4, self.prv, 0, self.nxt)
                self.a1.wait_recv()
                self.c1 = self.send(5, self.nxt, 1, self.prv)

            def end(self):
                for cp in (self.b0, self.b1, self.c0, self.c1):
                    cp.wait_recv()

        in_cp = [pltpu.make_async_copy(e_hbm, et, in_sem.at[0])]
        for h in range(2):
            rows = pl.ds(h * ht, ht)
            in_cp.append(pltpu.make_async_copy(t_hbm.at[rows, :], t_v.at[rows, :], in_sem.at[1 + h]))
        for cp in (in_cp[1], in_cp[0], in_cp[2]):
            cp.start()

        barrier = pltpu.get_barrier_semaphore()
        for k in range(1, nt):
            pl.semaphore_signal(barrier, inc=1, device_id={'tp': lax.rem(t + k, nt), 'dp': d}, device_id_type=MESH)
        for k in range(1, nd):
            pl.semaphore_signal(barrier, inc=1, device_id={'tp': t, 'dp': lax.rem(d + k, nd)}, device_id_type=MESH)

        def pad_f(a, axis):
            shape = list(a.shape)
            shape[axis] = dpad - dim
            return jnp.concatenate([a, jnp.zeros(shape, F32)], axis=axis) if dpad > dim else a

        wrow = pad_f(1.0 + w_ref[...].astype(F32).reshape(1, dim), 1)
        wpc[...] = jnp.broadcast_to(wrow, (128, dpad)).T[:dim, :]

        def norm_step(i, _):
            r0 = pl.multiple_of(i * 128, 128)
            xv = hid[:, pl.ds(r0, 128)].astype(F32)
            s = lax.rsqrt(jnp.mean(xv * xv, axis=0, keepdims=True) + EPS)
            g = xv * s * wpc[...]
            gb[pl.ds(r0, 128), :] = pad_f(g, 0).T[:, :dim].astype(BF16)
            gp = [g[(2 * xx + cc) * cols:(2 * xx + cc + 1) * cols, :] for cc in range(2) for xx in range(SIDE)]
            gt[:, pl.ds(r0, 128)] = jnp.concatenate(gp, axis=0).astype(BF16)
            return 0

        lax.fori_loop(0, tok // 128, norm_step, 0)

        maskf = mask_ref[...].astype(F32)
        mk_s[...] = jnp.broadcast_to(jnp.sum(maskf, axis=1, keepdims=True), (8, 128))
        mk_r[d] = mk_s[...]

        def forward(h):
            base = h * ht
            in_cp[1 + h].wait()

            def mx(i, _):
                r = pl.multiple_of(base + i * 64, 64)
                m = t_v[pl.ds(r, 64), 0:128]
                for q in range(1, voc // 128):
                    m = jnp.maximum(m, t_v[pl.ds(r, 64), q * 128:(q + 1) * 128])
                mm = jnp.max(m.astype(F32), axis=1, keepdims=True)
                mcol[h, pl.ds(pl.multiple_of(i * 64, 64), 64), :] = jnp.broadcast_to(mm, (64, 128))
                return 0

            lax.fori_loop(0, ht // 64, mx, 0)
            if h == 0:
                in_cp[0].wait()
            acc[...] = jnp.zeros_like(acc)

            def fdot(b, slot):
                v0 = pl.multiple_of(b * vb, vb)
                scr[slot] = jnp.dot(gb[base:base + ht, :], et[:, pl.ds(v0, vb)], preferred_element_type=F32)

            def elem(b, slot):
                for i in range(0, ht, 16):
                    r = slice(base + i, base + i + 16)
                    a = slice(i, i + 16)
                    m = mcol[h, a, :]
                    zs, zt, qs = acc[0, a, :], acc[1, a, :], acc[2, a, :]
                    for q in range(vb // 128):
                        lanes = pl.ds(pl.multiple_of(b * vb + q * 128, 128), 128)
                        th = jnp.tanh(scr[slot, a, q * 128:(q + 1) * 128] * (1.0 / CAP))
                        tv[r, lanes] = th
                        u = (t_v[r, lanes].astype(F32) - m) * LOG2E
                        v = th * (CAP * LOG2E)
                        ex = jnp.exp2(u)
                        tx[r, lanes] = ex
                        zs = zs + jnp.exp2(v)
                        zt = zt + ex
                        qs = qs + ex * (u - v)
                    acc[0, a, :] = zs
                    acc[1, a, :] = zt
                    acc[2, a, :] = qs

            fdot(0, 0)

            def vstep(i, _):
                b = i * 2
                fdot(b + 1, 1)
                elem(b, 0)
                fdot(jnp.minimum(b + 2, nvb - 1), 0)
                elem(b + 1, 1)
                return 0

            lax.fori_loop(0, nvb // 2, vstep, 0)
            parts = [mcol[h].T[0:1, :]] + [jnp.sum(acc[k].T, axis=0, keepdims=True) for k in range(3)]
            st_s[h] = jnp.concatenate(parts + [jnp.zeros((4, ht), F32)], axis=0)
            st_r[h, t] = st_s[h]
            if h == 0:
                pl.semaphore_wait(barrier, nt + nd - 2)
            return [rcopy(st_s.at[h], st_r.at[h, t], ss_st.at[h, k], rs_st.at[h, k], {'tp': lax.rem(t + k, nt), 'dp': d})
                    for k in range(1, nt)]

        def combine(h, cps, inv_m):
            for cp in cps:
                cp.wait_recv()
            mts = st_r[h, :, 0, :]
            mt = jnp.max(mts, axis=0, keepdims=True)
            dm = jnp.maximum(mts - mt, -3e38)
            e = jnp.exp(dm)
            zte = st_r[h, :, 2, :] * e
            zt = jnp.sum(zte, axis=0, keepdims=True)
            zs = jnp.sum(st_r[h, :, 1, :], axis=0, keepdims=True)
            a = jnp.sum(st_r[h, :, 3, :] * LN2 * e + zte * dm, axis=0, keepdims=True)
            kl = a / zt - jnp.log(zt) + jnp.log(zs)
            w = maskf[:, h * ht:(h + 1) * ht] * inv_m
            mine = jnp.exp(jnp.maximum(st_s[h, 0:1, :] - mt, -3e38))
            for k, row in enumerate((w / zs, w / zt * mine)):
                col[k, h * ht:(h + 1) * ht, :] = jnp.broadcast_to(row, (128, ht)).T
            return jnp.sum(w * kl, axis=1, keepdims=True)

        def dlogit(h):
            base = h * ht

            def rstep(i, _):
                r = pl.ds(pl.multiple_of(base + i * 16, 16), 16)
                cs, ct = col[0, r, :], col[1, r, :]
                for q in range(voc // 128):
                    lanes = slice(q * 128, (q + 1) * 128)
                    th = tv[r, lanes]
                    ps = jnp.exp2(th * (CAP * LOG2E)) * cs
                    t_v[r, lanes] = ((ps - tx[r, lanes] * ct) * (1.0 - th * th)).astype(BF16)
                return 0

            lax.fori_loop(0, ht // 16, rstep, 0)

        def dgrad(h):
            rows = slice(h * ht, (h + 1) * ht)
            dg[:, rows] = lax.dot_general(et[...], t_v[rows, :], (((1,), (1,)), ((), ())), preferred_element_type=F32)

        pos1, pos2 = (z, y), (y, z)

        def chunk(h, q):
            return pl.ds(pl.multiple_of(h * ht + q * zc, zc), zc)

        def frows(q, half):
            return pl.ds(pl.multiple_of(q * fp + half * (fp // 2), 8), fp // 2)

        def dev1(h):
            return lambda q: {'tp': q * SIDE + y if h == 0 else z * SIDE + q, 'dp': d}

        def dev2(h):
            return lambda q: {'tp': z * SIDE + q if h == 0 else q * SIDE + y, 'dp': d}

        def make(h):
            r1 = RingSum(lambda q, half: dg.at[half * half_d:(half + 1) * half_d, chunk(h, q)], lambda k: zr.at[h, k],
                         ss_z.at[h], rs_z.at[h], dev1(h), pos1[h])
            r2 = RingSum(lambda q, half: dg.at[frows(q, half), chunk(h, pos1[h])], lambda k: p2r.at[h, k],
                         ss_p.at[h], rs_p.at[h], dev2(h), pos2[h])
            g1 = RingGather(lambda q, half: agb.at[h, frows(q, half), :], ss_g.at[h], rs_g.at[h], dev2(h), pos2[h])
            g2 = RingGather(lambda q, half: dhf.at[half * half_d:(half + 1) * half_d, chunk(h, q)],
                            ss_h.at[h], rs_h.at[h], dev1(h), pos1[h])
            return r1, r2, g1, g2

        ring = (make(0), make(1))

        def rs_end(h):
            r1, r2 = ring[h][:2]
            lo_v, hi_v = r1.end()
            r1.sl(r1.p, 0)[...] = lo_v
            r1.sl(r1.p, 1)[...] = hi_v
            r2.start()

        def p2_end(h):
            r2, g1 = ring[h][1:3]
            lo_v, hi_v = r2.end()
            g1.sl(g1.p, 0)[...] = lo_v
            g1.sl(g1.p, 1)[...] = hi_v
            g1.start()

        def norm_back(h):
            g1, g2 = ring[h][2:]
            g1.end()
            ck = chunk(h, pos1[h])
            gv = agb[h]
            xv = hid[:, ck].astype(F32)
            s = lax.rsqrt(jnp.mean(xv * xv, axis=0, keepdims=True) + EPS)
            cv = gv * wpc[:, :zc]
            m = jnp.mean(cv * xv, axis=0, keepdims=True)
            dwv = jnp.sum(pad_f(gv * xv * s, 0).T, axis=0, keepdims=True)
            for k in range(8):
                part = dwv[:, k * 128:(k + 1) * 128] if k < dpad // 128 else jnp.zeros((1, 128), F32)
                dwa_s[h, k:k + 1, :] = part
            dwa_r[h, pos1[h]] = dwa_s[h]
            cps = [rcopy(dwa_s.at[h], dwa_r.at[h, pos1[h]], ss_wa.at[h, k], rs_wa.at[h, k], dev1(h)(lax.rem(pos1[h] + k, SIDE)))
                   for k in range(1, SIDE)]
            dhf[:, ck] = s * cv - xv * (s * s * s * m)
            g2.start()
            return cps

        def ag_end(h):
            ring[h][3].end()
            rows = slice(h * ht, (h + 1) * ht)
            dhb[:, rows] = dhf[:, rows].astype(BF16)
            cp = pltpu.make_async_copy(dhb.at[:, rows], dh_out.at[:, rows], out_sem.at[h])
            cp.start()
            outs.append(cp)

        def de_start(j):
            tv[0:dim, j * vc:(j + 1) * vc] = jnp.dot(gt[...], t_v[:, j * vc:(j + 1) * vc], preferred_element_type=F32)
            other = pl.ds(pl.multiple_of((1 - c) * half_d, 8), half_d)
            return rcopy(tv.at[other, j * vc:(j + 1) * vc], d2r.at[j], ss_d.at[j], rs_d.at[j], {'tp': t, 'dp': x * 2 + 1 - c})

        def make_x(j):
            def sl(q, half):
                return tv.at[pl.ds(pl.multiple_of(c * half_d + q * cols, 8), cols), j * vc + half * vh:j * vc + (half + 1) * vh]

            return RingSum(sl, lambda k: xr.at[j, k], ss_x.at[j], rs_x.at[j], lambda q: {'tp': t, 'dp': q * 2 + c}, x)

        xring = [make_x(j) for j in range(NV)]

        def x_start(j, cp):
            cp.wait_recv()
            mine = pl.ds(pl.multiple_of(c * half_d, 8), half_d)
            tv[mine, j * vc:(j + 1) * vc] += d2r[j]
            xring[j].start()

        def x_end(j):
            lo_v, hi_v = xring[j].end()
            deb[:, j * vc:j * vc + vh] = lo_v
            deb[:, j * vc + vh:(j + 1) * vc] = hi_v
            cp = pltpu.make_async_copy(deb.at[:, j * vc:(j + 1) * vc], det_out.at[:, j * vc:(j + 1) * vc], out_sem.at[2 + j])
            cp.start()
            outs.append(cp)

        with jax.named_scope('s00_st0_forward_0_'):
            st0 = forward(0)
        with jax.named_scope('s01_mk_cp_rcopy_mk_s_mk_r_at_d_s'):
            mk_cp = [rcopy(mk_s, mk_r.at[d], ss_mk.at[k], rs_mk.at[k], {'tp': t, 'dp': lax.rem(d + k, nd)}) for k in range(1, nd)]
        with jax.named_scope('s02_st1_forward_1_'):
            st1 = forward(1)
        with jax.named_scope('s03_for_cp_in_mk_cp_'):
            for cp in mk_cp:
                cp.wait_recv()
        with jax.named_scope('s04_inv_m_1_0_jnp_sum_mk_r_0_axi'):
            inv_m = 1.0 / jnp.sum(mk_r[:, 0, :], axis=0, keepdims=True)[:, 0:1]
        with jax.named_scope('s05_loss_combine_0_st0_inv_m_'):
            loss = combine(0, st0, inv_m)
        with jax.named_scope('s06_dlogit_0_'):
            dlogit(0)
        with jax.named_scope('s07_dgrad_0_'):
            dgrad(0)
        with jax.named_scope('s08_ring_0_0_start_'):
            ring[0][0].start()
        with jax.named_scope('s09_loss_loss_combine_1_st1_inv_'):
            loss = loss + combine(1, st1, inv_m)
        with jax.named_scope('s10_dlogit_1_'):
            dlogit(1)
        with jax.named_scope('s11_dgrad_1_'):
            dgrad(1)
        with jax.named_scope('s12_ring_1_0_start_'):
            ring[1][0].start()
        with jax.named_scope('s13_dd_None_NV'):
            dd = [None] * NV
        with jax.named_scope('s14_dd_0_de_start_0_'):
            dd[0] = de_start(0)
        with jax.named_scope('s15_dd_1_de_start_1_'):
            dd[1] = de_start(1)
        with jax.named_scope('s16_ring_0_0_mid_'):
            ring[0][0].mid()
        with jax.named_scope('s17_dd_2_de_start_2_'):
            dd[2] = de_start(2)
        with jax.named_scope('s18_x_start_0_dd_0_'):
            x_start(0, dd[0])
        with jax.named_scope('s19_dd_3_de_start_3_'):
            dd[3] = de_start(3)
        with jax.named_scope('s20_x_start_1_dd_1_'):
            x_start(1, dd[1])
        with jax.named_scope('s21_dd_4_de_start_4_'):
            dd[4] = de_start(4)
        with jax.named_scope('s22_x_start_2_dd_2_'):
            x_start(2, dd[2])
        with jax.named_scope('s23_dd_5_de_start_5_'):
            dd[5] = de_start(5)
        with jax.named_scope('s24_x_start_3_dd_3_'):
            x_start(3, dd[3])
        with jax.named_scope('s25_x_start_4_dd_4_'):
            x_start(4, dd[4])
        with jax.named_scope('s26_ring_1_0_mid_'):
            ring[1][0].mid()
        with jax.named_scope('s27_x_start_5_dd_5_'):
            x_start(5, dd[5])
        with jax.named_scope('s28_xring_0_mid_'):
            xring[0].mid()
        with jax.named_scope('s29_rs_end_0_'):
            rs_end(0)
        with jax.named_scope('s30_xring_1_mid_'):
            xring[1].mid()
        with jax.named_scope('s31_ring_0_1_mid_'):
            ring[0][1].mid()
        with jax.named_scope('s32_rs_end_1_'):
            rs_end(1)
        with jax.named_scope('s33_xring_2_mid_'):
            xring[2].mid()
        with jax.named_scope('s34_p2_end_0_'):
            p2_end(0)
        with jax.named_scope('s35_ring_1_1_mid_'):
            ring[1][1].mid()
        with jax.named_scope('s36_xring_3_mid_'):
            xring[3].mid()
        with jax.named_scope('s37_ring_0_2_mid_'):
            ring[0][2].mid()
        with jax.named_scope('s38_p2_end_1_'):
            p2_end(1)
        with jax.named_scope('s39_xring_4_mid_'):
            xring[4].mid()
        with jax.named_scope('s40_wa0_norm_back_0_'):
            wa0 = norm_back(0)
        with jax.named_scope('s41_ring_1_2_mid_'):
            ring[1][2].mid()
        with jax.named_scope('s42_xring_5_mid_'):
            xring[5].mid()
        with jax.named_scope('s43_wa1_norm_back_1_'):
            wa1 = norm_back(1)
        with jax.named_scope('s44_ring_0_3_mid_'):
            ring[0][3].mid()
        with jax.named_scope('s45_for_cp_in_wa0_wa1_'):
            for cp in wa0 + wa1:
                cp.wait_recv()
        with jax.named_scope('s46_dws_jnp_sum_dwa_r_0_axis_0_j'):
            dws = jnp.sum(dwa_r[0], axis=0) + jnp.sum(dwa_r[1], axis=0)
        with jax.named_scope('s47_rowi_lax_broadcasted_iota_jn'):
            rowi = lax.broadcasted_iota(jnp.int32, (8, 128), 0)
        with jax.named_scope('s48_dwd_s_jnp_where_rowi_7_jnp_b'):
            dwd_s[...] = jnp.where(rowi == 7, jnp.broadcast_to(loss, (8, 128)), dws)
        with jax.named_scope('s49_dwd_r_d_dwd_s_'):
            dwd_r[d] = dwd_s[...]
        with jax.named_scope('s50_wd_rcopy_dwd_s_dwd_r_at_d_ss'):
            wd = [rcopy(dwd_s, dwd_r.at[d], ss_wd.at[k], rs_wd.at[k], {'tp': t, 'dp': lax.rem(d + k, nd)}) for k in range(1, nd)]
        with jax.named_scope('s51_x_end_0_'):
            x_end(0)
        with jax.named_scope('s52_x_end_1_'):
            x_end(1)
        with jax.named_scope('s53_ring_1_3_mid_'):
            ring[1][3].mid()
        with jax.named_scope('s54_x_end_2_'):
            x_end(2)
        with jax.named_scope('s55_x_end_3_'):
            x_end(3)
        with jax.named_scope('s56_x_end_4_'):
            x_end(4)
        with jax.named_scope('s57_ag_end_0_'):
            ag_end(0)
        with jax.named_scope('s58_x_end_5_'):
            x_end(5)
        with jax.named_scope('s59_for_cp_in_wd_'):
            for cp in wd:
                cp.wait_recv()
        with jax.named_scope('s60_dwf_jnp_sum_dwd_r_axis_0_'):
            dwf = jnp.sum(dwd_r[...], axis=0)
        with jax.named_scope('s61_loss_out_dwf_7_8_0_1_'):
            loss_out[...] = dwf[7:8, 0:1]
        with jax.named_scope('s62_for_k_in_range_dpad_128_'):
            for k in range(dpad // 128):
                n = min(128, dim - k * 128)
                dw_out[:, k * 128:k * 128 + n] = dwf[k:k + 1, 0:n]
        with jax.named_scope('s63_for_cp_in_sends_'):
            for cp in sends:
                cp.wait_send()
        with jax.named_scope('s64_ag_end_1_'):
            ag_end(1)
        with jax.named_scope('s65_for_cp_in_outs_'):
            for cp in outs:
                cp.wait()

    sem = pltpu.SemaphoreType.DMA
    vmem = pltpu.VMEM
    scratch = [
        vmem((dim, voc), BF16), vmem((tok, voc), BF16), vmem((tok, dim), BF16), vmem((dim, tok), BF16),
        vmem((tok, voc), F32), vmem((tok, voc), F32), vmem((2, ht, vb), F32), vmem((dim, 128), F32),
        vmem((dim, tok), F32), vmem((dim, tok), F32),
        vmem((3, ht, 128), F32), vmem((2, ht, 128), F32), vmem((2, tok, 128), F32),
        vmem((2, 8, ht), F32), vmem((2, nt, 8, ht), F32), vmem((8, 128), F32), vmem((nd, 8, 128), F32),
        vmem((2, 8, 128), F32), vmem((2, SIDE, 8, 128), F32), vmem((8, 128), F32), vmem((nd, 8, 128), F32),
        vmem((dim, tok), BF16), vmem((cols, voc), F32),
        vmem((2, 6, half_d, zc), F32), vmem((2, 6, fp // 2, zc), F32), vmem((2, dim, zc), F32),
        vmem((NV, half_d, vc), F32), vmem((NV, 6, cols, vh), F32),
        sem((3,)), sem((2, nt)), sem((2, nt)), sem((nd,)), sem((nd,)), sem((2, 6)), sem((2, 6)), sem((2, 6)), sem((2, 6)),
        sem((2, 6)), sem((2, 6)), sem((2, 6)), sem((2, 6)), sem((NV,)), sem((NV,)), sem((NV, 6)), sem((NV, 6)),
        sem((2, SIDE)), sem((2, SIDE)), sem((nd,)), sem((nd,)), sem((2 + NV,)),
    ]
    vm = pl.BlockSpec(memory_space=pltpu.VMEM)
    anys = pl.BlockSpec(memory_space=pl.ANY)
    return pl.pallas_call(
        kernel,
        out_shape=(jax.ShapeDtypeStruct((1, 1), F32), jax.ShapeDtypeStruct((dim, tok), BF16),
                   jax.ShapeDtypeStruct((cols, voc), F32), jax.ShapeDtypeStruct((1, dim), F32)),
        in_specs=[vm, vm, vm, anys, anys],
        out_specs=(vm, anys, anys, vm),
        scratch_shapes=scratch,
        compiler_params=pltpu.CompilerParams(collective_id=0, has_side_effects=True, vmem_limit_bytes=67043328),
        name='head',
    )


def finish(tok, dim, voc, cols):
    parts = 4
    rb, lb = tok // parts, voc // parts

    def kernel(dh, det, dw, dh_o, det_o, dw_o, hb, eb, sem_i, sem_o):
        views = []
        for i in range(parts):
            ls, es = pl.ds(i * rb, rb), pl.ds(i * lb, lb)
            views.append((dh.at[:, ls], hb.at[:, ls], dh_o.at[:, ls]))
            views.append((det.at[:, es], eb.at[:, es], det_o.at[:, es]))
        ins = [pltpu.make_async_copy(a, b, sem_i.at[k]) for k, (a, b, _) in enumerate(views)]
        outs = [pltpu.make_async_copy(b, o, sem_o.at[k]) for k, (_, b, o) in enumerate(views)]
        for cp in ins:
            cp.start()
        dw_o[...] = dw[...].reshape(dim)
        for ci, co in zip(ins, outs):
            ci.wait()
            co.start()
        for co in outs:
            co.wait()

    vm = pl.BlockSpec(memory_space=pltpu.VMEM)
    anys = pl.BlockSpec(memory_space=pl.ANY)
    return pl.pallas_call(
        kernel,
        out_shape=(jax.ShapeDtypeStruct((dim, tok), BF16), jax.ShapeDtypeStruct((cols, voc), F32), jax.ShapeDtypeStruct((dim,), F32)),
        in_specs=[anys, anys, vm],
        out_specs=(anys, anys, vm),
        scratch_shapes=[pltpu.VMEM((dim, tok), BF16), pltpu.VMEM((cols, voc), F32),
                        pltpu.SemaphoreType.DMA((2 * parts,)), pltpu.SemaphoreType.DMA((2 * parts,))],
        compiler_params=pltpu.CompilerParams(vmem_limit_bytes=67043328),
        name='finish',
    )


def solution(mesh):
    nt, nd = mesh.shape['tp'], mesh.shape['dp']

    def device_fn(hid, norm_w, emb, teach, mask):
        tok, dim = hid.shape
        call = build(tok, dim, emb.shape[0], nt, nd)
        loss, dh, det, dw = call(hid.T, norm_w, mask.reshape(1, tok), emb.T, teach)
        dh, det, dw = finish(tok, dim, emb.shape[0], dim // nd)(dh, det, dw)
        return loss.reshape(()), dh.T, det.T, dw

    return jax.shard_map(device_fn, mesh=mesh, in_specs=(P('dp', None), P(None), P('tp', None), P('dp', 'tp'), P('dp')),
                         out_specs=(P(), P('dp', None), P('tp', 'dp'), P(None)), check_vma=False)
```

```python
import jax
import jax.numpy as jnp
from jax import lax
from jax.experimental import pallas as pl
from jax.experimental.pallas import tpu as pltpu
from jax.sharding import PartitionSpec as P

CAP = 30.0
EPS = 1e-6
LOG2E = 1.4426950408889634
LN2 = 0.6931471805599453
MESH = pl.DeviceIdType.MESH
F32 = jnp.float32
BF16 = jnp.bfloat16
SIDE = 4
NV = 6


def build(tok, dim, voc, nt, nd):
    ht = tok // 2
    zc = ht // SIDE
    fp = dim // SIDE
    cols = dim // nd
    vc = voc // NV
    vh = vc // 2
    vb = min(512, voc // 2)
    nvb = voc // vb
    half_d = dim // 2
    dpad = -(-dim // 128) * 128

    def kernel(hid, w_ref, mask_ref, e_hbm, t_hbm, loss_out, dh_out, det_out, dw_out,
               et, t_v, gb, gt, tv, tx, scr, wpc, dg, dhf, acc, mcol, col, st_s, st_r, mk_s, mk_r, dwa_s, dwa_r, dwd_s, dwd_r,
               zr, p2r, agb, d2r, xr,
               in_sem, ss_st, rs_st, ss_mk, rs_mk, ss_z, rs_z, ss_p, rs_p, ss_g, rs_g, ss_h, rs_h,
               ss_d, rs_d, ss_x, rs_x, ss_wa, rs_wa, ss_wd, rs_wd, out_sem):
        t = lax.axis_index('tp')
        d = lax.axis_index('dp')
        z, y = t // SIDE, lax.rem(t, SIDE)
        x, c = d // 2, lax.rem(d, 2)
        sends = []
        outs = []

        def rcopy(src, dst, ssem, rsem, dev):
            cp = pltpu.make_async_remote_copy(src_ref=src, dst_ref=dst, send_sem=ssem, recv_sem=rsem,
                                              device_id=dev, device_id_type=MESH)
            cp.start()
            sends.append(cp)
            return cp

        class RingSum:
            def __init__(self, sl, buf, ss, rs, dev, p):
                self.sl, self.buf, self.ss, self.rs, self.dev = sl, buf, ss, rs, dev
                self.p, self.nxt, self.prv, self.opp = p, lax.rem(p + 1, SIDE), lax.rem(p + 3, SIDE), lax.rem(p + 2, SIDE)

            def send(self, k, q, half, to):
                return rcopy(self.sl(q, half), self.buf(k), self.ss.at[k], self.rs.at[k], self.dev(to))

            def start(self):
                self.a0 = self.send(0, self.opp, 0, self.nxt)
                self.a1 = self.send(1, self.opp, 1, self.prv)
                self.b0 = self.send(2, self.nxt, 1, self.nxt)
                self.b1 = self.send(3, self.prv, 0, self.prv)

            def mid(self):
                self.a0.wait_recv()
                part = self.sl(self.nxt, 0)
                part[...] += self.buf(0)[...]
                self.c0 = self.send(4, self.nxt, 0, self.nxt)
                self.a1.wait_recv()
                part = self.sl(self.prv, 1)
                part[...] += self.buf(1)[...]
                self.c1 = self.send(5, self.prv, 1, self.prv)

            def end(self):
                for cp in (self.b0, self.b1, self.c0, self.c1):
                    cp.wait_recv()
                return (self.sl(self.p, 0)[...] + self.buf(4)[...] + self.buf(3)[...],
                        self.sl(self.p, 1)[...] + self.buf(2)[...] + self.buf(5)[...])

        class RingGather:
            def __init__(self, sl, ss, rs, dev, p):
                self.sl, self.ss, self.rs, self.dev = sl, ss, rs, dev
                self.p, self.nxt, self.prv = p, lax.rem(p + 1, SIDE), lax.rem(p + 3, SIDE)

            def send(self, k, q, half, to):
                return rcopy(self.sl(q, half), self.sl(q, half), self.ss.at[k], self.rs.at[k], self.dev(to))

            def start(self):
                self.a0 = self.send(0, self.p, 0, self.nxt)
                self.a1 = self.send(1, self.p, 1, self.prv)
                self.b0 = self.send(2, self.p, 1, self.nxt)
                self.b1 = self.send(3, self.p, 0, self.prv)

            def mid(self):
                self.a0.wait_recv()
                self.c0 = self.send(4, self.prv, 0, self.nxt)
                self.a1.wait_recv()
                self.c1 = self.send(5, self.nxt, 1, self.prv)

            def end(self):
                for cp in (self.b0, self.b1, self.c0, self.c1):
                    cp.wait_recv()

        in_cp = [pltpu.make_async_copy(e_hbm, et, in_sem.at[0])]
        for h in range(2):
            rows = pl.ds(h * ht, ht)
            in_cp.append(pltpu.make_async_copy(t_hbm.at[rows, :], t_v.at[rows, :], in_sem.at[1 + h]))
        for cp in (in_cp[1], in_cp[0], in_cp[2]):
            cp.start()

        barrier = pltpu.get_barrier_semaphore()
        for k in range(1, nt):
            pl.semaphore_signal(barrier, inc=1, device_id={'tp': lax.rem(t + k, nt), 'dp': d}, device_id_type=MESH)
        for k in range(1, nd):
            pl.semaphore_signal(barrier, inc=1, device_id={'tp': t, 'dp': lax.rem(d + k, nd)}, device_id_type=MESH)

        def pad_f(a, axis):
            shape = list(a.shape)
            shape[axis] = dpad - dim
            return jnp.concatenate([a, jnp.zeros(shape, F32)], axis=axis) if dpad > dim else a

        wrow = pad_f(1.0 + w_ref[...].astype(F32).reshape(1, dim), 1)
        wpc[...] = jnp.broadcast_to(wrow, (128, dpad)).T[:dim, :]

        def norm_step(i, _):
            r0 = pl.multiple_of(i * 128, 128)
            xv = hid[:, pl.ds(r0, 128)].astype(F32)
            s = lax.rsqrt(jnp.mean(xv * xv, axis=0, keepdims=True) + EPS)
            g = xv * s * wpc[...]
            gb[pl.ds(r0, 128), :] = pad_f(g, 0).T[:, :dim].astype(BF16)
            gp = [g[(2 * xx + cc) * cols:(2 * xx + cc + 1) * cols, :] for cc in range(2) for xx in range(SIDE)]
            gt[:, pl.ds(r0, 128)] = jnp.concatenate(gp, axis=0).astype(BF16)
            return 0

        lax.fori_loop(0, tok // 128, norm_step, 0)

        maskf = mask_ref[...].astype(F32)
        mk_s[...] = jnp.broadcast_to(jnp.sum(maskf, axis=1, keepdims=True), (8, 128))
        mk_r[d] = mk_s[...]

        def forward(h):
            base = h * ht
            in_cp[1 + h].wait()

            def mx(i, _):
                r = pl.multiple_of(base + i * 64, 64)
                m = t_v[pl.ds(r, 64), 0:128]
                for q in range(1, voc // 128):
                    m = jnp.maximum(m, t_v[pl.ds(r, 64), q * 128:(q + 1) * 128])
                mm = jnp.max(m.astype(F32), axis=1, keepdims=True)
                mcol[h, pl.ds(pl.multiple_of(i * 64, 64), 64), :] = jnp.broadcast_to(mm, (64, 128))
                return 0

            lax.fori_loop(0, ht // 64, mx, 0)
            if h == 0:
                in_cp[0].wait()
            acc[...] = jnp.zeros_like(acc)

            def fdot(b, slot):
                v0 = pl.multiple_of(b * vb, vb)
                scr[slot] = jnp.dot(gb[base:base + ht, :], et[:, pl.ds(v0, vb)], preferred_element_type=F32)

            def elem(b, slot):
                for i in range(0, ht, 16):
                    r = slice(base + i, base + i + 16)
                    a = slice(i, i + 16)
                    m = mcol[h, a, :]
                    zs, zt, qs = acc[0, a, :], acc[1, a, :], acc[2, a, :]
                    for q in range(vb // 128):
                        lanes = pl.ds(pl.multiple_of(b * vb + q * 128, 128), 128)
                        th = jnp.tanh(scr[slot, a, q * 128:(q + 1) * 128] * (1.0 / CAP))
                        tv[r, lanes] = th
                        u = (t_v[r, lanes].astype(F32) - m) * LOG2E
                        v = th * (CAP * LOG2E)
                        ex = jnp.exp2(u)
                        tx[r, pl.ds(pl.multiple_of(b * vb + (q ^ 2) * 128, 128), 128)] = ex
                        zs = zs + jnp.exp2(v)
                        zt = zt + ex
                        qs = qs + ex * (u - v)
                    acc[0, a, :] = zs
                    acc[1, a, :] = zt
                    acc[2, a, :] = qs

            fdot(0, 0)

            def vstep(i, _):
                b = i * 2
                fdot(b + 1, 1)
                elem(b, 0)
                fdot(jnp.minimum(b + 2, nvb - 1), 0)
                elem(b + 1, 1)
                return 0

            lax.fori_loop(0, nvb // 2, vstep, 0)
            parts = [mcol[h].T[0:1, :]] + [jnp.sum(acc[k].T, axis=0, keepdims=True) for k in range(3)]
            st_s[h] = jnp.concatenate(parts + [jnp.zeros((4, ht), F32)], axis=0)
            st_r[h, t] = st_s[h]
            if h == 0:
                pl.semaphore_wait(barrier, nt + nd - 2)
            return [rcopy(st_s.at[h], st_r.at[h, t], ss_st.at[h, k], rs_st.at[h, k], {'tp': lax.rem(t + k, nt), 'dp': d})
                    for k in range(1, nt)]

        def combine(h, cps, inv_m):
            for cp in cps:
                cp.wait_recv()
            mts = st_r[h, :, 0, :]
            mt = jnp.max(mts, axis=0, keepdims=True)
            dm = jnp.maximum(mts - mt, -3e38)
            e = jnp.exp(dm)
            zte = st_r[h, :, 2, :] * e
            zt = jnp.sum(zte, axis=0, keepdims=True)
            zs = jnp.sum(st_r[h, :, 1, :], axis=0, keepdims=True)
            a = jnp.sum(st_r[h, :, 3, :] * LN2 * e + zte * dm, axis=0, keepdims=True)
            kl = a / zt - jnp.log(zt) + jnp.log(zs)
            w = maskf[:, h * ht:(h + 1) * ht] * inv_m
            mine = jnp.exp(jnp.maximum(st_s[h, 0:1, :] - mt, -3e38))
            for k, row in enumerate((w / zs, w / zt * mine)):
                col[k, h * ht:(h + 1) * ht, :] = jnp.broadcast_to(row, (128, ht)).T
            return jnp.sum(w * kl, axis=1, keepdims=True)

        def dlogit(h):
            base = h * ht

            def rstep(i, _):
                r = pl.ds(pl.multiple_of(base + i * 16, 16), 16)
                cs, ct = col[0, r, :], col[1, r, :]
                for q in range(voc // 128):
                    lanes = slice(q * 128, (q + 1) * 128)
                    th = tv[r, lanes]
                    ps = jnp.exp2(th * (CAP * LOG2E)) * cs
                    t_v[r, lanes] = ((ps - tx[r, (q ^ 2) * 128:(q ^ 2) * 128 + 128] * ct) * (1.0 - th * th)).astype(BF16)
                return 0

            lax.fori_loop(0, ht // 16, rstep, 0)

        def dgrad(h):
            rows = slice(h * ht, (h + 1) * ht)
            dg[:, rows] = lax.dot_general(et[...], t_v[rows, :], (((1,), (1,)), ((), ())), preferred_element_type=F32)

        pos1, pos2 = (z, y), (y, z)

        def chunk(h, q):
            return pl.ds(pl.multiple_of(h * ht + q * zc, zc), zc)

        def frows(q, half):
            return pl.ds(pl.multiple_of(q * fp + half * (fp // 2), 8), fp // 2)

        def dev1(h):
            return lambda q: {'tp': q * SIDE + y if h == 0 else z * SIDE + q, 'dp': d}

        def dev2(h):
            return lambda q: {'tp': z * SIDE + q if h == 0 else q * SIDE + y, 'dp': d}

        def make(h):
            r1 = RingSum(lambda q, half: dg.at[half * half_d:(half + 1) * half_d, chunk(h, q)], lambda k: zr.at[h, k],
                         ss_z.at[h], rs_z.at[h], dev1(h), pos1[h])
            r2 = RingSum(lambda q, half: dg.at[frows(q, half), chunk(h, pos1[h])], lambda k: p2r.at[h, k],
                         ss_p.at[h], rs_p.at[h], dev2(h), pos2[h])
            g1 = RingGather(lambda q, half: agb.at[h, frows(q, half), :], ss_g.at[h], rs_g.at[h], dev2(h), pos2[h])
            g2 = RingGather(lambda q, half: dhf.at[half * half_d:(half + 1) * half_d, chunk(h, q)],
                            ss_h.at[h], rs_h.at[h], dev1(h), pos1[h])
            return r1, r2, g1, g2

        ring = (make(0), make(1))

        def rs_end(h):
            r1, r2 = ring[h][:2]
            lo_v, hi_v = r1.end()
            r1.sl(r1.p, 0)[...] = lo_v
            r1.sl(r1.p, 1)[...] = hi_v
            r2.start()

        def p2_end(h):
            r2, g1 = ring[h][1:3]
            lo_v, hi_v = r2.end()
            g1.sl(g1.p, 0)[...] = lo_v
            g1.sl(g1.p, 1)[...] = hi_v
            g1.start()

        def norm_back(h):
            g1, g2 = ring[h][2:]
            g1.end()
            ck = chunk(h, pos1[h])
            gv = agb[h]
            xv = hid[:, ck].astype(F32)
            s = lax.rsqrt(jnp.mean(xv * xv, axis=0, keepdims=True) + EPS)
            cv = gv * wpc[:, :zc]
            m = jnp.mean(cv * xv, axis=0, keepdims=True)
            dwv = jnp.sum(pad_f(gv * xv * s, 0).T, axis=0, keepdims=True)
            for k in range(8):
                part = dwv[:, k * 128:(k + 1) * 128] if k < dpad // 128 else jnp.zeros((1, 128), F32)
                dwa_s[h, k:k + 1, :] = part
            dwa_r[h, pos1[h]] = dwa_s[h]
            cps = [rcopy(dwa_s.at[h], dwa_r.at[h, pos1[h]], ss_wa.at[h, k], rs_wa.at[h, k], dev1(h)(lax.rem(pos1[h] + k, SIDE)))
                   for k in range(1, SIDE)]
            dhf[:, ck] = s * cv - xv * (s * s * s * m)
            g2.start()
            return cps

        def ag_end(h):
            ring[h][3].end()
            rows = slice(h * ht, (h + 1) * ht)
            t_v[0:dim, rows] = dhf[:, rows].astype(BF16)
            cp = pltpu.make_async_copy(t_v.at[0:dim, rows], dh_out.at[:, rows], out_sem.at[h])
            cp.start()
            outs.append(cp)

        def de_start(j):
            tv[0:dim, j * vc:(j + 1) * vc] = jnp.dot(gt[...], t_v[:, j * vc:(j + 1) * vc], preferred_element_type=F32)
            other = pl.ds(pl.multiple_of((1 - c) * half_d, 8), half_d)
            return rcopy(tv.at[other, j * vc:(j + 1) * vc], d2r.at[j], ss_d.at[j], rs_d.at[j], {'tp': t, 'dp': x * 2 + 1 - c})

        def make_x(j):
            def sl(q, half):
                return tv.at[pl.ds(pl.multiple_of(c * half_d + q * cols, 8), cols), j * vc + half * vh:j * vc + (half + 1) * vh]

            return RingSum(sl, lambda k: xr.at[j, k], ss_x.at[j], rs_x.at[j], lambda q: {'tp': t, 'dp': q * 2 + c}, x)

        xring = [make_x(j) for j in range(NV)]

        def x_start(j, cp):
            cp.wait_recv()
            mine = pl.ds(pl.multiple_of(c * half_d, 8), half_d)
            tv[mine, j * vc:(j + 1) * vc] += d2r[j]
            xring[j].start()

        def x_end(j):
            lo_v, hi_v = xring[j].end()
            tx[0:cols, j * vc:j * vc + vh] = lo_v
            tx[0:cols, j * vc + vh:(j + 1) * vc] = hi_v
            cp = pltpu.make_async_copy(tx.at[0:cols, j * vc:(j + 1) * vc], det_out.at[:, j * vc:(j + 1) * vc], out_sem.at[2 + j])
            cp.start()
            outs.append(cp)

        with jax.named_scope('s00_st0_forward_0_'):
            st0 = forward(0)
        with jax.named_scope('s01_mk_cp_rcopy_mk_s_mk_r_at_d_s'):
            mk_cp = [rcopy(mk_s, mk_r.at[d], ss_mk.at[k], rs_mk.at[k], {'tp': t, 'dp': lax.rem(d + k, nd)}) for k in range(1, nd)]
        with jax.named_scope('s02_st1_forward_1_'):
            st1 = forward(1)
        with jax.named_scope('s03_for_cp_in_mk_cp_'):
            for cp in mk_cp:
                cp.wait_recv()
        with jax.named_scope('s04_inv_m_1_0_jnp_sum_mk_r_0_axi'):
            inv_m = 1.0 / jnp.sum(mk_r[:, 0, :], axis=0, keepdims=True)[:, 0:1]
        with jax.named_scope('s05_loss_combine_0_st0_inv_m_'):
            loss = combine(0, st0, inv_m)
        with jax.named_scope('s06_dlogit_0_'):
            dlogit(0)
        with jax.named_scope('s07_dgrad_0_'):
            dgrad(0)
        with jax.named_scope('s08_ring_0_0_start_'):
            ring[0][0].start()
        with jax.named_scope('s09_loss_loss_combine_1_st1_inv_'):
            loss = loss + combine(1, st1, inv_m)
        with jax.named_scope('s10_dlogit_1_'):
            dlogit(1)
        with jax.named_scope('s11_dgrad_1_'):
            dgrad(1)
        with jax.named_scope('s12_ring_1_0_start_'):
            ring[1][0].start()
        with jax.named_scope('s13_dd_None_NV'):
            dd = [None] * NV
        with jax.named_scope('s14_dd_0_de_start_0_'):
            dd[0] = de_start(0)
        with jax.named_scope('s15_dd_1_de_start_1_'):
            dd[1] = de_start(1)
        with jax.named_scope('s16_ring_0_0_mid_'):
            ring[0][0].mid()
        with jax.named_scope('s17_dd_2_de_start_2_'):
            dd[2] = de_start(2)
        with jax.named_scope('s18_x_start_0_dd_0_'):
            x_start(0, dd[0])
        with jax.named_scope('s19_dd_3_de_start_3_'):
            dd[3] = de_start(3)
        with jax.named_scope('s20_x_start_1_dd_1_'):
            x_start(1, dd[1])
        with jax.named_scope('s21_dd_4_de_start_4_'):
            dd[4] = de_start(4)
        with jax.named_scope('s22_x_start_2_dd_2_'):
            x_start(2, dd[2])
        with jax.named_scope('s23_dd_5_de_start_5_'):
            dd[5] = de_start(5)
        with jax.named_scope('s24_x_start_3_dd_3_'):
            x_start(3, dd[3])
        with jax.named_scope('s25_x_start_4_dd_4_'):
            x_start(4, dd[4])
        with jax.named_scope('s26_ring_1_0_mid_'):
            ring[1][0].mid()
        with jax.named_scope('s27_x_start_5_dd_5_'):
            x_start(5, dd[5])
        with jax.named_scope('s28_xring_0_mid_'):
            xring[0].mid()
        with jax.named_scope('s29_rs_end_0_'):
            rs_end(0)
        with jax.named_scope('s30_xring_1_mid_'):
            xring[1].mid()
        with jax.named_scope('s31_ring_0_1_mid_'):
            ring[0][1].mid()
        with jax.named_scope('s32_rs_end_1_'):
            rs_end(1)
        with jax.named_scope('s33_xring_2_mid_'):
            xring[2].mid()
        with jax.named_scope('s34_p2_end_0_'):
            p2_end(0)
        with jax.named_scope('s35_ring_1_1_mid_'):
            ring[1][1].mid()
        with jax.named_scope('s36_xring_3_mid_'):
            xring[3].mid()
        with jax.named_scope('s37_ring_0_2_mid_'):
            ring[0][2].mid()
        with jax.named_scope('s38_p2_end_1_'):
            p2_end(1)
        with jax.named_scope('s39_xring_4_mid_'):
            xring[4].mid()
        with jax.named_scope('s40_wa0_norm_back_0_'):
            wa0 = norm_back(0)
        with jax.named_scope('s41_ring_1_2_mid_'):
            ring[1][2].mid()
        with jax.named_scope('s42_xring_5_mid_'):
            xring[5].mid()
        with jax.named_scope('s43_wa1_norm_back_1_'):
            wa1 = norm_back(1)
        with jax.named_scope('s44_ring_0_3_mid_'):
            ring[0][3].mid()
        with jax.named_scope('s45_for_cp_in_wa0_wa1_'):
            for cp in wa0 + wa1:
                cp.wait_recv()
        with jax.named_scope('s46_dws_jnp_sum_dwa_r_0_axis_0_j'):
            dws = jnp.sum(dwa_r[0], axis=0) + jnp.sum(dwa_r[1], axis=0)
        with jax.named_scope('s47_rowi_lax_broadcasted_iota_jn'):
            rowi = lax.broadcasted_iota(jnp.int32, (8, 128), 0)
        with jax.named_scope('s48_dwd_s_jnp_where_rowi_7_jnp_b'):
            dwd_s[...] = jnp.where(rowi == 7, jnp.broadcast_to(loss, (8, 128)), dws)
        with jax.named_scope('s49_dwd_r_d_dwd_s_'):
            dwd_r[d] = dwd_s[...]
        with jax.named_scope('s50_wd_rcopy_dwd_s_dwd_r_at_d_ss'):
            wd = [rcopy(dwd_s, dwd_r.at[d], ss_wd.at[k], rs_wd.at[k], {'tp': t, 'dp': lax.rem(d + k, nd)}) for k in range(1, nd)]
        with jax.named_scope('s51_x_end_0_'):
            x_end(0)
        with jax.named_scope('s52_x_end_1_'):
            x_end(1)
        with jax.named_scope('s53_ring_1_3_mid_'):
            ring[1][3].mid()
        with jax.named_scope('s54_x_end_2_'):
            x_end(2)
        with jax.named_scope('s55_x_end_3_'):
            x_end(3)
        with jax.named_scope('s56_x_end_4_'):
            x_end(4)
        with jax.named_scope('s57_ag_end_0_'):
            ag_end(0)
        with jax.named_scope('s58_x_end_5_'):
            x_end(5)
        with jax.named_scope('s59_for_cp_in_wd_'):
            for cp in wd:
                cp.wait_recv()
        with jax.named_scope('s60_dwf_jnp_sum_dwd_r_axis_0_'):
            dwf = jnp.sum(dwd_r[...], axis=0)
        with jax.named_scope('s61_loss_out_dwf_7_8_0_1_'):
            loss_out[...] = dwf[7:8, 0:1]
        with jax.named_scope('s62_for_k_in_range_dpad_128_'):
            for k in range(dpad // 128):
                n = min(128, dim - k * 128)
                dw_out[:, k * 128:k * 128 + n] = dwf[k:k + 1, 0:n]
        with jax.named_scope('s63_for_cp_in_sends_'):
            for cp in sends:
                cp.wait_send()
        with jax.named_scope('s64_ag_end_1_'):
            ag_end(1)
        with jax.named_scope('s65_for_cp_in_outs_'):
            for cp in outs:
                cp.wait()

    sem = pltpu.SemaphoreType.DMA
    vmem = pltpu.VMEM
    scratch = [
        vmem((dim, voc), BF16), vmem((tok, voc), BF16), vmem((tok, dim), BF16), vmem((dim, tok), BF16),
        vmem((tok, voc), F32), vmem((tok, voc), F32), vmem((2, ht, vb), F32), vmem((dim, 128), F32),
        vmem((dim, tok), F32), vmem((dim, tok), F32),
        vmem((3, ht, 128), F32), vmem((2, ht, 128), F32), vmem((2, tok, 128), F32),
        vmem((2, 8, ht), F32), vmem((2, nt, 8, ht), F32), vmem((8, 128), F32), vmem((nd, 8, 128), F32),
        vmem((2, 8, 128), F32), vmem((2, SIDE, 8, 128), F32), vmem((8, 128), F32), vmem((nd, 8, 128), F32),
        vmem((2, 6, half_d, zc), F32), vmem((2, 6, fp // 2, zc), F32), vmem((2, dim, zc), F32),
        vmem((NV, half_d, vc), F32), vmem((NV, 6, cols, vh), F32),
        sem((3,)), sem((2, nt)), sem((2, nt)), sem((nd,)), sem((nd,)), sem((2, 6)), sem((2, 6)), sem((2, 6)), sem((2, 6)),
        sem((2, 6)), sem((2, 6)), sem((2, 6)), sem((2, 6)), sem((NV,)), sem((NV,)), sem((NV, 6)), sem((NV, 6)),
        sem((2, SIDE)), sem((2, SIDE)), sem((nd,)), sem((nd,)), sem((2 + NV,)),
    ]
    vm = pl.BlockSpec(memory_space=pltpu.VMEM)
    anys = pl.BlockSpec(memory_space=pl.ANY)
    return pl.pallas_call(
        kernel,
        out_shape=(jax.ShapeDtypeStruct((1, 1), F32), jax.ShapeDtypeStruct((dim, tok), BF16),
                   jax.ShapeDtypeStruct((cols, voc), F32), jax.ShapeDtypeStruct((1, dim), F32)),
        in_specs=[vm, vm, vm, anys, anys],
        out_specs=(vm, anys, anys, vm),
        scratch_shapes=scratch,
        compiler_params=pltpu.CompilerParams(collective_id=0, has_side_effects=True, vmem_limit_bytes=67043328),
        name='head',
    )


def finish(tok, dim, voc, cols):
    parts = 4
    rb, lb = tok // parts, voc // parts

    def kernel(dh, det, dw, dh_o, det_o, dw_o, hb, eb, sem_i, sem_o):
        views = []
        for i in range(parts):
            ls, es = pl.ds(i * rb, rb), pl.ds(i * lb, lb)
            views.append((dh.at[:, ls], hb.at[:, ls], dh_o.at[:, ls]))
            views.append((det.at[:, es], eb.at[:, es], det_o.at[:, es]))
        ins = [pltpu.make_async_copy(a, b, sem_i.at[k]) for k, (a, b, _) in enumerate(views)]
        outs = [pltpu.make_async_copy(b, o, sem_o.at[k]) for k, (_, b, o) in enumerate(views)]
        for cp in ins:
            cp.start()
        dw_o[...] = dw[...].reshape(dim)
        for ci, co in zip(ins, outs):
            ci.wait()
            co.start()
        for co in outs:
            co.wait()

    vm = pl.BlockSpec(memory_space=pltpu.VMEM)
    anys = pl.BlockSpec(memory_space=pl.ANY)
    return pl.pallas_call(
        kernel,
        out_shape=(jax.ShapeDtypeStruct((dim, tok), BF16), jax.ShapeDtypeStruct((cols, voc), F32), jax.ShapeDtypeStruct((dim,), F32)),
        in_specs=[anys, anys, vm],
        out_specs=(anys, anys, vm),
        scratch_shapes=[pltpu.VMEM((dim, tok), BF16), pltpu.VMEM((cols, voc), F32),
                        pltpu.SemaphoreType.DMA((2 * parts,)), pltpu.SemaphoreType.DMA((2 * parts,))],
        compiler_params=pltpu.CompilerParams(vmem_limit_bytes=67043328),
        name='finish',
    )


def solution(mesh):
    nt, nd = mesh.shape['tp'], mesh.shape['dp']

    def device_fn(hid, norm_w, emb, teach, mask):
        tok, dim = hid.shape
        call = build(tok, dim, emb.shape[0], nt, nd)
        loss, dh, det, dw = call(hid.T, norm_w, mask.reshape(1, tok), emb.T, teach)
        dh, det, dw = finish(tok, dim, emb.shape[0], dim // nd)(dh, det, dw)
        return loss.reshape(()), dh.T, det.T, dw

    return jax.shard_map(device_fn, mesh=mesh, in_specs=(P('dp', None), P(None), P('tp', None), P('dp', 'tp'), P('dp')),
                         out_specs=(P(), P('dp', None), P('tp', 'dp'), P(None)), check_vma=False)
```

```python
import jax
import jax.numpy as jnp
from jax import lax
from jax.experimental import pallas as pl
from jax.experimental.pallas import tpu as pltpu
from jax.sharding import PartitionSpec as P

CAP = 30.0
EPS = 1e-6
LOG2E = 1.4426950408889634
LN2 = 0.6931471805599453
MESH = pl.DeviceIdType.MESH
F32 = jnp.float32
BF16 = jnp.bfloat16
SIDE = 4
NV = 6


def build(tok, dim, voc, nt, nd):
    ht = tok // 2
    hh = ht // 2
    zc = ht // SIDE
    fp = dim // SIDE
    cols = dim // nd
    vc = voc // NV
    vh = vc // 2
    vb = min(512, voc // 2)
    nvb = voc // vb
    half_d = dim // 2
    dpad = -(-dim // 128) * 128

    def kernel(hid, w_ref, mask_ref, e_hbm, t_hbm, loss_out, dh_out, det_out, dw_out,
               et, t_v, gb, gt, tv, tx, scr, wpc, dg, dhf, acc, mcol, col, st_s, st_r, mk_s, mk_r, dwa_s, dwa_r, dwd_s, dwd_r,
               zr, p2r, agb, d2r, xr,
               in_sem, ss_st, rs_st, ss_mk, rs_mk, ss_z, rs_z, ss_p, rs_p, ss_g, rs_g, ss_h, rs_h,
               ss_d, rs_d, ss_x, rs_x, ss_wa, rs_wa, ss_wd, rs_wd, out_sem):
        t = lax.axis_index('tp')
        d = lax.axis_index('dp')
        z, y = t // SIDE, lax.rem(t, SIDE)
        x, c = d // 2, lax.rem(d, 2)
        sends = []
        outs = []

        def rcopy(src, dst, ssem, rsem, dev):
            cp = pltpu.make_async_remote_copy(src_ref=src, dst_ref=dst, send_sem=ssem, recv_sem=rsem,
                                              device_id=dev, device_id_type=MESH)
            cp.start()
            sends.append(cp)
            return cp

        class RingSum:
            def __init__(self, sl, buf, ss, rs, dev, p):
                self.sl, self.buf, self.ss, self.rs, self.dev = sl, buf, ss, rs, dev
                self.p, self.nxt, self.prv, self.opp = p, lax.rem(p + 1, SIDE), lax.rem(p + 3, SIDE), lax.rem(p + 2, SIDE)

            def send(self, k, q, half, to):
                return rcopy(self.sl(q, half), self.buf(k), self.ss.at[k], self.rs.at[k], self.dev(to))

            def start(self):
                self.a0 = self.send(0, self.opp, 0, self.nxt)
                self.a1 = self.send(1, self.opp, 1, self.prv)
                self.b0 = self.send(2, self.nxt, 1, self.nxt)
                self.b1 = self.send(3, self.prv, 0, self.prv)

            def mid(self):
                self.a0.wait_recv()
                part = self.sl(self.nxt, 0)
                part[...] += self.buf(0)[...]
                self.c0 = self.send(4, self.nxt, 0, self.nxt)
                self.a1.wait_recv()
                part = self.sl(self.prv, 1)
                part[...] += self.buf(1)[...]
                self.c1 = self.send(5, self.prv, 1, self.prv)

            def end(self):
                for cp in (self.b0, self.b1, self.c0, self.c1):
                    cp.wait_recv()
                return (self.sl(self.p, 0)[...] + self.buf(4)[...] + self.buf(3)[...],
                        self.sl(self.p, 1)[...] + self.buf(2)[...] + self.buf(5)[...])

        class RingGather:
            def __init__(self, sl, ss, rs, dev, p):
                self.sl, self.ss, self.rs, self.dev = sl, ss, rs, dev
                self.p, self.nxt, self.prv = p, lax.rem(p + 1, SIDE), lax.rem(p + 3, SIDE)

            def send(self, k, q, half, to):
                return rcopy(self.sl(q, half), self.sl(q, half), self.ss.at[k], self.rs.at[k], self.dev(to))

            def start(self):
                self.a0 = self.send(0, self.p, 0, self.nxt)
                self.a1 = self.send(1, self.p, 1, self.prv)
                self.b0 = self.send(2, self.p, 1, self.nxt)
                self.b1 = self.send(3, self.p, 0, self.prv)

            def mid(self):
                self.a0.wait_recv()
                self.c0 = self.send(4, self.prv, 0, self.nxt)
                self.a1.wait_recv()
                self.c1 = self.send(5, self.nxt, 1, self.prv)

            def end(self):
                for cp in (self.b0, self.b1, self.c0, self.c1):
                    cp.wait_recv()

        in_cp = [pltpu.make_async_copy(e_hbm, et, in_sem.at[0])]
        for h in range(2):
            rows = pl.ds(h * ht, ht)
            in_cp.append(pltpu.make_async_copy(t_hbm.at[rows, :], t_v.at[rows, :], in_sem.at[1 + h]))
        for cp in (in_cp[1], in_cp[0], in_cp[2]):
            cp.start()

        barrier = pltpu.get_barrier_semaphore()
        for k in range(1, nt):
            pl.semaphore_signal(barrier, inc=1, device_id={'tp': lax.rem(t + k, nt), 'dp': d}, device_id_type=MESH)
        for k in range(1, nd):
            pl.semaphore_signal(barrier, inc=1, device_id={'tp': t, 'dp': lax.rem(d + k, nd)}, device_id_type=MESH)

        def pad_f(a, axis):
            shape = list(a.shape)
            shape[axis] = dpad - dim
            return jnp.concatenate([a, jnp.zeros(shape, F32)], axis=axis) if dpad > dim else a

        wrow = pad_f(1.0 + w_ref[...].astype(F32).reshape(1, dim), 1)
        wpc[...] = jnp.broadcast_to(wrow, (128, dpad)).T[:dim, :]

        def norm_step(i, _):
            r0 = pl.multiple_of(i * 128, 128)
            xv = hid[:, pl.ds(r0, 128)].astype(F32)
            s = lax.rsqrt(jnp.mean(xv * xv, axis=0, keepdims=True) + EPS)
            g = xv * s * wpc[...]
            gb[pl.ds(r0, 128), :] = pad_f(g, 0).T[:, :dim].astype(BF16)
            gp = [g[(2 * xx + cc) * cols:(2 * xx + cc + 1) * cols, :] for cc in range(2) for xx in range(SIDE)]
            gt[:, pl.ds(r0, 128)] = jnp.concatenate(gp, axis=0).astype(BF16)
            return 0

        lax.fori_loop(0, tok // 128, norm_step, 0)

        maskf = mask_ref[...].astype(F32)
        mk_s[...] = jnp.broadcast_to(jnp.sum(maskf, axis=1, keepdims=True), (8, 128))
        mk_r[d] = mk_s[...]

        def forward(h):
            base = h * ht
            in_cp[1 + h].wait()

            def mx(i, _):
                r = pl.multiple_of(base + i * 64, 64)
                m = t_v[pl.ds(r, 64), 0:128]
                for q in range(1, voc // 128):
                    m = jnp.maximum(m, t_v[pl.ds(r, 64), q * 128:(q + 1) * 128])
                mm = jnp.max(m.astype(F32), axis=1, keepdims=True)
                mcol[h, pl.ds(pl.multiple_of(i * 64, 64), 64), :] = jnp.broadcast_to(mm, (64, 128))
                return 0

            lax.fori_loop(0, ht // 64, mx, 0)
            if h == 0:
                in_cp[0].wait()
            acc[...] = jnp.zeros_like(acc)

            def fdot(b, slot):
                v0 = pl.multiple_of(b * vb, vb)
                scr[slot] = jnp.dot(gb[base:base + ht, :], et[:, pl.ds(v0, vb)], preferred_element_type=F32)

            def elem(b, slot):
                for i in range(0, ht, 16):
                    r = slice(base + i, base + i + 16)
                    a = slice(i, i + 16)
                    m = mcol[h, a, :]
                    zs, zt, qs = acc[0, a, :], acc[1, a, :], acc[2, a, :]
                    for q in range(vb // 128):
                        lanes = pl.ds(pl.multiple_of(b * vb + q * 128, 128), 128)
                        th = jnp.tanh(scr[slot, a, q * 128:(q + 1) * 128] * (1.0 / CAP))
                        tv[r, lanes] = th
                        u = (t_v[r, lanes].astype(F32) - m) * LOG2E
                        v = th * (CAP * LOG2E)
                        ex = jnp.exp2(u)
                        tx[r, pl.ds(pl.multiple_of(b * vb + (q ^ 2) * 128, 128), 128)] = ex
                        zs = zs + jnp.exp2(v)
                        zt = zt + ex
                        qs = qs + ex * (u - v)
                    acc[0, a, :] = zs
                    acc[1, a, :] = zt
                    acc[2, a, :] = qs

            fdot(0, 0)

            def vstep(i, _):
                b = i * 2
                fdot(b + 1, 1)
                elem(b, 0)
                fdot(jnp.minimum(b + 2, nvb - 1), 0)
                elem(b + 1, 1)
                return 0

            lax.fori_loop(0, nvb // 2, vstep, 0)
            parts = [mcol[h].T[0:1, :]] + [jnp.sum(acc[k].T, axis=0, keepdims=True) for k in range(3)]
            st_s[h] = jnp.concatenate([p[:, i * hh:(i + 1) * hh] for p in parts for i in range(2)], axis=0)
            st_r[h, t] = st_s[h]
            if h == 0:
                pl.semaphore_wait(barrier, nt + nd - 2)
            return [rcopy(st_s.at[h], st_r.at[h, t], ss_st.at[h, k], rs_st.at[h, k], {'tp': lax.rem(t + k, nt), 'dp': d})
                    for k in range(1, nt)]

        def combine(h, cps, inv_m):
            for cp in cps:
                cp.wait_recv()
            def stat(k):
                return jnp.concatenate([st_r[h, :, 2 * k, :], st_r[h, :, 2 * k + 1, :]], axis=1)

            mts = stat(0)
            mt = jnp.max(mts, axis=0, keepdims=True)
            dm = jnp.maximum(mts - mt, -3e38)
            e = jnp.exp(dm)
            zte = stat(2) * e
            zt = jnp.sum(zte, axis=0, keepdims=True)
            zs = jnp.sum(stat(1), axis=0, keepdims=True)
            a = jnp.sum(stat(3) * LN2 * e + zte * dm, axis=0, keepdims=True)
            kl = a / zt - jnp.log(zt) + jnp.log(zs)
            w = maskf[:, h * ht:(h + 1) * ht] * inv_m
            own = jnp.concatenate([st_s[h, 0:1, :], st_s[h, 1:2, :]], axis=1)
            mine = jnp.exp(jnp.maximum(own - mt, -3e38))
            for k, row in enumerate((w / zs, w / zt * mine)):
                col[k, h * ht:(h + 1) * ht, :] = jnp.broadcast_to(row, (128, ht)).T
            return jnp.sum(w * kl, axis=1, keepdims=True)

        def dlogit(h):
            base = h * ht

            def rstep(i, _):
                r = pl.ds(pl.multiple_of(base + i * 16, 16), 16)
                cs, ct = col[0, r, :], col[1, r, :]
                for q in range(voc // 128):
                    lanes = slice(q * 128, (q + 1) * 128)
                    th = tv[r, lanes]
                    ps = jnp.exp2(th * (CAP * LOG2E)) * cs
                    t_v[r, lanes] = ((ps - tx[r, (q ^ 2) * 128:(q ^ 2) * 128 + 128] * ct) * (1.0 - th * th)).astype(BF16)
                return 0

            lax.fori_loop(0, ht // 16, rstep, 0)

        def dgrad(h):
            rows = slice(h * ht, (h + 1) * ht)
            dg[:, rows] = lax.dot_general(et[...], t_v[rows, :], (((1,), (1,)), ((), ())), preferred_element_type=F32)

        pos1, pos2 = (z, y), (y, z)

        def chunk(h, q):
            return pl.ds(pl.multiple_of(h * ht + q * zc, zc), zc)

        def frows(q, half):
            return pl.ds(pl.multiple_of(q * fp + half * (fp // 2), 8), fp // 2)

        def dev1(h):
            return lambda q: {'tp': q * SIDE + y if h == 0 else z * SIDE + q, 'dp': d}

        def dev2(h):
            return lambda q: {'tp': z * SIDE + q if h == 0 else q * SIDE + y, 'dp': d}

        def make(h):
            r1 = RingSum(lambda q, half: dg.at[half * half_d:(half + 1) * half_d, chunk(h, q)], lambda k: zr.at[h, k],
                         ss_z.at[h], rs_z.at[h], dev1(h), pos1[h])
            r2 = RingSum(lambda q, half: dg.at[frows(q, half), chunk(h, pos1[h])], lambda k: p2r.at[h, k],
                         ss_p.at[h], rs_p.at[h], dev2(h), pos2[h])
            g1 = RingGather(lambda q, half: agb.at[h, frows(q, half), :], ss_g.at[h], rs_g.at[h], dev2(h), pos2[h])
            g2 = RingGather(lambda q, half: dhf.at[half * half_d:(half + 1) * half_d, chunk(h, q)],
                            ss_h.at[h], rs_h.at[h], dev1(h), pos1[h])
            return r1, r2, g1, g2

        ring = (make(0), make(1))

        def rs_end(h):
            r1, r2 = ring[h][:2]
            lo_v, hi_v = r1.end()
            r1.sl(r1.p, 0)[...] = lo_v
            r1.sl(r1.p, 1)[...] = hi_v
            r2.start()

        def p2_end(h):
            r2, g1 = ring[h][1:3]
            lo_v, hi_v = r2.end()
            g1.sl(g1.p, 0)[...] = lo_v
            g1.sl(g1.p, 1)[...] = hi_v
            g1.start()

        def norm_back(h):
            g1, g2 = ring[h][2:]
            g1.end()
            ck = chunk(h, pos1[h])
            gv = agb[h]
            xv = hid[:, ck].astype(F32)
            s = lax.rsqrt(jnp.mean(xv * xv, axis=0, keepdims=True) + EPS)
            cv = gv * wpc[:, :zc]
            m = jnp.mean(cv * xv, axis=0, keepdims=True)
            dwv = jnp.sum(pad_f(gv * xv * s, 0).T, axis=0, keepdims=True)
            for k in range(8):
                part = dwv[:, k * 128:(k + 1) * 128] if k < dpad // 128 else jnp.zeros((1, 128), F32)
                dwa_s[h, k:k + 1, :] = part
            dwa_r[h, pos1[h]] = dwa_s[h]
            cps = [rcopy(dwa_s.at[h], dwa_r.at[h, pos1[h]], ss_wa.at[h, k], rs_wa.at[h, k], dev1(h)(lax.rem(pos1[h] + k, SIDE)))
                   for k in range(1, SIDE)]
            dhf[:, ck] = s * cv - xv * (s * s * s * m)
            return cps

        def ag_end(h):
            ring[h][3].end()
            rows = slice(h * ht, (h + 1) * ht)
            t_v[0:dim, rows] = dhf[:, rows].astype(BF16)
            cp = pltpu.make_async_copy(t_v.at[0:dim, rows], dh_out.at[:, rows], out_sem.at[h])
            cp.start()
            outs.append(cp)

        def de_start(j):
            tv[0:dim, j * vc:(j + 1) * vc] = jnp.dot(gt[...], t_v[:, j * vc:(j + 1) * vc], preferred_element_type=F32)
            other = pl.ds(pl.multiple_of((1 - c) * half_d, 8), half_d)
            return rcopy(tv.at[other, j * vc:(j + 1) * vc], d2r.at[j], ss_d.at[j], rs_d.at[j], {'tp': t, 'dp': x * 2 + 1 - c})

        def make_x(j):
            def sl(q, half):
                return tv.at[pl.ds(pl.multiple_of(c * half_d + q * cols, 8), cols), j * vc + half * vh:j * vc + (half + 1) * vh]

            return RingSum(sl, lambda k: xr.at[j, k], ss_x.at[j], rs_x.at[j], lambda q: {'tp': t, 'dp': q * 2 + c}, x)

        xring = [make_x(j) for j in range(NV)]

        def x_start(j, cp):
            cp.wait_recv()
            mine = pl.ds(pl.multiple_of(c * half_d, 8), half_d)
            tv[mine, j * vc:(j + 1) * vc] += d2r[j]
            xring[j].start()

        def x_end(j):
            lo_v, hi_v = xring[j].end()
            tx[0:cols, j * vc:j * vc + vh] = lo_v
            tx[0:cols, j * vc + vh:(j + 1) * vc] = hi_v
            cp = pltpu.make_async_copy(tx.at[0:cols, j * vc:(j + 1) * vc], det_out.at[:, j * vc:(j + 1) * vc], out_sem.at[2 + j])
            cp.start()
            outs.append(cp)

        with jax.named_scope('s00_st0_forward_0_'):
            st0 = forward(0)
        with jax.named_scope('s01_mk_cp_rcopy_mk_s_mk_r_at_d_s'):
            mk_cp = [rcopy(mk_s, mk_r.at[d], ss_mk.at[k], rs_mk.at[k], {'tp': t, 'dp': lax.rem(d + k, nd)}) for k in range(1, nd)]
        with jax.named_scope('s02_st1_forward_1_'):
            st1 = forward(1)
        with jax.named_scope('s03_for_cp_in_mk_cp_'):
            for cp in mk_cp:
                cp.wait_recv()
        with jax.named_scope('s04_inv_m_1_0_jnp_sum_mk_r_0_axi'):
            inv_m = 1.0 / jnp.sum(mk_r[:, 0, :], axis=0, keepdims=True)[:, 0:1]
        with jax.named_scope('s05_loss_combine_0_st0_inv_m_'):
            loss = combine(0, st0, inv_m)
        with jax.named_scope('s06_dlogit_0_'):
            dlogit(0)
        with jax.named_scope('s07_dgrad_0_'):
            dgrad(0)
        with jax.named_scope('s08_ring_0_0_start_'):
            ring[0][0].start()
        with jax.named_scope('s09_loss_loss_combine_1_st1_inv_'):
            loss = loss + combine(1, st1, inv_m)
        with jax.named_scope('s10_dlogit_1_'):
            dlogit(1)
        with jax.named_scope('s11_dgrad_1_'):
            dgrad(1)
        with jax.named_scope('s12_ring_1_0_start_'):
            ring[1][0].start()
        with jax.named_scope('s13_dd_None_NV'):
            dd = [None] * NV
        with jax.named_scope('s14_dd_0_de_start_0_'):
            dd[0] = de_start(0)
        with jax.named_scope('s15_dd_1_de_start_1_'):
            dd[1] = de_start(1)
        with jax.named_scope('s16_ring_0_0_mid_'):
            ring[0][0].mid()
        with jax.named_scope('s17_dd_2_de_start_2_'):
            dd[2] = de_start(2)
        with jax.named_scope('s18_x_start_0_dd_0_'):
            x_start(0, dd[0])
        with jax.named_scope('s19_dd_3_de_start_3_'):
            dd[3] = de_start(3)
        with jax.named_scope('s20_x_start_1_dd_1_'):
            x_start(1, dd[1])
        with jax.named_scope('s21_dd_4_de_start_4_'):
            dd[4] = de_start(4)
        with jax.named_scope('s22_x_start_2_dd_2_'):
            x_start(2, dd[2])
        with jax.named_scope('s23_dd_5_de_start_5_'):
            dd[5] = de_start(5)
        with jax.named_scope('s24_x_start_3_dd_3_'):
            x_start(3, dd[3])
        with jax.named_scope('s25_x_start_4_dd_4_'):
            x_start(4, dd[4])
        with jax.named_scope('s26_ring_1_0_mid_'):
            ring[1][0].mid()
        with jax.named_scope('s27_x_start_5_dd_5_'):
            x_start(5, dd[5])
        with jax.named_scope('s28_xring_0_mid_'):
            xring[0].mid()
        with jax.named_scope('s29_rs_end_0_'):
            rs_end(0)
        with jax.named_scope('s30_xring_1_mid_'):
            xring[1].mid()
        with jax.named_scope('s31_ring_0_1_mid_'):
            ring[0][1].mid()
        with jax.named_scope('s32_rs_end_1_'):
            rs_end(1)
        with jax.named_scope('s33_xring_2_mid_'):
            xring[2].mid()
        with jax.named_scope('s34_p2_end_0_'):
            p2_end(0)
        with jax.named_scope('s35_ring_1_1_mid_'):
            ring[1][1].mid()
        with jax.named_scope('s36_xring_3_mid_'):
            xring[3].mid()
        with jax.named_scope('s37_ring_0_2_mid_'):
            ring[0][2].mid()
        with jax.named_scope('s38_p2_end_1_'):
            p2_end(1)
        with jax.named_scope('s39_xring_4_mid_'):
            xring[4].mid()
        with jax.named_scope('s40_wa0_norm_back_0_'):
            wa0 = norm_back(0)
        with jax.named_scope('s41_ring_1_2_mid_'):
            ring[1][2].mid()
        with jax.named_scope('s42_ring_0_3_start_'):
            ring[0][3].start()
        with jax.named_scope('s43_xring_5_mid_'):
            xring[5].mid()
        with jax.named_scope('s44_wa1_norm_back_1_'):
            wa1 = norm_back(1)
        with jax.named_scope('s45_ring_1_3_start_'):
            ring[1][3].start()
        with jax.named_scope('s46_ring_0_3_mid_'):
            ring[0][3].mid()
        with jax.named_scope('s47_for_cp_in_wa0_wa1_'):
            for cp in wa0 + wa1:
                cp.wait_recv()
        with jax.named_scope('s48_dws_jnp_sum_dwa_r_0_axis_0_j'):
            dws = jnp.sum(dwa_r[0], axis=0) + jnp.sum(dwa_r[1], axis=0)
        with jax.named_scope('s49_rowi_lax_broadcasted_iota_jn'):
            rowi = lax.broadcasted_iota(jnp.int32, (8, 128), 0)
        with jax.named_scope('s50_dwd_s_jnp_where_rowi_7_jnp_b'):
            dwd_s[...] = jnp.where(rowi == 7, jnp.broadcast_to(loss, (8, 128)), dws)
        with jax.named_scope('s51_dwd_r_d_dwd_s_'):
            dwd_r[d] = dwd_s[...]
        with jax.named_scope('s52_wd_rcopy_dwd_s_dwd_r_at_d_ss'):
            wd = [rcopy(dwd_s, dwd_r.at[d], ss_wd.at[k], rs_wd.at[k], {'tp': t, 'dp': lax.rem(d + k, nd)}) for k in range(1, nd)]
        with jax.named_scope('s53_x_end_0_'):
            x_end(0)
        with jax.named_scope('s54_ring_1_3_mid_'):
            ring[1][3].mid()
        with jax.named_scope('s55_x_end_1_'):
            x_end(1)
        with jax.named_scope('s56_x_end_2_'):
            x_end(2)
        with jax.named_scope('s57_x_end_3_'):
            x_end(3)
        with jax.named_scope('s58_ag_end_0_'):
            ag_end(0)
        with jax.named_scope('s59_x_end_4_'):
            x_end(4)
        with jax.named_scope('s60_x_end_5_'):
            x_end(5)
        with jax.named_scope('s61_for_cp_in_wd_'):
            for cp in wd:
                cp.wait_recv()
        with jax.named_scope('s62_dwf_jnp_sum_dwd_r_axis_0_'):
            dwf = jnp.sum(dwd_r[...], axis=0)
        with jax.named_scope('s63_loss_out_dwf_7_8_0_1_'):
            loss_out[...] = dwf[7:8, 0:1]
        with jax.named_scope('s64_for_k_in_range_dpad_128_'):
            for k in range(dpad // 128):
                n = min(128, dim - k * 128)
                dw_out[:, k * 128:k * 128 + n] = dwf[k:k + 1, 0:n]
        with jax.named_scope('s65_ag_end_1_'):
            ag_end(1)
        with jax.named_scope('s66_for_cp_in_sends_'):
            for cp in sends:
                cp.wait_send()
        with jax.named_scope('s67_for_cp_in_outs_'):
            for cp in outs:
                cp.wait()

    sem = pltpu.SemaphoreType.DMA
    vmem = pltpu.VMEM
    scratch = [
        vmem((dim, voc), BF16), vmem((tok, voc), BF16), vmem((tok, dim), BF16), vmem((dim, tok), BF16),
        vmem((tok, voc), F32), vmem((tok, voc), F32), vmem((2, ht, vb), F32), vmem((dim, 128), F32),
        vmem((dim, tok), F32), vmem((dim, tok), F32),
        vmem((3, ht, 128), F32), vmem((2, ht, 128), F32), vmem((2, tok, 128), F32),
        vmem((2, 8, hh), F32), vmem((2, nt, 8, hh), F32), vmem((8, 128), F32), vmem((nd, 8, 128), F32),
        vmem((2, 8, 128), F32), vmem((2, SIDE, 8, 128), F32), vmem((8, 128), F32), vmem((nd, 8, 128), F32),
        vmem((2, 6, half_d, zc), F32), vmem((2, 6, fp // 2, zc), F32), vmem((2, dim, zc), F32),
        vmem((NV, half_d, vc), F32), vmem((NV, 6, cols, vh), F32),
        sem((3,)), sem((2, nt)), sem((2, nt)), sem((nd,)), sem((nd,)), sem((2, 6)), sem((2, 6)), sem((2, 6)), sem((2, 6)),
        sem((2, 6)), sem((2, 6)), sem((2, 6)), sem((2, 6)), sem((NV,)), sem((NV,)), sem((NV, 6)), sem((NV, 6)),
        sem((2, SIDE)), sem((2, SIDE)), sem((nd,)), sem((nd,)), sem((2 + NV,)),
    ]
    vm = pl.BlockSpec(memory_space=pltpu.VMEM)
    anys = pl.BlockSpec(memory_space=pl.ANY)
    return pl.pallas_call(
        kernel,
        out_shape=(jax.ShapeDtypeStruct((1, 1), F32), jax.ShapeDtypeStruct((dim, tok), BF16),
                   jax.ShapeDtypeStruct((cols, voc), F32), jax.ShapeDtypeStruct((1, dim), F32)),
        in_specs=[vm, vm, vm, anys, anys],
        out_specs=(vm, anys, anys, vm),
        scratch_shapes=scratch,
        compiler_params=pltpu.CompilerParams(collective_id=0, has_side_effects=True, vmem_limit_bytes=67043328),
        name='head',
    )


def finish(tok, dim, voc, cols):
    parts = 4
    rb, lb = tok // parts, voc // parts

    def kernel(dh, det, dw, dh_o, det_o, dw_o, hb, eb, sem_i, sem_o):
        views = []
        for i in range(parts):
            ls, es = pl.ds(i * rb, rb), pl.ds(i * lb, lb)
            views.append((dh.at[:, ls], hb.at[:, ls], dh_o.at[:, ls]))
            views.append((det.at[:, es], eb.at[:, es], det_o.at[:, es]))
        ins = [pltpu.make_async_copy(a, b, sem_i.at[k]) for k, (a, b, _) in enumerate(views)]
        outs = [pltpu.make_async_copy(b, o, sem_o.at[k]) for k, (_, b, o) in enumerate(views)]
        for cp in ins:
            cp.start()
        dw_o[...] = dw[...].reshape(dim)
        for ci, co in zip(ins, outs):
            ci.wait()
            co.start()
        for co in outs:
            co.wait()

    vm = pl.BlockSpec(memory_space=pltpu.VMEM)
    anys = pl.BlockSpec(memory_space=pl.ANY)
    return pl.pallas_call(
        kernel,
        out_shape=(jax.ShapeDtypeStruct((dim, tok), BF16), jax.ShapeDtypeStruct((cols, voc), F32), jax.ShapeDtypeStruct((dim,), F32)),
        in_specs=[anys, anys, vm],
        out_specs=(anys, anys, vm),
        scratch_shapes=[pltpu.VMEM((dim, tok), BF16), pltpu.VMEM((cols, voc), F32),
                        pltpu.SemaphoreType.DMA((2 * parts,)), pltpu.SemaphoreType.DMA((2 * parts,))],
        compiler_params=pltpu.CompilerParams(vmem_limit_bytes=67043328),
        name='finish',
    )


def solution(mesh):
    nt, nd = mesh.shape['tp'], mesh.shape['dp']

    def device_fn(hid, norm_w, emb, teach, mask):
        tok, dim = hid.shape
        call = build(tok, dim, emb.shape[0], nt, nd)
        loss, dh, det, dw = call(hid.T, norm_w, mask.reshape(1, tok), emb.T, teach)
        dh, det, dw = finish(tok, dim, emb.shape[0], dim // nd)(dh, det, dw)
        return loss.reshape(()), dh.T, det.T, dw

    return jax.shard_map(device_fn, mesh=mesh, in_specs=(P('dp', None), P(None), P('tp', None), P('dp', 'tp'), P('dp')),
                         out_specs=(P(), P('dp', None), P('tp', 'dp'), P(None)), check_vma=False)
```

```python
import jax
import jax.numpy as jnp
from jax import lax
from jax.experimental import pallas as pl
from jax.experimental.pallas import tpu as pltpu
from jax.sharding import PartitionSpec as P

CAP = 30.0
EPS = 1e-6
LOG2E = 1.4426950408889634
LN2 = 0.6931471805599453
MESH = pl.DeviceIdType.MESH
F32 = jnp.float32
BF16 = jnp.bfloat16
SIDE = 4
NV = 6


def build(tok, dim, voc, nt, nd):
    ht = tok // 2
    hh = ht // 2
    zc = ht // SIDE
    fp = dim // SIDE
    cols = dim // nd
    vc = voc // NV
    vh = vc // 2
    vb = min(512, voc // 2)
    nvb = voc // vb
    half_d = dim // 2
    dpad = -(-dim // 128) * 128

    def kernel(hid, w_ref, mask_ref, e_hbm, t_hbm, dh_out, det_out, small_out,
               et, t_v, gb, gt, tv, tx, scr, wpc, dg, dhf, acc, mcol, col, st_s, st_r, mk_s, mk_r, dwa_s, dwa_r, dwd_s, dwd_r, fin,
               zr, p2r, agb, d2r, xr,
               in_sem, ss_st, rs_st, ss_mk, rs_mk, ss_z, rs_z, ss_p, rs_p, ss_g, rs_g, ss_h, rs_h,
               ss_d, rs_d, ss_x, rs_x, ss_wa, rs_wa, ss_wd, rs_wd, out_sem):
        t = lax.axis_index('tp')
        d = lax.axis_index('dp')
        z, y = t // SIDE, lax.rem(t, SIDE)
        x, c = d // 2, lax.rem(d, 2)
        sends = []
        outs = []

        def rcopy(src, dst, ssem, rsem, dev):
            cp = pltpu.make_async_remote_copy(src_ref=src, dst_ref=dst, send_sem=ssem, recv_sem=rsem,
                                              device_id=dev, device_id_type=MESH)
            cp.start()
            sends.append(cp)
            return cp

        class RingSum:
            def __init__(self, sl, buf, ss, rs, dev, p):
                self.sl, self.buf, self.ss, self.rs, self.dev = sl, buf, ss, rs, dev
                self.p, self.nxt, self.prv, self.opp = p, lax.rem(p + 1, SIDE), lax.rem(p + 3, SIDE), lax.rem(p + 2, SIDE)

            def send(self, k, q, half, to):
                return rcopy(self.sl(q, half), self.buf(k), self.ss.at[k], self.rs.at[k], self.dev(to))

            def start(self):
                self.a0 = self.send(0, self.opp, 0, self.nxt)
                self.a1 = self.send(1, self.opp, 1, self.prv)
                self.b0 = self.send(2, self.nxt, 1, self.nxt)
                self.b1 = self.send(3, self.prv, 0, self.prv)

            def mid(self):
                self.a0.wait_recv()
                part = self.sl(self.nxt, 0)
                part[...] += self.buf(0)[...]
                self.c0 = self.send(4, self.nxt, 0, self.nxt)
                self.a1.wait_recv()
                part = self.sl(self.prv, 1)
                part[...] += self.buf(1)[...]
                self.c1 = self.send(5, self.prv, 1, self.prv)

            def end(self):
                for cp in (self.b0, self.b1, self.c0, self.c1):
                    cp.wait_recv()
                return (self.sl(self.p, 0)[...] + self.buf(4)[...] + self.buf(3)[...],
                        self.sl(self.p, 1)[...] + self.buf(2)[...] + self.buf(5)[...])

        class RingGather:
            def __init__(self, sl, ss, rs, dev, p):
                self.sl, self.ss, self.rs, self.dev = sl, ss, rs, dev
                self.p, self.nxt, self.prv = p, lax.rem(p + 1, SIDE), lax.rem(p + 3, SIDE)

            def send(self, k, q, half, to):
                return rcopy(self.sl(q, half), self.sl(q, half), self.ss.at[k], self.rs.at[k], self.dev(to))

            def start(self):
                self.a0 = self.send(0, self.p, 0, self.nxt)
                self.a1 = self.send(1, self.p, 1, self.prv)
                self.b0 = self.send(2, self.p, 1, self.nxt)
                self.b1 = self.send(3, self.p, 0, self.prv)

            def mid(self):
                self.a0.wait_recv()
                self.c0 = self.send(4, self.prv, 0, self.nxt)
                self.a1.wait_recv()
                self.c1 = self.send(5, self.nxt, 1, self.prv)

            def end(self):
                for cp in (self.b0, self.b1, self.c0, self.c1):
                    cp.wait_recv()

        in_cp = [pltpu.make_async_copy(e_hbm, et, in_sem.at[0])]
        for h in range(2):
            rows = pl.ds(h * ht, ht)
            in_cp.append(pltpu.make_async_copy(t_hbm.at[rows, :], t_v.at[rows, :], in_sem.at[1 + h]))
        for cp in (in_cp[1], in_cp[0], in_cp[2]):
            cp.start()

        barrier = pltpu.get_barrier_semaphore()
        for k in range(1, nt):
            pl.semaphore_signal(barrier, inc=1, device_id={'tp': lax.rem(t + k, nt), 'dp': d}, device_id_type=MESH)
        for k in range(1, nd):
            pl.semaphore_signal(barrier, inc=1, device_id={'tp': t, 'dp': lax.rem(d + k, nd)}, device_id_type=MESH)

        def pad_f(a, axis):
            shape = list(a.shape)
            shape[axis] = dpad - dim
            return jnp.concatenate([a, jnp.zeros(shape, F32)], axis=axis) if dpad > dim else a

        wrow = pad_f(1.0 + w_ref[...].astype(F32).reshape(1, dim), 1)
        wpc[...] = jnp.broadcast_to(wrow, (128, dpad)).T[:dim, :]

        def norm_step(i, _):
            r0 = pl.multiple_of(i * 128, 128)
            xv = hid[:, pl.ds(r0, 128)].astype(F32)
            s = lax.rsqrt(jnp.mean(xv * xv, axis=0, keepdims=True) + EPS)
            g = xv * s * wpc[...]
            gb[pl.ds(r0, 128), :] = pad_f(g, 0).T[:, :dim].astype(BF16)
            gp = [g[(2 * xx + cc) * cols:(2 * xx + cc + 1) * cols, :] for cc in range(2) for xx in range(SIDE)]
            gt[:, pl.ds(r0, 128)] = jnp.concatenate(gp, axis=0).astype(BF16)
            return 0

        lax.fori_loop(0, tok // 128, norm_step, 0)

        maskf = mask_ref[...].astype(F32)
        mk_s[...] = jnp.broadcast_to(jnp.sum(maskf, axis=1, keepdims=True), (8, 128))
        mk_r[d] = mk_s[...]

        def forward(h):
            base = h * ht
            in_cp[1 + h].wait()

            def mx(i, _):
                r = pl.multiple_of(base + i * 64, 64)
                m = t_v[pl.ds(r, 64), 0:128]
                for q in range(1, voc // 128):
                    m = jnp.maximum(m, t_v[pl.ds(r, 64), q * 128:(q + 1) * 128])
                mm = jnp.max(m.astype(F32), axis=1, keepdims=True)
                mcol[h, pl.ds(pl.multiple_of(i * 64, 64), 64), :] = jnp.broadcast_to(mm, (64, 128))
                return 0

            lax.fori_loop(0, ht // 64, mx, 0)
            if h == 0:
                in_cp[0].wait()
            acc[...] = jnp.zeros_like(acc)

            def fdot(b, slot):
                v0 = pl.multiple_of(b * vb, vb)
                scr[slot] = jnp.dot(gb[base:base + ht, :], et[:, pl.ds(v0, vb)], preferred_element_type=F32)

            def elem(b, slot):
                for i in range(0, ht, 16):
                    r = slice(base + i, base + i + 16)
                    a = slice(i, i + 16)
                    m = mcol[h, a, :]
                    zs, zt, qs = acc[0, a, :], acc[1, a, :], acc[2, a, :]
                    for q in range(vb // 128):
                        lanes = pl.ds(pl.multiple_of(b * vb + q * 128, 128), 128)
                        th = jnp.tanh(scr[slot, a, q * 128:(q + 1) * 128] * (1.0 / CAP))
                        tv[r, lanes] = th
                        u = (t_v[r, lanes].astype(F32) - m) * LOG2E
                        v = th * (CAP * LOG2E)
                        ex = jnp.exp2(u)
                        tx[r, pl.ds(pl.multiple_of(b * vb + (q ^ 2) * 128, 128), 128)] = ex
                        zs = zs + jnp.exp2(v)
                        zt = zt + ex
                        qs = qs + ex * (u - v)
                    acc[0, a, :] = zs
                    acc[1, a, :] = zt
                    acc[2, a, :] = qs

            fdot(0, 0)

            def vstep(i, _):
                b = i * 2
                fdot(b + 1, 1)
                elem(b, 0)
                fdot(jnp.minimum(b + 2, nvb - 1), 0)
                elem(b + 1, 1)
                return 0

            lax.fori_loop(0, nvb // 2, vstep, 0)
            parts = [mcol[h].T[0:1, :]] + [jnp.sum(acc[k].T, axis=0, keepdims=True) for k in range(3)]
            st_s[h] = jnp.concatenate([p[:, i * hh:(i + 1) * hh] for p in parts for i in range(2)], axis=0)
            st_r[h, t] = st_s[h]
            if h == 0:
                pl.semaphore_wait(barrier, nt + nd - 2)
            return [rcopy(st_s.at[h], st_r.at[h, t], ss_st.at[h, k], rs_st.at[h, k], {'tp': lax.rem(t + k, nt), 'dp': d})
                    for k in range(1, nt)]

        def combine(h, cps, inv_m):
            for cp in cps:
                cp.wait_recv()
            def stat(k):
                return jnp.concatenate([st_r[h, :, 2 * k, :], st_r[h, :, 2 * k + 1, :]], axis=1)

            mts = stat(0)
            mt = jnp.max(mts, axis=0, keepdims=True)
            dm = jnp.maximum(mts - mt, -3e38)
            e = jnp.exp(dm)
            zte = stat(2) * e
            zt = jnp.sum(zte, axis=0, keepdims=True)
            zs = jnp.sum(stat(1), axis=0, keepdims=True)
            a = jnp.sum(stat(3) * LN2 * e + zte * dm, axis=0, keepdims=True)
            kl = a / zt - jnp.log(zt) + jnp.log(zs)
            w = maskf[:, h * ht:(h + 1) * ht] * inv_m
            own = jnp.concatenate([st_s[h, 0:1, :], st_s[h, 1:2, :]], axis=1)
            mine = jnp.exp(jnp.maximum(own - mt, -3e38))
            for k, row in enumerate((w / zs, w / zt * mine)):
                col[k, h * ht:(h + 1) * ht, :] = jnp.broadcast_to(row, (128, ht)).T
            return jnp.sum(w * kl, axis=1, keepdims=True)

        def dlogit(h):
            base = h * ht

            def rstep(i, _):
                r = pl.ds(pl.multiple_of(base + i * 16, 16), 16)
                cs, ct = col[0, r, :], col[1, r, :]
                for q in range(voc // 128):
                    lanes = slice(q * 128, (q + 1) * 128)
                    th = tv[r, lanes]
                    ps = jnp.exp2(th * (CAP * LOG2E)) * cs
                    t_v[r, lanes] = ((ps - tx[r, (q ^ 2) * 128:(q ^ 2) * 128 + 128] * ct) * (1.0 - th * th)).astype(BF16)
                return 0

            lax.fori_loop(0, ht // 16, rstep, 0)

        def dgrad(h):
            rows = slice(h * ht, (h + 1) * ht)
            dg[:, rows] = lax.dot_general(et[...], t_v[rows, :], (((1,), (1,)), ((), ())), preferred_element_type=F32)

        pos1, pos2 = (z, y), (y, z)

        def chunk(h, q):
            return pl.ds(pl.multiple_of(h * ht + q * zc, zc), zc)

        def frows(q, half):
            return pl.ds(pl.multiple_of(q * fp + half * (fp // 2), 8), fp // 2)

        def dev1(h):
            return lambda q: {'tp': q * SIDE + y if h == 0 else z * SIDE + q, 'dp': d}

        def dev2(h):
            return lambda q: {'tp': z * SIDE + q if h == 0 else q * SIDE + y, 'dp': d}

        def make(h):
            r1 = RingSum(lambda q, half: dg.at[half * half_d:(half + 1) * half_d, chunk(h, q)], lambda k: zr.at[h, k],
                         ss_z.at[h], rs_z.at[h], dev1(h), pos1[h])
            r2 = RingSum(lambda q, half: dg.at[frows(q, half), chunk(h, pos1[h])], lambda k: p2r.at[h, k],
                         ss_p.at[h], rs_p.at[h], dev2(h), pos2[h])
            g1 = RingGather(lambda q, half: agb.at[h, frows(q, half), :], ss_g.at[h], rs_g.at[h], dev2(h), pos2[h])
            g2 = RingGather(lambda q, half: dhf.at[half * half_d:(half + 1) * half_d, chunk(h, q)],
                            ss_h.at[h], rs_h.at[h], dev1(h), pos1[h])
            return r1, r2, g1, g2

        ring = (make(0), make(1))

        def rs_end(h):
            r1, r2 = ring[h][:2]
            lo_v, hi_v = r1.end()
            r1.sl(r1.p, 0)[...] = lo_v
            r1.sl(r1.p, 1)[...] = hi_v
            r2.start()

        def p2_end(h):
            r2, g1 = ring[h][1:3]
            lo_v, hi_v = r2.end()
            g1.sl(g1.p, 0)[...] = lo_v
            g1.sl(g1.p, 1)[...] = hi_v
            g1.start()

        def norm_back(h):
            g1, g2 = ring[h][2:]
            g1.end()
            ck = chunk(h, pos1[h])
            gv = agb[h]
            xv = hid[:, ck].astype(F32)
            s = lax.rsqrt(jnp.mean(xv * xv, axis=0, keepdims=True) + EPS)
            cv = gv * wpc[:, :zc]
            m = jnp.mean(cv * xv, axis=0, keepdims=True)
            dwv = jnp.sum(pad_f(gv * xv * s, 0).T, axis=0, keepdims=True)
            for k in range(8):
                part = dwv[:, k * 128:(k + 1) * 128] if k < dpad // 128 else jnp.zeros((1, 128), F32)
                dwa_s[h, k:k + 1, :] = part
            dwa_r[h, pos1[h]] = dwa_s[h]
            cps = [rcopy(dwa_s.at[h], dwa_r.at[h, pos1[h]], ss_wa.at[h, k], rs_wa.at[h, k], dev1(h)(lax.rem(pos1[h] + k, SIDE)))
                   for k in range(1, SIDE)]
            dhf[:, ck] = s * cv - xv * (s * s * s * m)
            return cps

        def ag_end(h):
            ring[h][3].end()
            rows = slice(h * ht, (h + 1) * ht)
            t_v[0:dim, rows] = dhf[:, rows].astype(BF16)
            cp = pltpu.make_async_copy(t_v.at[0:dim, rows], dh_out.at[:, rows], out_sem.at[h])
            cp.start()
            outs.append(cp)

        def de_start(j):
            tv[0:dim, j * vc:(j + 1) * vc] = jnp.dot(gt[...], t_v[:, j * vc:(j + 1) * vc], preferred_element_type=F32)
            other = pl.ds(pl.multiple_of((1 - c) * half_d, 8), half_d)
            return rcopy(tv.at[other, j * vc:(j + 1) * vc], d2r.at[j], ss_d.at[j], rs_d.at[j], {'tp': t, 'dp': x * 2 + 1 - c})

        def make_x(j):
            def sl(q, half):
                return tv.at[pl.ds(pl.multiple_of(c * half_d + q * cols, 8), cols), j * vc + half * vh:j * vc + (half + 1) * vh]

            return RingSum(sl, lambda k: xr.at[j, k], ss_x.at[j], rs_x.at[j], lambda q: {'tp': t, 'dp': q * 2 + c}, x)

        xring = [make_x(j) for j in range(NV)]

        def x_start(j, cp):
            cp.wait_recv()
            mine = pl.ds(pl.multiple_of(c * half_d, 8), half_d)
            tv[mine, j * vc:(j + 1) * vc] += d2r[j]
            xring[j].start()

        def x_end(j):
            lo_v, hi_v = xring[j].end()
            tx[0:cols, j * vc:j * vc + vh] = lo_v
            tx[0:cols, j * vc + vh:(j + 1) * vc] = hi_v
            cp = pltpu.make_async_copy(tx.at[0:cols, j * vc:(j + 1) * vc], det_out.at[:, j * vc:(j + 1) * vc], out_sem.at[2 + j])
            cp.start()
            outs.append(cp)

        with jax.named_scope('s00_st0_forward_0_'):
            st0 = forward(0)
        with jax.named_scope('s01_mk_cp_rcopy_mk_s_mk_r_at_d_s'):
            mk_cp = [rcopy(mk_s, mk_r.at[d], ss_mk.at[k], rs_mk.at[k], {'tp': t, 'dp': lax.rem(d + k, nd)}) for k in range(1, nd)]
        with jax.named_scope('s02_st1_forward_1_'):
            st1 = forward(1)
        with jax.named_scope('s03_for_cp_in_mk_cp_'):
            for cp in mk_cp:
                cp.wait_recv()
        with jax.named_scope('s04_inv_m_1_0_jnp_sum_mk_r_0_axi'):
            inv_m = 1.0 / jnp.sum(mk_r[:, 0, :], axis=0, keepdims=True)[:, 0:1]
        with jax.named_scope('s05_loss_combine_0_st0_inv_m_'):
            loss = combine(0, st0, inv_m)
        with jax.named_scope('s06_dlogit_0_'):
            dlogit(0)
        with jax.named_scope('s07_dgrad_0_'):
            dgrad(0)
        with jax.named_scope('s08_ring_0_0_start_'):
            ring[0][0].start()
        with jax.named_scope('s09_loss_loss_combine_1_st1_inv_'):
            loss = loss + combine(1, st1, inv_m)
        with jax.named_scope('s10_dlogit_1_'):
            dlogit(1)
        with jax.named_scope('s11_dgrad_1_'):
            dgrad(1)
        with jax.named_scope('s12_ring_1_0_start_'):
            ring[1][0].start()
        with jax.named_scope('s13_dd_None_NV'):
            dd = [None] * NV
        with jax.named_scope('s14_dd_0_de_start_0_'):
            dd[0] = de_start(0)
        with jax.named_scope('s15_dd_1_de_start_1_'):
            dd[1] = de_start(1)
        with jax.named_scope('s16_ring_0_0_mid_'):
            ring[0][0].mid()
        with jax.named_scope('s17_dd_2_de_start_2_'):
            dd[2] = de_start(2)
        with jax.named_scope('s18_x_start_0_dd_0_'):
            x_start(0, dd[0])
        with jax.named_scope('s19_dd_3_de_start_3_'):
            dd[3] = de_start(3)
        with jax.named_scope('s20_x_start_1_dd_1_'):
            x_start(1, dd[1])
        with jax.named_scope('s21_dd_4_de_start_4_'):
            dd[4] = de_start(4)
        with jax.named_scope('s22_x_start_2_dd_2_'):
            x_start(2, dd[2])
        with jax.named_scope('s23_dd_5_de_start_5_'):
            dd[5] = de_start(5)
        with jax.named_scope('s24_x_start_3_dd_3_'):
            x_start(3, dd[3])
        with jax.named_scope('s25_x_start_4_dd_4_'):
            x_start(4, dd[4])
        with jax.named_scope('s26_ring_1_0_mid_'):
            ring[1][0].mid()
        with jax.named_scope('s27_x_start_5_dd_5_'):
            x_start(5, dd[5])
        with jax.named_scope('s28_xring_0_mid_'):
            xring[0].mid()
        with jax.named_scope('s29_rs_end_0_'):
            rs_end(0)
        with jax.named_scope('s30_xring_1_mid_'):
            xring[1].mid()
        with jax.named_scope('s31_rs_end_1_'):
            rs_end(1)
        with jax.named_scope('s32_ring_0_1_mid_'):
            ring[0][1].mid()
        with jax.named_scope('s33_xring_2_mid_'):
            xring[2].mid()
        with jax.named_scope('s34_p2_end_0_'):
            p2_end(0)
        with jax.named_scope('s35_ring_1_1_mid_'):
            ring[1][1].mid()
        with jax.named_scope('s36_xring_3_mid_'):
            xring[3].mid()
        with jax.named_scope('s37_ring_0_2_mid_'):
            ring[0][2].mid()
        with jax.named_scope('s38_p2_end_1_'):
            p2_end(1)
        with jax.named_scope('s39_xring_4_mid_'):
            xring[4].mid()
        with jax.named_scope('s40_wa0_norm_back_0_'):
            wa0 = norm_back(0)
        with jax.named_scope('s41_ring_1_2_mid_'):
            ring[1][2].mid()
        with jax.named_scope('s42_ring_0_3_start_'):
            ring[0][3].start()
        with jax.named_scope('s43_xring_5_mid_'):
            xring[5].mid()
        with jax.named_scope('s44_wa1_norm_back_1_'):
            wa1 = norm_back(1)
        with jax.named_scope('s45_ring_1_3_start_'):
            ring[1][3].start()
        with jax.named_scope('s46_ring_0_3_mid_'):
            ring[0][3].mid()
        with jax.named_scope('s47_for_cp_in_wa0_wa1_'):
            for cp in wa0 + wa1:
                cp.wait_recv()
        with jax.named_scope('s48_dws_jnp_sum_dwa_r_0_axis_0_j'):
            dws = jnp.sum(dwa_r[0], axis=0) + jnp.sum(dwa_r[1], axis=0)
        with jax.named_scope('s49_rowi_lax_broadcasted_iota_jn'):
            rowi = lax.broadcasted_iota(jnp.int32, (8, 128), 0)
        with jax.named_scope('s50_dwd_s_jnp_where_rowi_7_jnp_b'):
            dwd_s[...] = jnp.where(rowi == 7, jnp.broadcast_to(loss, (8, 128)), dws)
        with jax.named_scope('s51_dwd_r_d_dwd_s_'):
            dwd_r[d] = dwd_s[...]
        with jax.named_scope('s52_wd_rcopy_dwd_s_dwd_r_at_d_ss'):
            wd = [rcopy(dwd_s, dwd_r.at[d], ss_wd.at[k], rs_wd.at[k], {'tp': t, 'dp': lax.rem(d + k, nd)}) for k in range(1, nd)]
        with jax.named_scope('s53_x_end_0_'):
            x_end(0)
        with jax.named_scope('s54_ring_1_3_mid_'):
            ring[1][3].mid()
        with jax.named_scope('s55_x_end_1_'):
            x_end(1)
        with jax.named_scope('s56_x_end_2_'):
            x_end(2)
        with jax.named_scope('s57_x_end_3_'):
            x_end(3)
        with jax.named_scope('s58_ag_end_0_'):
            ag_end(0)
        with jax.named_scope('s59_x_end_4_'):
            x_end(4)
        with jax.named_scope('s60_x_end_5_'):
            x_end(5)
        with jax.named_scope('s61_for_cp_in_wd_'):
            for cp in wd:
                cp.wait_recv()
        with jax.named_scope('s62_fin_jnp_sum_dwd_r_axis_0_'):
            fin[...] = jnp.sum(dwd_r[...], axis=0)
        with jax.named_scope('s63_outs_append_pltpu_make_async'):
            outs.append(pltpu.make_async_copy(fin, small_out, out_sem.at[2 + NV]))
        with jax.named_scope('s64_outs_1_start_'):
            outs[-1].start()
        with jax.named_scope('s65_ag_end_1_'):
            ag_end(1)
        with jax.named_scope('s66_for_cp_in_sends_'):
            for cp in sends:
                cp.wait_send()
        with jax.named_scope('s67_for_cp_in_outs_'):
            for cp in outs:
                cp.wait()

    sem = pltpu.SemaphoreType.DMA
    vmem = pltpu.VMEM
    scratch = [
        vmem((dim, voc), BF16), vmem((tok, voc), BF16), vmem((tok, dim), BF16), vmem((dim, tok), BF16),
        vmem((tok, voc), F32), vmem((tok, voc), F32), vmem((2, ht, vb), F32), vmem((dim, 128), F32),
        vmem((dim, tok), F32), vmem((dim, tok), F32),
        vmem((3, ht, 128), F32), vmem((2, ht, 128), F32), vmem((2, tok, 128), F32),
        vmem((2, 8, hh), F32), vmem((2, nt, 8, hh), F32), vmem((8, 128), F32), vmem((nd, 8, 128), F32),
        vmem((2, 8, 128), F32), vmem((2, SIDE, 8, 128), F32), vmem((8, 128), F32), vmem((nd, 8, 128), F32), vmem((8, 128), F32),
        vmem((2, 6, half_d, zc), F32), vmem((2, 6, fp // 2, zc), F32), vmem((2, dim, zc), F32),
        vmem((NV, half_d, vc), F32), vmem((NV, 6, cols, vh), F32),
        sem((3,)), sem((2, nt)), sem((2, nt)), sem((nd,)), sem((nd,)), sem((2, 6)), sem((2, 6)), sem((2, 6)), sem((2, 6)),
        sem((2, 6)), sem((2, 6)), sem((2, 6)), sem((2, 6)), sem((NV,)), sem((NV,)), sem((NV, 6)), sem((NV, 6)),
        sem((2, SIDE)), sem((2, SIDE)), sem((nd,)), sem((nd,)), sem((3 + NV,)),
    ]
    vm = pl.BlockSpec(memory_space=pltpu.VMEM)
    anys = pl.BlockSpec(memory_space=pl.ANY)
    return pl.pallas_call(
        kernel,
        out_shape=(jax.ShapeDtypeStruct((dim, tok), BF16), jax.ShapeDtypeStruct((cols, voc), F32), jax.ShapeDtypeStruct((8, 128), F32)),
        in_specs=[vm, vm, vm, anys, anys],
        out_specs=(anys, anys, anys),
        scratch_shapes=scratch,
        compiler_params=pltpu.CompilerParams(collective_id=0, has_side_effects=True, vmem_limit_bytes=67043328),
        name='head',
    )


def finish(tok, dim, voc, cols):
    parts = 4
    rb, lb = tok // parts, voc // parts

    def kernel(dh, det, small, dh_o, det_o, dw_o, loss_o, hb, eb, sb, wb, lb_v, sem_i, sem_o):
        views = []
        for i in range(parts):
            ls, es = pl.ds(i * rb, rb), pl.ds(i * lb, lb)
            views.append((dh.at[:, ls], hb.at[:, ls], dh_o.at[:, ls]))
            views.append((det.at[:, es], eb.at[:, es], det_o.at[:, es]))
        ins = [pltpu.make_async_copy(small, sb, sem_i.at[2 * parts])]
        ins += [pltpu.make_async_copy(a, b, sem_i.at[k]) for k, (a, b, _) in enumerate(views)]
        outs = [pltpu.make_async_copy(wb, dw_o, sem_o.at[2 * parts]), pltpu.make_async_copy(lb_v, loss_o, sem_o.at[2 * parts + 1])]
        outs += [pltpu.make_async_copy(b, o, sem_o.at[k]) for k, (_, b, o) in enumerate(views)]
        for cp in ins:
            cp.start()
        ins[0].wait()
        row = jnp.concatenate([sb[k:k + 1, :] for k in range(-(-dim // 128))], axis=1)
        wb[...] = row[:, :dim].reshape(dim)
        lb_v[...] = sb[7:8, 0:1]
        outs[0].start()
        outs[1].start()
        for ci, co in zip(ins[1:], outs[2:]):
            ci.wait()
            co.start()
        for co in outs:
            co.wait()

    anys = pl.BlockSpec(memory_space=pl.ANY)
    return pl.pallas_call(
        kernel,
        out_shape=(jax.ShapeDtypeStruct((dim, tok), BF16), jax.ShapeDtypeStruct((cols, voc), F32),
                   jax.ShapeDtypeStruct((dim,), F32), jax.ShapeDtypeStruct((1, 1), F32)),
        in_specs=[anys, anys, anys],
        out_specs=(anys, anys, anys, anys),
        scratch_shapes=[pltpu.VMEM((dim, tok), BF16), pltpu.VMEM((cols, voc), F32), pltpu.VMEM((8, 128), F32), pltpu.VMEM((dim,), F32),
                        pltpu.VMEM((1, 1), F32), pltpu.SemaphoreType.DMA((2 * parts + 1,)), pltpu.SemaphoreType.DMA((2 * parts + 2,))],
        compiler_params=pltpu.CompilerParams(vmem_limit_bytes=67043328),
        name='finish',
    )


def solution(mesh):
    nt, nd = mesh.shape['tp'], mesh.shape['dp']

    def device_fn(hid, norm_w, emb, teach, mask):
        tok, dim = hid.shape
        call = build(tok, dim, emb.shape[0], nt, nd)
        dh, det, small = call(hid.T, norm_w, mask.reshape(1, tok), emb.T, teach)
        dh, det, dw, loss = finish(tok, dim, emb.shape[0], dim // nd)(dh, det, small)
        return loss.reshape(()), dh.T, det.T, dw

    return jax.shard_map(device_fn, mesh=mesh, in_specs=(P('dp', None), P(None), P('tp', None), P('dp', 'tp'), P('dp')),
                         out_specs=(P(), P('dp', None), P('tp', 'dp'), P(None)), check_vma=False)
```

```python
import jax
import jax.numpy as jnp
from jax import lax
from jax.experimental import pallas as pl
from jax.experimental.pallas import tpu as pltpu
from jax.sharding import PartitionSpec as P

CAP = 30.0
EPS = 1e-6
LOG2E = 1.4426950408889634
LN2 = 0.6931471805599453
MESH = pl.DeviceIdType.MESH
F32 = jnp.float32
BF16 = jnp.bfloat16
SIDE = 4
NV = 6


def build(tok, dim, voc, nt, nd):
    ht = tok // 2
    hh = ht // 2
    zc = ht // SIDE
    fp = dim // SIDE
    cols = dim // nd
    vc = voc // NV
    vh = vc // 2
    vb = min(512, voc // 2)
    nvb = voc // vb
    half_d = dim // 2
    dpad = -(-dim // 128) * 128

    def kernel(hid, w_ref, mask_ref, e_hbm, t_hbm, dh_out, det_out, small_out,
               et, t_v, gb, gt, tv, tx, scr, wpc, dg, dhf, acc, mcol, col, st_s, st_r, mk_s, mk_r, dwa_s, dwa_r, dwd_s, dwd_r, fin,
               zr, p2r, agb, d2r, xr,
               in_sem, ss_st, rs_st, ss_mk, rs_mk, ss_z, rs_z, ss_p, rs_p, ss_g, rs_g, ss_h, rs_h,
               ss_d, rs_d, ss_x, rs_x, ss_wa, rs_wa, ss_wd, rs_wd, out_sem):
        t = lax.axis_index('tp')
        d = lax.axis_index('dp')
        z, y = t // SIDE, lax.rem(t, SIDE)
        x, c = d // 2, lax.rem(d, 2)
        sends = []
        outs = []

        def rcopy(src, dst, ssem, rsem, dev):
            cp = pltpu.make_async_remote_copy(src_ref=src, dst_ref=dst, send_sem=ssem, recv_sem=rsem,
                                              device_id=dev, device_id_type=MESH)
            cp.start()
            sends.append(cp)
            return cp

        class RingSum:
            def __init__(self, sl, buf, ss, rs, dev, p):
                self.sl, self.buf, self.ss, self.rs, self.dev = sl, buf, ss, rs, dev
                self.p, self.nxt, self.prv, self.opp = p, lax.rem(p + 1, SIDE), lax.rem(p + 3, SIDE), lax.rem(p + 2, SIDE)

            def send(self, k, q, half, to):
                return rcopy(self.sl(q, half), self.buf(k), self.ss.at[k], self.rs.at[k], self.dev(to))

            def start(self):
                self.a0 = self.send(0, self.opp, 0, self.nxt)
                self.a1 = self.send(1, self.opp, 1, self.prv)
                self.b0 = self.send(2, self.nxt, 1, self.nxt)
                self.b1 = self.send(3, self.prv, 0, self.prv)

            def mid(self):
                self.a0.wait_recv()
                part = self.sl(self.nxt, 0)
                part[...] += self.buf(0)[...]
                self.c0 = self.send(4, self.nxt, 0, self.nxt)
                self.a1.wait_recv()
                part = self.sl(self.prv, 1)
                part[...] += self.buf(1)[...]
                self.c1 = self.send(5, self.prv, 1, self.prv)

            def end(self):
                for cp in (self.b0, self.b1, self.c0, self.c1):
                    cp.wait_recv()
                return (self.sl(self.p, 0)[...] + self.buf(4)[...] + self.buf(3)[...],
                        self.sl(self.p, 1)[...] + self.buf(2)[...] + self.buf(5)[...])

        class RingGather:
            def __init__(self, sl, ss, rs, dev, p):
                self.sl, self.ss, self.rs, self.dev = sl, ss, rs, dev
                self.p, self.nxt, self.prv = p, lax.rem(p + 1, SIDE), lax.rem(p + 3, SIDE)

            def send(self, k, q, half, to):
                return rcopy(self.sl(q, half), self.sl(q, half), self.ss.at[k], self.rs.at[k], self.dev(to))

            def start(self):
                self.a0 = self.send(0, self.p, 0, self.nxt)
                self.a1 = self.send(1, self.p, 1, self.prv)
                self.b0 = self.send(2, self.p, 1, self.nxt)
                self.b1 = self.send(3, self.p, 0, self.prv)

            def mid(self):
                self.a0.wait_recv()
                self.c0 = self.send(4, self.prv, 0, self.nxt)
                self.a1.wait_recv()
                self.c1 = self.send(5, self.nxt, 1, self.prv)

            def end(self):
                for cp in (self.b0, self.b1, self.c0, self.c1):
                    cp.wait_recv()

        in_cp = [pltpu.make_async_copy(e_hbm, et, in_sem.at[0])]
        for h in range(2):
            rows = pl.ds(h * ht, ht)
            in_cp.append(pltpu.make_async_copy(t_hbm.at[rows, :], t_v.at[rows, :], in_sem.at[1 + h]))
        for cp in (in_cp[1], in_cp[0], in_cp[2]):
            cp.start()

        barrier = pltpu.get_barrier_semaphore()
        for k in range(1, nt):
            pl.semaphore_signal(barrier, inc=1, device_id={'tp': lax.rem(t + k, nt), 'dp': d}, device_id_type=MESH)
        for k in range(1, nd):
            pl.semaphore_signal(barrier, inc=1, device_id={'tp': t, 'dp': lax.rem(d + k, nd)}, device_id_type=MESH)

        def pad_f(a, axis):
            shape = list(a.shape)
            shape[axis] = dpad - dim
            return jnp.concatenate([a, jnp.zeros(shape, F32)], axis=axis) if dpad > dim else a

        wrow = pad_f(1.0 + w_ref[...].astype(F32).reshape(1, dim), 1)
        wpc[...] = jnp.broadcast_to(wrow, (128, dpad)).T[:dim, :]

        def norm_step(i, _):
            r0 = pl.multiple_of(i * 128, 128)
            xv = hid[:, pl.ds(r0, 128)].astype(F32)
            s = lax.rsqrt(jnp.mean(xv * xv, axis=0, keepdims=True) + EPS)
            g = xv * s * wpc[...]
            gb[pl.ds(r0, 128), :] = pad_f(g, 0).T[:, :dim].astype(BF16)
            gp = [g[(2 * xx + cc) * cols:(2 * xx + cc + 1) * cols, :] for cc in range(2) for xx in range(SIDE)]
            gt[:, pl.ds(r0, 128)] = jnp.concatenate(gp, axis=0).astype(BF16)
            return 0

        lax.fori_loop(0, tok // 128, norm_step, 0)

        maskf = mask_ref[...].astype(F32)
        mk_s[...] = jnp.broadcast_to(jnp.sum(maskf, axis=1, keepdims=True), (8, 128))
        mk_r[d] = mk_s[...]

        def forward(h):
            base = h * ht
            in_cp[1 + h].wait()

            def mx(i, _):
                r = pl.multiple_of(base + i * 64, 64)
                m = t_v[pl.ds(r, 64), 0:128]
                for q in range(1, voc // 128):
                    m = jnp.maximum(m, t_v[pl.ds(r, 64), q * 128:(q + 1) * 128])
                mm = jnp.max(m.astype(F32), axis=1, keepdims=True)
                mcol[h, pl.ds(pl.multiple_of(i * 64, 64), 64), :] = jnp.broadcast_to(mm, (64, 128))
                return 0

            lax.fori_loop(0, ht // 64, mx, 0)
            if h == 0:
                in_cp[0].wait()
            acc[...] = jnp.zeros_like(acc)

            def fdot(b, slot):
                v0 = pl.multiple_of(b * vb, vb)
                scr[slot] = jnp.dot(gb[base:base + ht, :], et[:, pl.ds(v0, vb)], preferred_element_type=F32)

            def elem(b, slot):
                for i in range(0, ht, 16):
                    r = slice(base + i, base + i + 16)
                    a = slice(i, i + 16)
                    m = mcol[h, a, :]
                    zs, zt, qs = acc[0, a, :], acc[1, a, :], acc[2, a, :]
                    for q in range(vb // 128):
                        lanes = pl.ds(pl.multiple_of(b * vb + q * 128, 128), 128)
                        th = jnp.tanh(scr[slot, a, q * 128:(q + 1) * 128] * (1.0 / CAP))
                        tv[r, lanes] = th
                        u = (t_v[r, lanes].astype(F32) - m) * LOG2E
                        v = th * (CAP * LOG2E)
                        ex = jnp.exp2(u)
                        tx[r, pl.ds(pl.multiple_of(b * vb + (q ^ 2) * 128, 128), 128)] = ex
                        zs = zs + jnp.exp2(v)
                        zt = zt + ex
                        qs = qs + ex * (u - v)
                    acc[0, a, :] = zs
                    acc[1, a, :] = zt
                    acc[2, a, :] = qs

            fdot(0, 0)

            def vstep(i, _):
                b = i * 2
                fdot(b + 1, 1)
                elem(b, 0)
                fdot(jnp.minimum(b + 2, nvb - 1), 0)
                elem(b + 1, 1)
                return 0

            lax.fori_loop(0, nvb // 2, vstep, 0)
            parts = [mcol[h].T[0:1, :]] + [jnp.sum(acc[k].T, axis=0, keepdims=True) for k in range(3)]
            st_s[h] = jnp.concatenate([p[:, i * hh:(i + 1) * hh] for p in parts for i in range(2)], axis=0)
            st_r[h, t] = st_s[h]
            if h == 0:
                pl.semaphore_wait(barrier, nt + nd - 2)
            return [rcopy(st_s.at[h], st_r.at[h, t], ss_st.at[h, k], rs_st.at[h, k], {'tp': lax.rem(t + k, nt), 'dp': d})
                    for k in range(1, nt)]

        def combine(h, cps, inv_m):
            for cp in cps:
                cp.wait_recv()
            def stat(k):
                return jnp.concatenate([st_r[h, :, 2 * k, :], st_r[h, :, 2 * k + 1, :]], axis=1)

            mts = stat(0)
            mt = jnp.max(mts, axis=0, keepdims=True)
            dm = jnp.maximum(mts - mt, -3e38)
            e = jnp.exp(dm)
            zte = stat(2) * e
            zt = jnp.sum(zte, axis=0, keepdims=True)
            zs = jnp.sum(stat(1), axis=0, keepdims=True)
            a = jnp.sum(stat(3) * LN2 * e + zte * dm, axis=0, keepdims=True)
            kl = a / zt - jnp.log(zt) + jnp.log(zs)
            w = maskf[:, h * ht:(h + 1) * ht] * inv_m
            own = jnp.concatenate([st_s[h, 0:1, :], st_s[h, 1:2, :]], axis=1)
            mine = jnp.exp(jnp.maximum(own - mt, -3e38))
            for k, row in enumerate((w / zs, w / zt * mine)):
                col[k, h * ht:(h + 1) * ht, :] = jnp.broadcast_to(row, (128, ht)).T
            return jnp.sum(w * kl, axis=1, keepdims=True)

        def dlogit(h):
            base = h * ht

            def rstep(i, _):
                r = pl.ds(pl.multiple_of(base + i * 16, 16), 16)
                cs, ct = col[0, r, :], col[1, r, :]
                for q in range(voc // 128):
                    lanes = slice(q * 128, (q + 1) * 128)
                    th = tv[r, lanes]
                    ps = jnp.exp2(th * (CAP * LOG2E)) * cs
                    t_v[r, lanes] = ((ps - tx[r, (q ^ 2) * 128:(q ^ 2) * 128 + 128] * ct) * (1.0 - th * th)).astype(BF16)
                return 0

            lax.fori_loop(0, ht // 16, rstep, 0)

        def dgrad(h):
            rows = slice(h * ht, (h + 1) * ht)
            dg[:, rows] = lax.dot_general(et[...], t_v[rows, :], (((1,), (1,)), ((), ())), preferred_element_type=F32)

        pos1, pos2 = (z, y), (y, z)

        def chunk(h, q):
            return pl.ds(pl.multiple_of(h * ht + q * zc, zc), zc)

        def frows(q, half):
            return pl.ds(pl.multiple_of(q * fp + half * (fp // 2), 8), fp // 2)

        def dev1(h):
            return lambda q: {'tp': q * SIDE + y if h == 0 else z * SIDE + q, 'dp': d}

        def dev2(h):
            return lambda q: {'tp': z * SIDE + q if h == 0 else q * SIDE + y, 'dp': d}

        def make(h):
            r1 = RingSum(lambda q, half: dg.at[half * half_d:(half + 1) * half_d, chunk(h, q)], lambda k: zr.at[h, k],
                         ss_z.at[h], rs_z.at[h], dev1(h), pos1[h])
            r2 = RingSum(lambda q, half: dg.at[frows(q, half), chunk(h, pos1[h])], lambda k: p2r.at[h, k],
                         ss_p.at[h], rs_p.at[h], dev2(h), pos2[h])
            g1 = RingGather(lambda q, half: agb.at[h, frows(q, half), :], ss_g.at[h], rs_g.at[h], dev2(h), pos2[h])
            g2 = RingGather(lambda q, half: dhf.at[half * half_d:(half + 1) * half_d, chunk(h, q)],
                            ss_h.at[h], rs_h.at[h], dev1(h), pos1[h])
            return r1, r2, g1, g2

        ring = (make(0), make(1))

        def rs_end(h):
            r1, r2 = ring[h][:2]
            lo_v, hi_v = r1.end()
            r1.sl(r1.p, 0)[...] = lo_v
            r1.sl(r1.p, 1)[...] = hi_v
            r2.start()

        def p2_end(h):
            r2, g1 = ring[h][1:3]
            lo_v, hi_v = r2.end()
            g1.sl(g1.p, 0)[...] = lo_v
            g1.sl(g1.p, 1)[...] = hi_v
            g1.start()

        def norm_back(h):
            g1, g2 = ring[h][2:]
            g1.end()
            ck = chunk(h, pos1[h])
            gv = agb[h]
            xv = hid[:, ck].astype(F32)
            s = lax.rsqrt(jnp.mean(xv * xv, axis=0, keepdims=True) + EPS)
            cv = gv * wpc[:, :zc]
            m = jnp.mean(cv * xv, axis=0, keepdims=True)
            dwv = jnp.sum(pad_f(gv * xv * s, 0).T, axis=0, keepdims=True)
            for k in range(8):
                part = dwv[:, k * 128:(k + 1) * 128] if k < dpad // 128 else jnp.zeros((1, 128), F32)
                dwa_s[h, k:k + 1, :] = part
            dwa_r[h, pos1[h]] = dwa_s[h]
            cps = [rcopy(dwa_s.at[h], dwa_r.at[h, pos1[h]], ss_wa.at[h, k], rs_wa.at[h, k], dev1(h)(lax.rem(pos1[h] + k, SIDE)))
                   for k in range(1, SIDE)]
            dhf[:, ck] = s * cv - xv * (s * s * s * m)
            return cps

        def ag_end(h):
            ring[h][3].end()
            rows = slice(h * ht, (h + 1) * ht)
            t_v[0:dim, rows] = dhf[:, rows].astype(BF16)
            cp = pltpu.make_async_copy(t_v.at[0:dim, rows], dh_out.at[:, rows], out_sem.at[h])
            cp.start()
            outs.append(cp)

        def de_start(j):
            tv[0:dim, j * vc:(j + 1) * vc] = jnp.dot(gt[...], t_v[:, j * vc:(j + 1) * vc], preferred_element_type=F32)
            other = pl.ds(pl.multiple_of((1 - c) * half_d, 8), half_d)
            return rcopy(tv.at[other, j * vc:(j + 1) * vc], d2r.at[j], ss_d.at[j], rs_d.at[j], {'tp': t, 'dp': x * 2 + 1 - c})

        def make_x(j):
            def sl(q, half):
                return tv.at[pl.ds(pl.multiple_of(c * half_d + q * cols, 8), cols), j * vc + half * vh:j * vc + (half + 1) * vh]

            return RingSum(sl, lambda k: xr.at[j, k], ss_x.at[j], rs_x.at[j], lambda q: {'tp': t, 'dp': q * 2 + c}, x)

        xring = [make_x(j) for j in range(NV)]

        def x_start(j, cp):
            cp.wait_recv()
            mine = pl.ds(pl.multiple_of(c * half_d, 8), half_d)
            tv[mine, j * vc:(j + 1) * vc] += d2r[j]
            xring[j].start()

        def x_end(j):
            lo_v, hi_v = xring[j].end()
            tx[0:cols, j * vc:j * vc + vh] = lo_v
            tx[0:cols, j * vc + vh:(j + 1) * vc] = hi_v
            cp = pltpu.make_async_copy(tx.at[0:cols, j * vc:(j + 1) * vc], det_out.at[:, j * vc:(j + 1) * vc], out_sem.at[2 + j])
            cp.start()
            outs.append(cp)

        with jax.named_scope('s00_st0_forward_0_'):
            st0 = forward(0)
        with jax.named_scope('s01_mk_cp_rcopy_mk_s_mk_r_at_d_s'):
            mk_cp = [rcopy(mk_s, mk_r.at[d], ss_mk.at[k], rs_mk.at[k], {'tp': t, 'dp': lax.rem(d + k, nd)}) for k in range(1, nd)]
        with jax.named_scope('s02_st1_forward_1_'):
            st1 = forward(1)
        with jax.named_scope('s03_for_cp_in_mk_cp_'):
            for cp in mk_cp:
                cp.wait_recv()
        with jax.named_scope('s04_inv_m_1_0_jnp_sum_mk_r_0_axi'):
            inv_m = 1.0 / jnp.sum(mk_r[:, 0, :], axis=0, keepdims=True)[:, 0:1]
        with jax.named_scope('s05_loss_combine_0_st0_inv_m_'):
            loss = combine(0, st0, inv_m)
        with jax.named_scope('s06_dlogit_0_'):
            dlogit(0)
        with jax.named_scope('s07_dgrad_0_'):
            dgrad(0)
        with jax.named_scope('s08_ring_0_0_start_'):
            ring[0][0].start()
        with jax.named_scope('s09_loss_loss_combine_1_st1_inv_'):
            loss = loss + combine(1, st1, inv_m)
        with jax.named_scope('s10_dlogit_1_'):
            dlogit(1)
        with jax.named_scope('s11_dgrad_1_'):
            dgrad(1)
        with jax.named_scope('s12_ring_1_0_start_'):
            ring[1][0].start()
        with jax.named_scope('s13_dd_None_NV'):
            dd = [None] * NV
        with jax.named_scope('s14_dd_0_de_start_0_'):
            dd[0] = de_start(0)
        with jax.named_scope('s15_dd_1_de_start_1_'):
            dd[1] = de_start(1)
        with jax.named_scope('s16_ring_0_0_mid_'):
            ring[0][0].mid()
        with jax.named_scope('s17_dd_2_de_start_2_'):
            dd[2] = de_start(2)
        with jax.named_scope('s18_x_start_0_dd_0_'):
            x_start(0, dd[0])
        with jax.named_scope('s19_dd_3_de_start_3_'):
            dd[3] = de_start(3)
        with jax.named_scope('s20_x_start_1_dd_1_'):
            x_start(1, dd[1])
        with jax.named_scope('s21_dd_4_de_start_4_'):
            dd[4] = de_start(4)
        with jax.named_scope('s22_x_start_2_dd_2_'):
            x_start(2, dd[2])
        with jax.named_scope('s23_dd_5_de_start_5_'):
            dd[5] = de_start(5)
        with jax.named_scope('s24_x_start_3_dd_3_'):
            x_start(3, dd[3])
        with jax.named_scope('s25_x_start_4_dd_4_'):
            x_start(4, dd[4])
        with jax.named_scope('s26_ring_1_0_mid_'):
            ring[1][0].mid()
        with jax.named_scope('s27_x_start_5_dd_5_'):
            x_start(5, dd[5])
        with jax.named_scope('s28_xring_0_mid_'):
            xring[0].mid()
        with jax.named_scope('s29_rs_end_0_'):
            rs_end(0)
        with jax.named_scope('s30_xring_1_mid_'):
            xring[1].mid()
        with jax.named_scope('s31_rs_end_1_'):
            rs_end(1)
        with jax.named_scope('s32_ring_0_1_mid_'):
            ring[0][1].mid()
        with jax.named_scope('s33_xring_2_mid_'):
            xring[2].mid()
        with jax.named_scope('s34_ring_1_1_mid_'):
            ring[1][1].mid()
        with jax.named_scope('s35_p2_end_0_'):
            p2_end(0)
        with jax.named_scope('s36_xring_3_mid_'):
            xring[3].mid()
        with jax.named_scope('s37_p2_end_1_'):
            p2_end(1)
        with jax.named_scope('s38_ring_0_2_mid_'):
            ring[0][2].mid()
        with jax.named_scope('s39_ring_1_2_mid_'):
            ring[1][2].mid()
        with jax.named_scope('s40_wa0_norm_back_0_'):
            wa0 = norm_back(0)
        with jax.named_scope('s41_ring_0_3_start_'):
            ring[0][3].start()
        with jax.named_scope('s42_xring_4_mid_'):
            xring[4].mid()
        with jax.named_scope('s43_wa1_norm_back_1_'):
            wa1 = norm_back(1)
        with jax.named_scope('s44_ring_1_3_start_'):
            ring[1][3].start()
        with jax.named_scope('s45_xring_5_mid_'):
            xring[5].mid()
        with jax.named_scope('s46_ring_0_3_mid_'):
            ring[0][3].mid()
        with jax.named_scope('s47_for_cp_in_wa0_wa1_'):
            for cp in wa0 + wa1:
                cp.wait_recv()
        with jax.named_scope('s48_dws_jnp_sum_dwa_r_0_axis_0_j'):
            dws = jnp.sum(dwa_r[0], axis=0) + jnp.sum(dwa_r[1], axis=0)
        with jax.named_scope('s49_rowi_lax_broadcasted_iota_jn'):
            rowi = lax.broadcasted_iota(jnp.int32, (8, 128), 0)
        with jax.named_scope('s50_dwd_s_jnp_where_rowi_7_jnp_b'):
            dwd_s[...] = jnp.where(rowi == 7, jnp.broadcast_to(loss, (8, 128)), dws)
        with jax.named_scope('s51_dwd_r_d_dwd_s_'):
            dwd_r[d] = dwd_s[...]
        with jax.named_scope('s52_wd_rcopy_dwd_s_dwd_r_at_d_ss'):
            wd = [rcopy(dwd_s, dwd_r.at[d], ss_wd.at[k], rs_wd.at[k], {'tp': t, 'dp': lax.rem(d + k, nd)}) for k in range(1, nd)]
        with jax.named_scope('s53_x_end_0_'):
            x_end(0)
        with jax.named_scope('s54_ring_1_3_mid_'):
            ring[1][3].mid()
        with jax.named_scope('s55_x_end_1_'):
            x_end(1)
        with jax.named_scope('s56_x_end_2_'):
            x_end(2)
        with jax.named_scope('s57_x_end_3_'):
            x_end(3)
        with jax.named_scope('s58_ag_end_0_'):
            ag_end(0)
        with jax.named_scope('s59_x_end_4_'):
            x_end(4)
        with jax.named_scope('s60_x_end_5_'):
            x_end(5)
        with jax.named_scope('s61_for_cp_in_wd_'):
            for cp in wd:
                cp.wait_recv()
        with jax.named_scope('s62_fin_jnp_sum_dwd_r_axis_0_'):
            fin[...] = jnp.sum(dwd_r[...], axis=0)
        with jax.named_scope('s63_outs_append_pltpu_make_async'):
            outs.append(pltpu.make_async_copy(fin, small_out, out_sem.at[2 + NV]))
        with jax.named_scope('s64_outs_1_start_'):
            outs[-1].start()
        with jax.named_scope('s65_ag_end_1_'):
            ag_end(1)
        with jax.named_scope('s66_for_cp_in_sends_'):
            for cp in sends:
                cp.wait_send()
        with jax.named_scope('s67_for_cp_in_outs_'):
            for cp in outs:
                cp.wait()

    sem = pltpu.SemaphoreType.DMA
    vmem = pltpu.VMEM
    scratch = [
        vmem((dim, voc), BF16), vmem((tok, voc), BF16), vmem((tok, dim), BF16), vmem((dim, tok), BF16),
        vmem((tok, voc), F32), vmem((tok, voc), F32), vmem((2, ht, vb), F32), vmem((dim, 128), F32),
        vmem((dim, tok), F32), vmem((dim, tok), F32),
        vmem((3, ht, 128), F32), vmem((2, ht, 128), F32), vmem((2, tok, 128), F32),
        vmem((2, 8, hh), F32), vmem((2, nt, 8, hh), F32), vmem((8, 128), F32), vmem((nd, 8, 128), F32),
        vmem((2, 8, 128), F32), vmem((2, SIDE, 8, 128), F32), vmem((8, 128), F32), vmem((nd, 8, 128), F32), vmem((8, 128), F32),
        vmem((2, 6, half_d, zc), F32), vmem((2, 6, fp // 2, zc), F32), vmem((2, dim, zc), F32),
        vmem((NV, half_d, vc), F32), vmem((NV, 6, cols, vh), F32),
        sem((3,)), sem((2, nt)), sem((2, nt)), sem((nd,)), sem((nd,)), sem((2, 6)), sem((2, 6)), sem((2, 6)), sem((2, 6)),
        sem((2, 6)), sem((2, 6)), sem((2, 6)), sem((2, 6)), sem((NV,)), sem((NV,)), sem((NV, 6)), sem((NV, 6)),
        sem((2, SIDE)), sem((2, SIDE)), sem((nd,)), sem((nd,)), sem((3 + NV,)),
    ]
    vm = pl.BlockSpec(memory_space=pltpu.VMEM)
    anys = pl.BlockSpec(memory_space=pl.ANY)
    return pl.pallas_call(
        kernel,
        out_shape=(jax.ShapeDtypeStruct((dim, tok), BF16), jax.ShapeDtypeStruct((cols, voc), F32), jax.ShapeDtypeStruct((8, 128), F32)),
        in_specs=[vm, vm, vm, anys, anys],
        out_specs=(anys, anys, anys),
        scratch_shapes=scratch,
        compiler_params=pltpu.CompilerParams(collective_id=0, has_side_effects=True, vmem_limit_bytes=67043328),
        name='head',
    )


def finish(tok, dim, voc, cols):
    parts = 4
    rb, lb = tok // parts, voc // parts

    def kernel(dh, det, small, dh_o, det_o, dw_o, loss_o, hb, eb, sb, wb, lb_v, sem_i, sem_o):
        views = []
        for i in range(parts):
            ls, es = pl.ds(i * rb, rb), pl.ds(i * lb, lb)
            views.append((dh.at[:, ls], hb.at[:, ls], dh_o.at[:, ls]))
            views.append((det.at[:, es], eb.at[:, es], det_o.at[:, es]))
        ins = [pltpu.make_async_copy(small, sb, sem_i.at[2 * parts])]
        ins += [pltpu.make_async_copy(a, b, sem_i.at[k]) for k, (a, b, _) in enumerate(views)]
        outs = [pltpu.make_async_copy(wb, dw_o, sem_o.at[2 * parts]), pltpu.make_async_copy(lb_v, loss_o, sem_o.at[2 * parts + 1])]
        outs += [pltpu.make_async_copy(b, o, sem_o.at[k]) for k, (_, b, o) in enumerate(views)]
        for cp in ins:
            cp.start()
        ins[0].wait()
        row = jnp.concatenate([sb[k:k + 1, :] for k in range(-(-dim // 128))], axis=1)
        wb[...] = row[:, :dim].reshape(dim)
        lb_v[...] = sb[7:8, 0:1]
        outs[0].start()
        outs[1].start()
        for ci, co in zip(ins[1:], outs[2:]):
            ci.wait()
            co.start()
        for co in outs:
            co.wait()

    anys = pl.BlockSpec(memory_space=pl.ANY)
    return pl.pallas_call(
        kernel,
        out_shape=(jax.ShapeDtypeStruct((dim, tok), BF16), jax.ShapeDtypeStruct((cols, voc), F32),
                   jax.ShapeDtypeStruct((dim,), F32), jax.ShapeDtypeStruct((1, 1), F32)),
        in_specs=[anys, anys, anys],
        out_specs=(anys, anys, anys, anys),
        scratch_shapes=[pltpu.VMEM((dim, tok), BF16), pltpu.VMEM((cols, voc), F32), pltpu.VMEM((8, 128), F32), pltpu.VMEM((dim,), F32),
                        pltpu.VMEM((1, 1), F32), pltpu.SemaphoreType.DMA((2 * parts + 1,)), pltpu.SemaphoreType.DMA((2 * parts + 2,))],
        compiler_params=pltpu.CompilerParams(vmem_limit_bytes=67043328),
        name='finish',
    )


def solution(mesh):
    nt, nd = mesh.shape['tp'], mesh.shape['dp']

    def device_fn(hid, norm_w, emb, teach, mask):
        tok, dim = hid.shape
        call = build(tok, dim, emb.shape[0], nt, nd)
        dh, det, small = call(hid.T, norm_w, mask.reshape(1, tok), emb.T, teach)
        dh, det, dw, loss = finish(tok, dim, emb.shape[0], dim // nd)(dh, det, small)
        return loss.reshape(()), dh.T, det.T, dw

    return jax.shard_map(device_fn, mesh=mesh, in_specs=(P('dp', None), P(None), P('tp', None), P('dp', 'tp'), P('dp')),
                         out_specs=(P(), P('dp', None), P('tp', 'dp'), P(None)), check_vma=False)
```

```python
import jax
import jax.numpy as jnp
from jax import lax
from jax.experimental import pallas as pl
from jax.experimental.pallas import tpu as pltpu
from jax.sharding import PartitionSpec as P

CAP = 30.0
EPS = 1e-6
LOG2E = 1.4426950408889634
LN2 = 0.6931471805599453
MESH = pl.DeviceIdType.MESH
F32 = jnp.float32
BF16 = jnp.bfloat16
SIDE = 4
NV = 6


def build(tok, dim, voc, nt, nd):
    ht = tok // 2
    hh = ht // 2
    zc = ht // SIDE
    fp = dim // SIDE
    cols = dim // nd
    vc = voc // NV
    vh = vc // 2
    half_d = dim // 2
    dpad = -(-dim // 128) * 128

    def kernel(hid, w_ref, mask_ref, e_hbm, t_hbm, dh_out, det_out, small_out,
               et, t_v, gb, gt, tv, tx, wpc, dg, dhf, acc, mcol, col, st_s, st_r, mk_s, mk_r, dwa_s, dwa_r, dwd_s, dwd_r, fin,
               zr, p2r, agb, d2r, xr,
               in_sem, ss_st, rs_st, ss_mk, rs_mk, ss_z, rs_z, ss_p, rs_p, ss_g, rs_g, ss_h, rs_h,
               ss_d, rs_d, ss_x, rs_x, ss_wa, rs_wa, ss_wd, rs_wd, out_sem):
        t = lax.axis_index('tp')
        d = lax.axis_index('dp')
        z, y = t // SIDE, lax.rem(t, SIDE)
        x, c = d // 2, lax.rem(d, 2)
        sends = []
        outs = []

        def rcopy(src, dst, ssem, rsem, dev):
            cp = pltpu.make_async_remote_copy(src_ref=src, dst_ref=dst, send_sem=ssem, recv_sem=rsem,
                                              device_id=dev, device_id_type=MESH)
            cp.start()
            sends.append(cp)
            return cp

        class RingSum:
            def __init__(self, sl, buf, ss, rs, dev, p):
                self.sl, self.buf, self.ss, self.rs, self.dev = sl, buf, ss, rs, dev
                self.p, self.nxt, self.prv, self.opp = p, lax.rem(p + 1, SIDE), lax.rem(p + 3, SIDE), lax.rem(p + 2, SIDE)

            def send(self, k, q, half, to):
                return rcopy(self.sl(q, half), self.buf(k), self.ss.at[k], self.rs.at[k], self.dev(to))

            def start(self):
                self.a0 = self.send(0, self.opp, 0, self.nxt)
                self.a1 = self.send(1, self.opp, 1, self.prv)
                self.b0 = self.send(2, self.nxt, 1, self.nxt)
                self.b1 = self.send(3, self.prv, 0, self.prv)

            def mid(self):
                self.a0.wait_recv()
                part = self.sl(self.nxt, 0)
                part[...] += self.buf(0)[...]
                self.c0 = self.send(4, self.nxt, 0, self.nxt)
                self.a1.wait_recv()
                part = self.sl(self.prv, 1)
                part[...] += self.buf(1)[...]
                self.c1 = self.send(5, self.prv, 1, self.prv)

            def end(self):
                for cp in (self.b0, self.b1, self.c0, self.c1):
                    cp.wait_recv()
                return (self.sl(self.p, 0)[...] + self.buf(4)[...] + self.buf(3)[...],
                        self.sl(self.p, 1)[...] + self.buf(2)[...] + self.buf(5)[...])

        class RingGather:
            def __init__(self, sl, ss, rs, dev, p):
                self.sl, self.ss, self.rs, self.dev = sl, ss, rs, dev
                self.p, self.nxt, self.prv = p, lax.rem(p + 1, SIDE), lax.rem(p + 3, SIDE)

            def send(self, k, q, half, to):
                return rcopy(self.sl(q, half), self.sl(q, half), self.ss.at[k], self.rs.at[k], self.dev(to))

            def start(self):
                self.a0 = self.send(0, self.p, 0, self.nxt)
                self.a1 = self.send(1, self.p, 1, self.prv)
                self.b0 = self.send(2, self.p, 1, self.nxt)
                self.b1 = self.send(3, self.p, 0, self.prv)

            def mid(self):
                self.a0.wait_recv()
                self.c0 = self.send(4, self.prv, 0, self.nxt)
                self.a1.wait_recv()
                self.c1 = self.send(5, self.nxt, 1, self.prv)

            def end(self):
                for cp in (self.b0, self.b1, self.c0, self.c1):
                    cp.wait_recv()

        in_cp = [pltpu.make_async_copy(e_hbm, et, in_sem.at[0])]
        for h in range(2):
            rows = pl.ds(h * ht, ht)
            in_cp.append(pltpu.make_async_copy(t_hbm.at[rows, :], t_v.at[rows, :], in_sem.at[1 + h]))
        for cp in (in_cp[1], in_cp[0], in_cp[2]):
            cp.start()

        barrier = pltpu.get_barrier_semaphore()
        for k in range(1, nt):
            pl.semaphore_signal(barrier, inc=1, device_id={'tp': lax.rem(t + k, nt), 'dp': d}, device_id_type=MESH)
        for k in range(1, nd):
            pl.semaphore_signal(barrier, inc=1, device_id={'tp': t, 'dp': lax.rem(d + k, nd)}, device_id_type=MESH)

        def pad_f(a, axis):
            shape = list(a.shape)
            shape[axis] = dpad - dim
            return jnp.concatenate([a, jnp.zeros(shape, F32)], axis=axis) if dpad > dim else a

        wrow = pad_f(1.0 + w_ref[...].astype(F32).reshape(1, dim), 1)
        wpc[...] = jnp.broadcast_to(wrow, (128, dpad)).T[:dim, :]

        def norm_step(i, _):
            r0 = pl.multiple_of(i * 128, 128)
            xv = hid[:, pl.ds(r0, 128)].astype(F32)
            s = lax.rsqrt(jnp.mean(xv * xv, axis=0, keepdims=True) + EPS)
            g = xv * s * wpc[...]
            gb[pl.ds(r0, 128), :] = pad_f(g, 0).T[:, :dim].astype(BF16)
            gp = [g[(2 * xx + cc) * cols:(2 * xx + cc + 1) * cols, :] for cc in range(2) for xx in range(SIDE)]
            gt[:, pl.ds(r0, 128)] = jnp.concatenate(gp, axis=0).astype(BF16)
            return 0

        lax.fori_loop(0, tok // 128, norm_step, 0)

        maskf = mask_ref[...].astype(F32)
        mk_s[...] = jnp.broadcast_to(jnp.sum(maskf, axis=1, keepdims=True), (8, 128))
        mk_r[d] = mk_s[...]

        def forward(h):
            base = h * ht
            in_cp[1 + h].wait()

            def mx(i, _):
                r = pl.multiple_of(base + i * 64, 64)
                m = t_v[pl.ds(r, 64), 0:128]
                for q in range(1, voc // 128):
                    m = jnp.maximum(m, t_v[pl.ds(r, 64), q * 128:(q + 1) * 128])
                mm = jnp.max(m.astype(F32), axis=1, keepdims=True)
                mcol[h, pl.ds(pl.multiple_of(i * 64, 64), 64), :] = jnp.broadcast_to(mm, (64, 128))
                return 0

            lax.fori_loop(0, ht // 64, mx, 0)
            if h == 0:
                in_cp[0].wait()
            tv[base:base + ht, :] = jnp.dot(gb[base:base + ht, :], et[...], preferred_element_type=F32)

            def rstep(i, _):
                a = pl.ds(pl.multiple_of(i * 16, 16), 16)
                r = pl.ds(pl.multiple_of(base + i * 16, 16), 16)
                m = mcol[h, a, :]
                zs = zt = qs = jnp.zeros((16, 128), F32)
                for q in range(voc // 128):
                    lanes = slice(q * 128, (q + 1) * 128)
                    th = jnp.tanh(tv[r, lanes] * (1.0 / CAP))
                    tv[r, lanes] = th
                    u = (t_v[r, lanes].astype(F32) - m) * LOG2E
                    v = th * (CAP * LOG2E)
                    ex = jnp.exp2(u)
                    tx[r, (q ^ 2) * 128:(q ^ 2) * 128 + 128] = ex
                    zs = zs + jnp.exp2(v)
                    zt = zt + ex
                    qs = qs + ex * (u - v)
                acc[0, a, :] = zs
                acc[1, a, :] = zt
                acc[2, a, :] = qs
                return 0

            lax.fori_loop(0, ht // 16, rstep, 0)
            parts = [mcol[h].T[0:1, :]] + [jnp.sum(acc[k].T, axis=0, keepdims=True) for k in range(3)]
            st_s[h] = jnp.concatenate([p[:, i * hh:(i + 1) * hh] for p in parts for i in range(2)], axis=0)
            st_r[h, t] = st_s[h]
            if h == 0:
                pl.semaphore_wait(barrier, nt + nd - 2)
            return [rcopy(st_s.at[h], st_r.at[h, t], ss_st.at[h, k], rs_st.at[h, k], {'tp': lax.rem(t + k, nt), 'dp': d})
                    for k in range(1, nt)]

        def combine(h, cps, inv_m):
            for cp in cps:
                cp.wait_recv()
            def stat(k):
                return jnp.concatenate([st_r[h, :, 2 * k, :], st_r[h, :, 2 * k + 1, :]], axis=1)

            mts = stat(0)
            mt = jnp.max(mts, axis=0, keepdims=True)
            dm = jnp.maximum(mts - mt, -3e38)
            e = jnp.exp(dm)
            zte = stat(2) * e
            zt = jnp.sum(zte, axis=0, keepdims=True)
            zs = jnp.sum(stat(1), axis=0, keepdims=True)
            a = jnp.sum(stat(3) * LN2 * e + zte * dm, axis=0, keepdims=True)
            kl = a / zt - jnp.log(zt) + jnp.log(zs)
            w = maskf[:, h * ht:(h + 1) * ht] * inv_m
            own = jnp.concatenate([st_s[h, 0:1, :], st_s[h, 1:2, :]], axis=1)
            mine = jnp.exp(jnp.maximum(own - mt, -3e38))
            for k, row in enumerate((w / zs, w / zt * mine)):
                col[k, h * ht:(h + 1) * ht, :] = jnp.broadcast_to(row, (128, ht)).T
            return jnp.sum(w * kl, axis=1, keepdims=True)

        def dlogit(h):
            base = h * ht

            def rstep(i, _):
                r = pl.ds(pl.multiple_of(base + i * 16, 16), 16)
                cs, ct = col[0, r, :], col[1, r, :]
                for q in range(voc // 128):
                    lanes = slice(q * 128, (q + 1) * 128)
                    th = tv[r, lanes]
                    ps = jnp.exp2(th * (CAP * LOG2E)) * cs
                    t_v[r, lanes] = ((ps - tx[r, (q ^ 2) * 128:(q ^ 2) * 128 + 128] * ct) * (1.0 - th * th)).astype(BF16)
                return 0

            lax.fori_loop(0, ht // 16, rstep, 0)

        def dgrad(h):
            rows = slice(h * ht, (h + 1) * ht)
            dg[:, rows] = lax.dot_general(et[...], t_v[rows, :], (((1,), (1,)), ((), ())), preferred_element_type=F32)

        pos1, pos2 = (z, y), (y, z)

        def chunk(h, q):
            return pl.ds(pl.multiple_of(h * ht + q * zc, zc), zc)

        def frows(q, half):
            return pl.ds(pl.multiple_of(q * fp + half * (fp // 2), 8), fp // 2)

        def dev1(h):
            return lambda q: {'tp': q * SIDE + y if h == 0 else z * SIDE + q, 'dp': d}

        def dev2(h):
            return lambda q: {'tp': z * SIDE + q if h == 0 else q * SIDE + y, 'dp': d}

        def make(h):
            r1 = RingSum(lambda q, half: dg.at[half * half_d:(half + 1) * half_d, chunk(h, q)], lambda k: zr.at[h, k],
                         ss_z.at[h], rs_z.at[h], dev1(h), pos1[h])
            r2 = RingSum(lambda q, half: dg.at[frows(q, half), chunk(h, pos1[h])], lambda k: p2r.at[h, k],
                         ss_p.at[h], rs_p.at[h], dev2(h), pos2[h])
            g1 = RingGather(lambda q, half: agb.at[h, frows(q, half), :], ss_g.at[h], rs_g.at[h], dev2(h), pos2[h])
            g2 = RingGather(lambda q, half: dhf.at[half * half_d:(half + 1) * half_d, chunk(h, q)],
                            ss_h.at[h], rs_h.at[h], dev1(h), pos1[h])
            return r1, r2, g1, g2

        ring = (make(0), make(1))

        def rs_end(h):
            r1, r2 = ring[h][:2]
            lo_v, hi_v = r1.end()
            r1.sl(r1.p, 0)[...] = lo_v
            r1.sl(r1.p, 1)[...] = hi_v
            r2.start()

        def p2_end(h):
            r2, g1 = ring[h][1:3]
            lo_v, hi_v = r2.end()
            g1.sl(g1.p, 0)[...] = lo_v
            g1.sl(g1.p, 1)[...] = hi_v
            g1.start()

        def norm_back(h):
            g1, g2 = ring[h][2:]
            g1.end()
            ck = chunk(h, pos1[h])
            gv = agb[h]
            xv = hid[:, ck].astype(F32)
            s = lax.rsqrt(jnp.mean(xv * xv, axis=0, keepdims=True) + EPS)
            cv = gv * wpc[:, :zc]
            m = jnp.mean(cv * xv, axis=0, keepdims=True)
            dwv = jnp.sum(pad_f(gv * xv * s, 0).T, axis=0, keepdims=True)
            for k in range(8):
                part = dwv[:, k * 128:(k + 1) * 128] if k < dpad // 128 else jnp.zeros((1, 128), F32)
                dwa_s[h, k:k + 1, :] = part
            dwa_r[h, pos1[h]] = dwa_s[h]
            cps = [rcopy(dwa_s.at[h], dwa_r.at[h, pos1[h]], ss_wa.at[h, k], rs_wa.at[h, k], dev1(h)(lax.rem(pos1[h] + k, SIDE)))
                   for k in range(1, SIDE)]
            dhf[:, ck] = s * cv - xv * (s * s * s * m)
            return cps

        def ag_end(h):
            ring[h][3].end()
            rows = slice(h * ht, (h + 1) * ht)
            t_v[0:dim, rows] = dhf[:, rows].astype(BF16)
            cp = pltpu.make_async_copy(t_v.at[0:dim, rows], dh_out.at[:, rows], out_sem.at[h])
            cp.start()
            outs.append(cp)

        def de_start(j):
            tv[0:dim, j * vc:(j + 1) * vc] = jnp.dot(gt[...], t_v[:, j * vc:(j + 1) * vc], preferred_element_type=F32)
            other = pl.ds(pl.multiple_of((1 - c) * half_d, 8), half_d)
            return rcopy(tv.at[other, j * vc:(j + 1) * vc], d2r.at[j], ss_d.at[j], rs_d.at[j], {'tp': t, 'dp': x * 2 + 1 - c})

        def make_x(j):
            def sl(q, half):
                return tv.at[pl.ds(pl.multiple_of(c * half_d + q * cols, 8), cols), j * vc + half * vh:j * vc + (half + 1) * vh]

            return RingSum(sl, lambda k: xr.at[j, k], ss_x.at[j], rs_x.at[j], lambda q: {'tp': t, 'dp': q * 2 + c}, x)

        xring = [make_x(j) for j in range(NV)]

        def x_start(j, cp):
            cp.wait_recv()
            mine = pl.ds(pl.multiple_of(c * half_d, 8), half_d)
            tv[mine, j * vc:(j + 1) * vc] += d2r[j]
            xring[j].start()

        def x_end(j):
            lo_v, hi_v = xring[j].end()
            tx[0:cols, j * vc:j * vc + vh] = lo_v
            tx[0:cols, j * vc + vh:(j + 1) * vc] = hi_v
            cp = pltpu.make_async_copy(tx.at[0:cols, j * vc:(j + 1) * vc], det_out.at[:, j * vc:(j + 1) * vc], out_sem.at[2 + j])
            cp.start()
            outs.append(cp)

        with jax.named_scope('s00_st0_forward_0_'):
            st0 = forward(0)
        with jax.named_scope('s01_mk_cp_rcopy_mk_s_mk_r_at_d_s'):
            mk_cp = [rcopy(mk_s, mk_r.at[d], ss_mk.at[k], rs_mk.at[k], {'tp': t, 'dp': lax.rem(d + k, nd)}) for k in range(1, nd)]
        with jax.named_scope('s02_st1_forward_1_'):
            st1 = forward(1)
        with jax.named_scope('s03_for_cp_in_mk_cp_'):
            for cp in mk_cp:
                cp.wait_recv()
        with jax.named_scope('s04_inv_m_1_0_jnp_sum_mk_r_0_axi'):
            inv_m = 1.0 / jnp.sum(mk_r[:, 0, :], axis=0, keepdims=True)[:, 0:1]
        with jax.named_scope('s05_loss_combine_0_st0_inv_m_'):
            loss = combine(0, st0, inv_m)
        with jax.named_scope('s06_dlogit_0_'):
            dlogit(0)
        with jax.named_scope('s07_dgrad_0_'):
            dgrad(0)
        with jax.named_scope('s08_ring_0_0_start_'):
            ring[0][0].start()
        with jax.named_scope('s09_loss_loss_combine_1_st1_inv_'):
            loss = loss + combine(1, st1, inv_m)
        with jax.named_scope('s10_dlogit_1_'):
            dlogit(1)
        with jax.named_scope('s11_dgrad_1_'):
            dgrad(1)
        with jax.named_scope('s12_ring_1_0_start_'):
            ring[1][0].start()
        with jax.named_scope('s13_dd_None_NV'):
            dd = [None] * NV
        with jax.named_scope('s14_dd_0_de_start_0_'):
            dd[0] = de_start(0)
        with jax.named_scope('s15_dd_1_de_start_1_'):
            dd[1] = de_start(1)
        with jax.named_scope('s16_ring_0_0_mid_'):
            ring[0][0].mid()
        with jax.named_scope('s17_dd_2_de_start_2_'):
            dd[2] = de_start(2)
        with jax.named_scope('s18_x_start_0_dd_0_'):
            x_start(0, dd[0])
        with jax.named_scope('s19_dd_3_de_start_3_'):
            dd[3] = de_start(3)
        with jax.named_scope('s20_x_start_1_dd_1_'):
            x_start(1, dd[1])
        with jax.named_scope('s21_dd_4_de_start_4_'):
            dd[4] = de_start(4)
        with jax.named_scope('s22_x_start_2_dd_2_'):
            x_start(2, dd[2])
        with jax.named_scope('s23_dd_5_de_start_5_'):
            dd[5] = de_start(5)
        with jax.named_scope('s24_x_start_3_dd_3_'):
            x_start(3, dd[3])
        with jax.named_scope('s25_x_start_4_dd_4_'):
            x_start(4, dd[4])
        with jax.named_scope('s26_ring_1_0_mid_'):
            ring[1][0].mid()
        with jax.named_scope('s27_x_start_5_dd_5_'):
            x_start(5, dd[5])
        with jax.named_scope('s28_xring_0_mid_'):
            xring[0].mid()
        with jax.named_scope('s29_rs_end_0_'):
            rs_end(0)
        with jax.named_scope('s30_xring_1_mid_'):
            xring[1].mid()
        with jax.named_scope('s31_rs_end_1_'):
            rs_end(1)
        with jax.named_scope('s32_ring_0_1_mid_'):
            ring[0][1].mid()
        with jax.named_scope('s33_xring_2_mid_'):
            xring[2].mid()
        with jax.named_scope('s34_ring_1_1_mid_'):
            ring[1][1].mid()
        with jax.named_scope('s35_p2_end_0_'):
            p2_end(0)
        with jax.named_scope('s36_xring_3_mid_'):
            xring[3].mid()
        with jax.named_scope('s37_p2_end_1_'):
            p2_end(1)
        with jax.named_scope('s38_ring_0_2_mid_'):
            ring[0][2].mid()
        with jax.named_scope('s39_ring_1_2_mid_'):
            ring[1][2].mid()
        with jax.named_scope('s40_wa0_norm_back_0_'):
            wa0 = norm_back(0)
        with jax.named_scope('s41_ring_0_3_start_'):
            ring[0][3].start()
        with jax.named_scope('s42_xring_4_mid_'):
            xring[4].mid()
        with jax.named_scope('s43_wa1_norm_back_1_'):
            wa1 = norm_back(1)
        with jax.named_scope('s44_ring_1_3_start_'):
            ring[1][3].start()
        with jax.named_scope('s45_xring_5_mid_'):
            xring[5].mid()
        with jax.named_scope('s46_ring_0_3_mid_'):
            ring[0][3].mid()
        with jax.named_scope('s47_for_cp_in_wa0_wa1_'):
            for cp in wa0 + wa1:
                cp.wait_recv()
        with jax.named_scope('s48_dws_jnp_sum_dwa_r_0_axis_0_j'):
            dws = jnp.sum(dwa_r[0], axis=0) + jnp.sum(dwa_r[1], axis=0)
        with jax.named_scope('s49_rowi_lax_broadcasted_iota_jn'):
            rowi = lax.broadcasted_iota(jnp.int32, (8, 128), 0)
        with jax.named_scope('s50_dwd_s_jnp_where_rowi_7_jnp_b'):
            dwd_s[...] = jnp.where(rowi == 7, jnp.broadcast_to(loss, (8, 128)), dws)
        with jax.named_scope('s51_dwd_r_d_dwd_s_'):
            dwd_r[d] = dwd_s[...]
        with jax.named_scope('s52_wd_rcopy_dwd_s_dwd_r_at_d_ss'):
            wd = [rcopy(dwd_s, dwd_r.at[d], ss_wd.at[k], rs_wd.at[k], {'tp': t, 'dp': lax.rem(d + k, nd)}) for k in range(1, nd)]
        with jax.named_scope('s53_x_end_0_'):
            x_end(0)
        with jax.named_scope('s54_ring_1_3_mid_'):
            ring[1][3].mid()
        with jax.named_scope('s55_x_end_1_'):
            x_end(1)
        with jax.named_scope('s56_x_end_2_'):
            x_end(2)
        with jax.named_scope('s57_x_end_3_'):
            x_end(3)
        with jax.named_scope('s58_ag_end_0_'):
            ag_end(0)
        with jax.named_scope('s59_x_end_4_'):
            x_end(4)
        with jax.named_scope('s60_x_end_5_'):
            x_end(5)
        with jax.named_scope('s61_for_cp_in_wd_'):
            for cp in wd:
                cp.wait_recv()
        with jax.named_scope('s62_fin_jnp_sum_dwd_r_axis_0_'):
            fin[...] = jnp.sum(dwd_r[...], axis=0)
        with jax.named_scope('s63_outs_append_pltpu_make_async'):
            outs.append(pltpu.make_async_copy(fin, small_out, out_sem.at[2 + NV]))
        with jax.named_scope('s64_outs_1_start_'):
            outs[-1].start()
        with jax.named_scope('s65_ag_end_1_'):
            ag_end(1)
        with jax.named_scope('s66_for_cp_in_sends_'):
            for cp in sends:
                cp.wait_send()
        with jax.named_scope('s67_for_cp_in_outs_'):
            for cp in outs:
                cp.wait()

    sem = pltpu.SemaphoreType.DMA
    vmem = pltpu.VMEM
    scratch = [
        vmem((dim, voc), BF16), vmem((tok, voc), BF16), vmem((tok, dim), BF16), vmem((dim, tok), BF16),
        vmem((tok, voc), F32), vmem((tok, voc), F32), vmem((dim, 128), F32),
        vmem((dim, tok), F32), vmem((dim, tok), F32),
        vmem((3, ht, 128), F32), vmem((2, ht, 128), F32), vmem((2, tok, 128), F32),
        vmem((2, 8, hh), F32), vmem((2, nt, 8, hh), F32), vmem((8, 128), F32), vmem((nd, 8, 128), F32),
        vmem((2, 8, 128), F32), vmem((2, SIDE, 8, 128), F32), vmem((8, 128), F32), vmem((nd, 8, 128), F32), vmem((8, 128), F32),
        vmem((2, 6, half_d, zc), F32), vmem((2, 6, fp // 2, zc), F32), vmem((2, dim, zc), F32),
        vmem((NV, half_d, vc), F32), vmem((NV, 6, cols, vh), F32),
        sem((3,)), sem((2, nt)), sem((2, nt)), sem((nd,)), sem((nd,)), sem((2, 6)), sem((2, 6)), sem((2, 6)), sem((2, 6)),
        sem((2, 6)), sem((2, 6)), sem((2, 6)), sem((2, 6)), sem((NV,)), sem((NV,)), sem((NV, 6)), sem((NV, 6)),
        sem((2, SIDE)), sem((2, SIDE)), sem((nd,)), sem((nd,)), sem((3 + NV,)),
    ]
    vm = pl.BlockSpec(memory_space=pltpu.VMEM)
    anys = pl.BlockSpec(memory_space=pl.ANY)
    return pl.pallas_call(
        kernel,
        out_shape=(jax.ShapeDtypeStruct((dim, tok), BF16), jax.ShapeDtypeStruct((cols, voc), F32), jax.ShapeDtypeStruct((8, 128), F32)),
        in_specs=[vm, vm, vm, anys, anys],
        out_specs=(anys, anys, anys),
        scratch_shapes=scratch,
        compiler_params=pltpu.CompilerParams(collective_id=0, has_side_effects=True, vmem_limit_bytes=67043328),
        name='head',
    )


def finish(tok, dim, voc, cols):
    parts = 4
    rb, lb = tok // parts, voc // parts

    def kernel(dh, det, small, dh_o, det_o, dw_o, loss_o, hb, eb, sb, wb, lb_v, sem_i, sem_o):
        views = []
        for i in range(parts):
            ls, es = pl.ds(i * rb, rb), pl.ds(i * lb, lb)
            views.append((dh.at[:, ls], hb.at[:, ls], dh_o.at[:, ls]))
            views.append((det.at[:, es], eb.at[:, es], det_o.at[:, es]))
        ins = [pltpu.make_async_copy(small, sb, sem_i.at[2 * parts])]
        ins += [pltpu.make_async_copy(a, b, sem_i.at[k]) for k, (a, b, _) in enumerate(views)]
        outs = [pltpu.make_async_copy(wb, dw_o, sem_o.at[2 * parts]), pltpu.make_async_copy(lb_v, loss_o, sem_o.at[2 * parts + 1])]
        outs += [pltpu.make_async_copy(b, o, sem_o.at[k]) for k, (_, b, o) in enumerate(views)]
        for cp in ins:
            cp.start()
        ins[0].wait()
        row = jnp.concatenate([sb[k:k + 1, :] for k in range(-(-dim // 128))], axis=1)
        wb[...] = row[:, :dim].reshape(dim)
        lb_v[...] = sb[7:8, 0:1]
        outs[0].start()
        outs[1].start()
        for ci, co in zip(ins[1:], outs[2:]):
            ci.wait()
            co.start()
        for co in outs:
            co.wait()

    anys = pl.BlockSpec(memory_space=pl.ANY)
    return pl.pallas_call(
        kernel,
        out_shape=(jax.ShapeDtypeStruct((dim, tok), BF16), jax.ShapeDtypeStruct((cols, voc), F32),
                   jax.ShapeDtypeStruct((dim,), F32), jax.ShapeDtypeStruct((1, 1), F32)),
        in_specs=[anys, anys, anys],
        out_specs=(anys, anys, anys, anys),
        scratch_shapes=[pltpu.VMEM((dim, tok), BF16), pltpu.VMEM((cols, voc), F32), pltpu.VMEM((8, 128), F32), pltpu.VMEM((dim,), F32),
                        pltpu.VMEM((1, 1), F32), pltpu.SemaphoreType.DMA((2 * parts + 1,)), pltpu.SemaphoreType.DMA((2 * parts + 2,))],
        compiler_params=pltpu.CompilerParams(vmem_limit_bytes=67043328),
        name='finish',
    )


def solution(mesh):
    nt, nd = mesh.shape['tp'], mesh.shape['dp']

    def device_fn(hid, norm_w, emb, teach, mask):
        tok, dim = hid.shape
        call = build(tok, dim, emb.shape[0], nt, nd)
        dh, det, small = call(hid.T, norm_w, mask.reshape(1, tok), emb.T, teach)
        dh, det, dw, loss = finish(tok, dim, emb.shape[0], dim // nd)(dh, det, small)
        return loss.reshape(()), dh.T, det.T, dw

    return jax.shard_map(device_fn, mesh=mesh, in_specs=(P('dp', None), P(None), P('tp', None), P('dp', 'tp'), P('dp')),
                         out_specs=(P(), P('dp', None), P('tp', 'dp'), P(None)), check_vma=False)
```
